32 devices in a mesh: sp: 4 (over z), ctx: 4 (over y, x), fsdp: 2 (over core).
Axes of the slice: x: 2, y: 2, z: 4, core: 2. Of those that a mesh axis runs over, the one named last changes fastest.
Arguments:
- block_input: bfloat16 [2, 4, 512, 2048], P('fsdp', 'ctx', 'sp'), may hold values from -6 to 6
- cotangent: bfloat16 [2, 4, 512, 2048], P('fsdp', 'ctx', 'sp'), may hold values from -6 to 6
- decay_rate: float32 [8], replicated, may hold values from 4.8828125e-05 to 0.0333333333
- weight_in: float32 [2048, 16384], P(('sp', 'ctx', 'fsdp')), may hold values from -0.125 to 0.125
- weight_out: float32 [4096, 4096], P(('sp', 'ctx', 'fsdp')), may hold values from -0.09375 to 0.09375
- norm_gains: float32 [4, 2048], P(None, ('sp', 'ctx', 'fsdp')), may hold values from -0.9 to 1.6
- moment_in: float32 [2048, 16384], P(('sp', 'ctx', 'fsdp')), may hold values from -6 to 6
- square_in: float32 [2048, 16384], P(('sp', 'ctx', 'fsdp')), may hold values from 8.192 to 32.768
- moment_out: float32 [4096, 4096], P(('sp', 'ctx', 'fsdp')), may hold values from -6 to 6
- square_out: float32 [4096, 4096], P(('sp', 'ctx', 'fsdp')), may hold values from 8.192 to 32.768
- moment_norm: float32 [4, 2048], P(None, ('sp', 'ctx', 'fsdp')), may hold values from -6 to 6
- square_norm: float32 [4, 2048], P(None, ('sp', 'ctx', 'fsdp')), may hold values from 8.192 to 32.768
Outputs:
- block_output: bfloat16 [2, 4, 512, 2048], P('fsdp', 'ctx', 'sp')
- grad_input: bfloat16 [2, 4, 512, 2048], P('fsdp', 'ctx', 'sp')
- grad_weight_in: float32 [2048, 16384], P(('sp', 'ctx', 'fsdp'))
- new_moment_in: float32 [2048, 16384], P(('sp', 'ctx', 'fsdp'))
- new_square_in: float32 [2048, 16384], P(('sp', 'ctx', 'fsdp'))
- update_in: float32 [2048, 16384], P(('sp', 'ctx', 'fsdp'))
- grad_weight_out: float32 [4096, 4096], P(('sp', 'ctx', 'fsdp'))
- new_moment_out: float32 [4096, 4096], P(('sp', 'ctx', 'fsdp'))
- new_square_out: float32 [4096, 4096], P(('sp', 'ctx', 'fsdp'))
- update_out: float32 [4096, 4096], P(('sp', 'ctx', 'fsdp'))
- grad_norm: float32 [4, 2048], P(None, ('sp', 'ctx', 'fsdp'))
- new_moment_norm: float32 [4, 2048], P(None, ('sp', 'ctx', 'fsdp'))
- new_square_norm: float32 [4, 2048], P(None, ('sp', 'ctx', 'fsdp'))
- update_norm: float32 [4, 2048], P(None, ('sp', 'ctx', 'fsdp'))
The draws below stay inside these ranges and needn't reach their ends.
All inputs are finite; a program needn't handle non-finite values.
Results may differ from the reference program's by a relative error of at most 0.018.
The reference program's roundings to bfloat16 on the way count: a program that leaves them out, or rounds other values in their place, can miss the bound.
Values may be sent and summed in bfloat16 or wider, within the bound.
A program may use at most 456 MiB of HBM per device.

```python
import math
import jax
import jax.numpy as jnp
from jax import lax

D = 2048
H = 8
DK = 256
DV = 512
SPAN = 512
STEP = 10
QK = 2048
VD = 4096
WIN = 16384
BLOCK = 512
SEQ_LEN = 2048
SEQS = 2
TOKENS = 4096
N_CTX = 4


def draw_decay_rate(key, part):
    order = jax.random.permutation(jax.random.fold_in(key, 11), H)
    slow_count = H // 2
    spread = jax.random.uniform(jax.random.fold_in(key, 12), (H,), jnp.float32)
    slow_rate = jnp.exp(jnp.log(0.1 / SEQ_LEN) + spread * jnp.log(10.0))
    fast_rate = jnp.exp(jnp.log(1.0 / 50.0) + spread * jnp.log(50.0 / 30.0))
    return jnp.where(order < slow_count, slow_rate, fast_rate).astype(jnp.float32)


def draw_norm_gains(key, part):
    spread = jax.random.truncated_normal(jax.random.fold_in(key, 21), -3.0, 3.0, (4, D), jnp.float32)
    row_index = lax.broadcasted_iota(jnp.int32, (4, D), 0)
    return jnp.where(row_index % 2 == 0, 1.0 + 0.2 * spread, 0.3 * spread).astype(jnp.float32)


def level_of(own_key, extent, shards, least, largest):
    def one(axis_at, blocks):
        draws = jax.random.uniform(jax.random.fold_in(jax.random.fold_in(own_key, 6), axis_at), (blocks,), jnp.float32, least / len(shards), largest / len(shards))
        return jnp.repeat(jnp.exp(draws), extent[axis_at] // blocks).reshape((-1,) + (1,) * (len(extent) - axis_at - 1))

    loudness = one(*shards[0])
    for cut in shards[1:]:
        loudness = loudness * one(*cut)
    return loudness


def normal_values(own_key, shape, width, most, cuts=(), kind=jnp.bfloat16):
    drawn = width * jax.random.normal(own_key, shape, jnp.float32)
    if cuts:
        drawn = drawn * level_of(own_key, shape, cuts, -0.22, 0.18)
    return jnp.clip(drawn, -most, most).astype(kind)


def setup_inputs(seed: int = 0) -> dict:
    key_of = jax.random.split(jax.random.key(seed), 13)
    block_input = normal_values(key_of[0], (SEQS, N_CTX, BLOCK, D), 1.0, 6.0, ((0, 2), (1, 4), (2, 4)))
    cotangent = normal_values(key_of[1], (SEQS, N_CTX, BLOCK, D), 1.0, 6.0, ((0, 2), (1, 4), (2, 4)))
    decay_rate = draw_decay_rate(jax.random.fold_in(key_of[12], 71), 0)
    weight_in = normal_values(key_of[3], (D, WIN), D ** -0.5, 0.125, ((0, 32),), jnp.float32)
    weight_out = normal_values(key_of[4], (VD, 2 * D), VD ** -0.5, 0.09375, ((0, 32),), jnp.float32)
    norm_gains = draw_norm_gains(jax.random.fold_in(key_of[12], 71), 0)
    moment_in = normal_values(key_of[6], (D, WIN), (0.03 * TOKENS ** 0.5), 6.0, ((0, 32),), jnp.float32)
    square_in = jnp.clip(8.192 + 24.576 * jax.random.uniform(key_of[7], (D, WIN), jnp.float32) ** level_of(key_of[7], (D, WIN), ((0, 32),), -0.2, 0.2), 8.192, 32.768)
    moment_out = normal_values(key_of[8], (VD, 2 * D), (0.03 * TOKENS ** 0.5), 6.0, ((0, 32),), jnp.float32)
    square_out = jnp.clip(8.192 + 24.576 * jax.random.uniform(key_of[9], (VD, 2 * D), jnp.float32) ** level_of(key_of[9], (VD, 2 * D), ((0, 32),), -0.2, 0.2), 8.192, 32.768)
    moment_norm = normal_values(key_of[10], (4, D), (0.03 * TOKENS ** 0.5), 6.0, ((1, 32),), jnp.float32)
    square_norm = jnp.clip(8.192 + 24.576 * jax.random.uniform(key_of[11], (4, D), jnp.float32) ** level_of(key_of[11], (4, D), ((1, 32),), -0.2, 0.2), 8.192, 32.768)
    return dict(block_input=block_input, cotangent=cotangent, decay_rate=decay_rate, weight_in=weight_in, weight_out=weight_out, norm_gains=norm_gains, moment_in=moment_in, square_in=square_in, moment_out=moment_out, square_out=square_out, moment_norm=moment_norm, square_norm=square_norm)


@jax.custom_vjp
def reduced_precision(v):
    return lax.optimization_barrier(v.astype(jnp.bfloat16)).astype(jnp.float32)

@jax.custom_vjp
def reduced_backward(v):
    return v

def low_keep(v):
    return (reduced_precision(v), None)

def low_pass(kept, grad):
    return (grad,)

def back_keep(v):
    return (v, None)

def back_low(kept, grad):
    return (reduced_precision(grad),)
reduced_precision.defvjp(low_keep, low_pass)
reduced_backward.defvjp(back_keep, back_low)
top_precision_mode = lax.Precision.HIGHEST
beta_one = 0.9
beta_two = 0.95
learn_rate = 0.01
decay_weight = 0.1
adam_eps = 1e-08
norm_eps = 1e-05

def layer_norm(values, gain_row, shift_row):
    centred = values - lax.optimization_barrier(jnp.mean(values, axis=-1, keepdims=True))
    return centred * lax.rsqrt(lax.optimization_barrier(jnp.mean(centred * centred, axis=-1, keepdims=True)) + norm_eps) * gain_row + shift_row

def angles(length):
    half_size = DK // 2
    inverse = jnp.exp(-math.log(10000.0) * (2.0 * jnp.arange(half_size, dtype=jnp.float32) / DK))
    phases = jnp.arange(length, dtype=jnp.float32)[:, None] * inverse[None, :]
    return (jnp.cos(phases), jnp.sin(phases))

def rotate(values, cosine, sine):
    half_size = values.shape[-1] // 2
    first_half = values[..., :half_size]
    second_half = values[..., half_size:]
    return jnp.concatenate([first_half * cosine - second_half * sine, second_half * cosine + first_half * sine], -1)

def retain(queries, keys_all, values_all, rates):
    pieces = queries.shape[0] // SPAN
    offsets = jnp.arange(SPAN, dtype=jnp.float32)
    spacing = offsets[:, None] - offsets[None, :]
    decay_mask = jnp.where(spacing[None] >= 0.0, jnp.exp(-rates[:, None, None] * jnp.maximum(spacing, 0.0)[None]), 0.0)
    inward = jnp.exp(-rates[None, :] * (offsets[:, None] + 1.0))
    target_dtype_cast = jnp.exp(-rates[None, :] * (SPAN - 1.0 - offsets[:, None]))
    span_fall = jnp.exp(-rates * SPAN)

    def advance(running_state, span_data):
        query_shard_piece, key_shard_piece, value_shard_piece = span_data
        scores = reduced_backward(jnp.einsum('ihk,jhk->hij', query_shard_piece, key_shard_piece, precision=top_precision_mode))
        prob_low = reduced_precision(scores * decay_mask)
        inner_sum = jnp.einsum('hij,jhv->ihv', prob_low, value_shard_piece, precision=top_precision_mode)
        readout_total = reduced_backward(jnp.einsum('map,apn->man', query_shard_piece, reduced_precision(running_state), precision=top_precision_mode))
        apply_adamw_step = reduced_backward(jnp.einsum('wfa,wfz->faz', reduced_precision(key_shard_piece * target_dtype_cast[:, :, None]), value_shard_piece, precision=top_precision_mode))
        return (span_fall[:, None, None] * running_state + apply_adamw_step, inner_sum + readout_total * inward[:, :, None])
    stacked = (queries.reshape(pieces, SPAN, H, DK), keys_all.reshape(pieces, SPAN, H, DK), values_all.reshape(pieces, SPAN, H, DV))
    _, outputs = lax.scan(jax.checkpoint(advance), jnp.zeros((H, DK, DV), jnp.float32), stacked)
    return outputs.reshape(queries.shape[0], H, DV)

def forward(inputs, first_weight, second_weight, gain_rows, rates):
    win_low = reduced_precision(first_weight)
    wout_low = reduced_precision(second_weight)
    gains = reduced_precision(gain_rows)
    seq_count = inputs.shape[0]
    flat_rows = inputs.reshape(-1, D)
    normed_a = reduced_precision(layer_norm(flat_rows, gains[0], gains[1]))
    cut_at = 2 * QK + 2 * VD
    projected = jnp.dot(normed_a, win_low[:, :cut_at], precision=top_precision_mode)
    cosine, sine = angles(SEQ_LEN)
    cosine = cosine[None, :, None, :]
    sine = sine[None, :, None, :]
    queries = reduced_precision(rotate(reduced_backward(projected[:, :QK]).reshape(seq_count, SEQ_LEN, H, DK), cosine, sine))
    keys_all = reduced_precision(rotate(reduced_backward(projected[:, QK:2 * QK]).reshape(seq_count, SEQ_LEN, H, DK), cosine, sine))
    values_all = reduced_backward(reduced_precision(projected[:, 2 * QK:2 * QK + VD])).reshape(seq_count, SEQ_LEN, H, DV)
    gate_pre = reduced_backward(projected[:, 2 * QK + VD:])
    retained = lax.map(lambda sequence: retain(sequence[0], sequence[1], sequence[2], rates), (queries, keys_all, values_all))
    retained = reduced_backward(reduced_precision(retained)).reshape(-1, H, DV)
    centred = retained - lax.optimization_barrier(jnp.mean(retained, axis=-1, keepdims=True))
    unit_vals = (centred * lax.rsqrt(lax.optimization_barrier(jnp.mean(centred * centred, axis=-1, keepdims=True)) + norm_eps)).reshape(-1, VD)
    gated = reduced_precision(gate_pre * jax.nn.sigmoid(gate_pre) * unit_vals)
    branch = reduced_backward(jnp.dot(gated, wout_low[:, :D], precision=top_precision_mode))
    hidden = flat_rows + branch
    normed_b = reduced_precision(layer_norm(hidden, gains[2], gains[3]))
    up_proj = reduced_backward(jnp.dot(normed_b, win_low[:, cut_at:], precision=top_precision_mode))
    activated = reduced_precision(jax.nn.gelu(up_proj, approximate=False))
    ffn_out = reduced_backward(jnp.dot(activated, wout_low[:, D:], precision=top_precision_mode))
    return (hidden + ffn_out).reshape(inputs.shape)

def adam_update(weight, grad_vals, moment, square):
    moment_new = beta_one * moment + (1.0 - beta_one) * grad_vals
    square_new = beta_two * square + (1.0 - beta_two) * grad_vals * grad_vals
    moment_hat = moment_new / (1.0 - beta_one ** STEP)
    square_hat = square_new / (1.0 - beta_two ** STEP)
    step_vals = -learn_rate * (moment_hat / (jnp.sqrt(square_hat) + adam_eps) + decay_weight * weight)
    return (moment_new, square_new, step_vals)

def reference(block_input, cotangent, decay_rate, weight_in, weight_out, norm_gains, moment_in, square_in, moment_out, square_out, moment_norm, square_norm):

    def wrapped(inputs, first_weight, second_weight, gain_rows):
        return forward(inputs, first_weight, second_weight, gain_rows, decay_rate)
    result, pull_back = jax.vjp(wrapped, block_input.astype(jnp.float32), weight_in, weight_out, norm_gains)
    grad_x, grad_first, grad_second, grad_gains = pull_back(cotangent.astype(jnp.float32))
    first_m, first_v, first_step = adam_update(weight_in, grad_first, moment_in, square_in)
    second_m, second_v, second_step = adam_update(weight_out, grad_second, moment_out, square_out)
    gain_m, gain_v, gain_step = adam_update(norm_gains, grad_gains, moment_norm, square_norm)
    return (result.astype(jnp.bfloat16), grad_x.astype(jnp.bfloat16), grad_first, first_m, first_v, first_step, grad_second, second_m, second_v, second_step, grad_gains, gain_m, gain_v, gain_step)
```

```python
import math

import jax
import jax.numpy as jnp
from jax import lax
from jax.sharding import PartitionSpec as P

H = 8
DK = 256
DV = 512
SPAN = 512
STEP = 10
QK = 2048
VD = 4096

beta_one = 0.9
beta_two = 0.95
learn_rate = 0.01
decay_weight = 0.1
adam_eps = 1e-08
norm_eps = 1e-05
root_half = 0.7071067811865476
inv_root_tau = 0.3989422804014327

BF = jnp.bfloat16
F32 = jnp.float32
ALL = ("sp", "ctx", "fsdp")
PLANE = ("ctx", "fsdp")


def layer_stats(values, gain_row, shift_row):
    centred = values - jnp.mean(values, axis=-1, keepdims=True)
    inv_std = lax.rsqrt(jnp.mean(centred * centred, axis=-1, keepdims=True) + norm_eps)
    unit_vals = centred * inv_std
    return (unit_vals * gain_row + shift_row, unit_vals, inv_std)


def layer_back(grad_vals, unit_vals, inv_std, gain_row):
    scaled = grad_vals * gain_row
    return inv_std * (
        scaled
        - jnp.mean(scaled, axis=-1, keepdims=True)
        - unit_vals * jnp.mean(scaled * unit_vals, axis=-1, keepdims=True)
    )


def angles(positions, head_size):
    half_size = head_size // 2
    inverse = jnp.exp(
        -math.log(10000.0) * (2.0 * jnp.arange(half_size, dtype=jnp.float32) / head_size)
    )
    phases = positions.astype(jnp.float32)[:, None] * inverse[None, :]
    return (jnp.cos(phases), jnp.sin(phases))


def rotate(values, cosine, sine, sign_flip):
    half_size = values.shape[-1] // 2
    first_half = values[..., :half_size]
    second_half = values[..., half_size:]
    return jnp.concatenate(
        [
            first_half * cosine - sign_flip * (second_half * sine),
            second_half * cosine + sign_flip * (first_half * sine),
        ],
        -1,
    )


def adam_update(weight, grad_vals, moment, square):
    moment_new = beta_one * moment + (1.0 - beta_one) * grad_vals
    square_new = beta_two * square + (1.0 - beta_two) * grad_vals * grad_vals
    moment_hat = moment_new / (1.0 - beta_one**STEP)
    square_hat = square_new / (1.0 - beta_two**STEP)
    step_vals = -learn_rate * (
        moment_hat / (jnp.sqrt(square_hat) + adam_eps) + decay_weight * weight
    )
    return (moment_new, square_new, step_vals)


def mm(a, b):
    return jnp.dot(a, b, preferred_element_type=F32)


def mm_t(a, b):
    return lax.dot_general(a, b, (((1,), (1,)), ((), ())), preferred_element_type=F32)


def mm_tn(a, b):
    return lax.dot_general(a, b, (((0,), (0,)), ((), ())), preferred_element_type=F32)


def ein(spec, a, b):
    return jnp.einsum(spec, a, b, preferred_element_type=F32)


def shards(
    block_input,
    cotangent,
    decay_rate,
    weight_in,
    weight_out,
    norm_gains,
    moment_in,
    square_in,
    moment_out,
    square_out,
    moment_norm,
    square_norm,
):
    tok_count = block_input.shape[2]
    width = block_input.shape[3]
    sp_n = lax.axis_size("sp")
    ctx_n = lax.axis_size("ctx")
    plane_n = ctx_n * lax.axis_size("fsdp")
    heads = H // sp_n
    block_len = tok_count * sp_n
    sp_i = lax.axis_index("sp")
    ctx_i = lax.axis_index("ctx")
    rows_in = weight_in.shape[0]
    qk_w, vd_w = QK // sp_n, VD // sp_n
    widths = (qk_w, qk_w, vd_w, vd_w, vd_w)
    starts = (0, QK, 2 * QK, 2 * QK + VD, 2 * QK + 2 * VD)
    cut = 2 * qk_w + 2 * vd_w

    def perm(v):
        return v.reshape(-1, sp_n, plane_n, rows_in).swapaxes(1, 2).reshape(v.shape)

    def unperm(v):
        return v.reshape(-1, plane_n, sp_n, rows_in).swapaxes(1, 2).reshape(v.shape)

    w_low = weight_in.astype(BF)
    slabs = jnp.concatenate(
        [w_low[:, o : o + sp_n * w].reshape(rows_in, sp_n, w) for o, w in zip(starts, widths)], 2
    )
    turned = lax.all_to_all(slabs.swapaxes(0, 1), "sp", split_axis=0, concat_axis=0, tiled=True)
    turned = turned.reshape(sp_n * rows_in, -1)
    w_proj = lax.all_gather(turned[:, :cut], PLANE, axis=0, tiled=True)
    w_up = lax.all_gather(turned[:, cut:], PLANE, axis=0, tiled=True)
    o_low = weight_out.astype(BF)
    w_o = lax.all_gather(o_low[:, :width], PLANE, axis=0, tiled=True)
    w_down = lax.all_gather(o_low[:, width:], PLANE, axis=0, tiled=True)
    gains = lax.all_gather(norm_gains.astype(BF), ALL, axis=1, tiled=True).astype(F32)
    gains_p = perm(gains)

    own_x = block_input.reshape(tok_count, width)
    own_xp = perm(own_x)
    grad_ffn_own = cotangent.reshape(tok_count, width)
    full_x = lax.all_gather(own_xp, "sp", axis=0, tiled=True).astype(F32)
    grad_ffn = lax.all_gather(grad_ffn_own, "sp", axis=0, tiled=True)
    normed_a, _, _ = layer_stats(full_x, gains_p[0], gains_p[1])
    a_low = normed_a.astype(BF)
    proj = mm(a_low, w_proj)
    head_pos = ctx_i * block_len + jnp.arange(block_len, dtype=jnp.int32)
    cos_h, sin_h = angles(head_pos, DK)

    def split_heads(v, size):
        return v.reshape(block_len, heads, size).swapaxes(0, 1)

    def join_heads(v):
        return v.swapaxes(0, 1).reshape(block_len, -1)

    qs = rotate(split_heads(proj[:, :qk_w], DK), cos_h, sin_h, 1.0).astype(BF)
    ks = rotate(split_heads(proj[:, qk_w : 2 * qk_w], DK), cos_h, sin_h, 1.0).astype(BF)
    vs = split_heads(proj[:, 2 * qk_w : 2 * qk_w + vd_w], DV).astype(BF)
    gate = split_heads(proj[:, 2 * qk_w + vd_w :], DV)

    rates = lax.dynamic_slice_in_dim(decay_rate, sp_i * heads, heads)
    offs = jnp.arange(block_len, dtype=F32)
    spacing = offs[:, None] - offs[None, :]
    mask = jnp.where(
        spacing[None] >= 0.0, jnp.exp(-rates[:, None, None] * jnp.maximum(spacing, 0.0)[None]), 0.0
    )
    inward = jnp.exp(-rates[:, None] * (offs[None, :] + 1.0))[:, :, None]
    outward = jnp.exp(-rates[:, None] * (block_len - 1.0 - offs[None, :]))[:, :, None]
    blocks = jnp.arange(ctx_n)
    back_gap = (ctx_i - 1 - blocks).astype(F32)
    back_w = jnp.where(
        blocks[:, None] < ctx_i,
        jnp.exp(-rates[None, :] * block_len * jnp.maximum(back_gap, 0.0)[:, None]),
        0.0,
    )
    fore_gap = (blocks - ctx_i - 1).astype(F32)
    fore_w = jnp.where(
        blocks[:, None] > ctx_i,
        jnp.exp(-rates[None, :] * block_len * jnp.maximum(fore_gap, 0.0)[:, None]),
        0.0,
    )

    key_decayed = (ks * outward).astype(BF)
    own_state = ein("hjk,hjv->hkv", key_decayed, vs)
    states = lax.all_gather(own_state.astype(BF), "ctx").astype(F32)
    state = jnp.sum(states * back_w[:, :, None, None], 0).astype(BF)
    scores = ein("hik,hjk->hij", qs, ks)
    probs = (scores * mask).astype(BF)
    mixed = (ein("hij,hjv->hiv", probs, vs) + ein("hik,hkv->hiv", qs, state) * inward).astype(BF)
    mixed_vals = mixed.astype(F32)
    centred = mixed_vals - jnp.mean(mixed_vals, axis=-1, keepdims=True)
    group_scale = lax.rsqrt(jnp.mean(centred * centred, axis=-1, keepdims=True) + norm_eps)
    unit_h = centred * group_scale
    gate_sig = jax.nn.sigmoid(gate)
    gate_act = gate * gate_sig
    gated = join_heads((gate_act * unit_h).astype(BF))
    branch = lax.psum_scatter(
        mm(gated, w_o).astype(BF), "sp", scatter_dimension=0, tiled=True
    ).astype(F32)
    hidden = own_x.astype(F32) + branch
    normed_b, unit_b, scale_b = layer_stats(hidden, gains[2], gains[3])
    b_low = lax.all_gather(perm(normed_b.astype(BF)), "sp", axis=0, tiled=True)
    up = mm(b_low, w_up)
    act_low = jax.nn.gelu(up, approximate=False).astype(BF)
    ffn = lax.psum_scatter(
        mm(act_low, w_down).astype(BF), "sp", scatter_dimension=0, tiled=True
    ).astype(F32)
    block_out = (hidden + ffn).astype(BF).reshape(block_input.shape)

    grad_top = grad_ffn_own.astype(F32)
    grad_act = mm_t(grad_ffn, w_down)
    density = (
        0.5 * (1.0 + lax.erf(up * root_half)) + up * jnp.exp(-0.5 * up * up) * inv_root_tau
    )
    grad_up = (grad_act * density).astype(BF)
    grad_b = unperm(
        lax.psum_scatter(
            mm_t(grad_up, w_up).astype(BF), "sp", scatter_dimension=0, tiled=True
        ).astype(F32)
    )
    grad_hidden = grad_top + layer_back(grad_b, unit_b, scale_b, gains[2])
    grad_branch = lax.all_gather(grad_hidden.astype(BF), "sp", axis=0, tiled=True)

    def reduce_rows(v):
        return lax.psum_scatter(v.astype(BF), PLANE, scatter_dimension=0, tiled=True)

    sum_down = reduce_rows(mm_tn(act_low, grad_ffn))
    sum_up = reduce_rows(mm_tn(b_low, grad_up))
    sum_o = reduce_rows(mm_tn(gated, grad_branch))

    grad_gated = split_heads(mm_t(grad_branch, w_o), DV)
    grad_gate = (grad_gated * unit_h * gate_sig * (1.0 + gate * (1.0 - gate_sig))).astype(BF)
    grad_unit = grad_gated * gate_act
    grad_mixed = (
        group_scale
        * (
            grad_unit
            - jnp.mean(grad_unit, axis=-1, keepdims=True)
            - unit_h * jnp.mean(grad_unit * unit_h, axis=-1, keepdims=True)
        )
    ).astype(BF)
    grad_read = (grad_mixed * inward).astype(BF)
    own_reach = ein("hik,hiv->hkv", qs, grad_read)
    reaches = lax.all_gather(own_reach.astype(BF), "ctx").astype(F32)
    reach = jnp.sum(reaches * fore_w[:, :, None, None], 0).astype(BF)
    grad_probs = ein("hiv,hjv->hij", grad_mixed, vs)
    grad_scores = (grad_probs * mask).astype(BF)
    grad_q = ein("hij,hjk->hik", grad_scores, ks) + ein("hiv,hkv->hik", grad_read, state)
    grad_k = ein("hij,hik->hjk", grad_scores, qs) + ein("hjv,hkv->hjk", vs, reach) * outward
    grad_v = ein("hij,hiv->hjv", probs, grad_mixed) + ein("hjk,hkv->hjv", key_decayed, reach)
    grad_proj = jnp.concatenate(
        [
            join_heads(rotate(grad_q, cos_h, sin_h, -1.0).astype(BF)),
            join_heads(rotate(grad_k, cos_h, sin_h, -1.0).astype(BF)),
            join_heads(grad_v.astype(BF)),
            join_heads(grad_gate),
        ],
        1,
    )
    grad_a = unperm(
        lax.psum_scatter(
            mm_t(grad_proj, w_proj).astype(BF), "sp", scatter_dimension=0, tiled=True
        ).astype(F32)
    )
    sum_proj = reduce_rows(mm_tn(a_low, grad_proj))
    _, unit_a, scale_a = layer_stats(own_x.astype(F32), gains[0], gains[1])
    grad_rows = grad_hidden + layer_back(grad_a, unit_a, scale_a, gains[0])
    grad_x = grad_rows.astype(BF).reshape(block_input.shape)
    norm_terms = jnp.stack(
        [
            jnp.sum(grad_a * unit_a, 0),
            jnp.sum(grad_a, 0),
            jnp.sum(grad_b * unit_b, 0),
            jnp.sum(grad_b, 0),
        ]
    )
    grad_gains = lax.psum_scatter(norm_terms, ALL, scatter_dimension=1, tiled=True)

    def home(v):
        v = v.reshape(sp_n, rows_in, -1)
        return lax.all_to_all(v, "sp", split_axis=0, concat_axis=0, tiled=True)

    back_proj = home(sum_proj)
    back_up = home(sum_up)
    edges = (0, qk_w, 2 * qk_w, 2 * qk_w + vd_w, cut)
    parts = [back_proj[:, :, a:b] for a, b in zip(edges[:-1], edges[1:])] + [back_up]
    grad_first = jnp.concatenate(
        [p.swapaxes(0, 1).reshape(rows_in, -1) for p in parts], 1
    ).astype(F32)
    grad_second = jnp.concatenate([sum_o, sum_down], 1).astype(F32)
    first_m, first_v, first_step = adam_update(weight_in, grad_first, moment_in, square_in)
    second_m, second_v, second_step = adam_update(weight_out, grad_second, moment_out, square_out)
    gain_m, gain_v, gain_step = adam_update(norm_gains, grad_gains, moment_norm, square_norm)
    return (
        block_out,
        grad_x,
        grad_first,
        first_m,
        first_v,
        first_step,
        grad_second,
        second_m,
        second_v,
        second_step,
        grad_gains,
        gain_m,
        gain_v,
        gain_step,
    )


def solution(mesh):
    tokens = P("fsdp", "ctx", "sp", None)
    rows = P(ALL, None)
    cols = P(None, ALL)
    in_specs = (tokens, tokens, P(), rows, rows, cols, rows, rows, rows, rows, cols, cols)
    out_specs = (tokens, tokens) + (rows,) * 8 + (cols,) * 4
    return jax.shard_map(shards, mesh=mesh, in_specs=in_specs, out_specs=out_specs, check_vma=False)
```

```python
import functools
import math

import jax
import jax.numpy as jnp
from jax import lax
from jax.experimental import pallas as pl
from jax.experimental.pallas import tpu as pltpu
from jax.sharding import PartitionSpec as P

H = 8
DK = 256
DV = 512
SPAN = 512
STEP = 10
QK = 2048
VD = 4096

beta_one = 0.9
beta_two = 0.95
learn_rate = 0.01
decay_weight = 0.1
adam_eps = 1e-08
norm_eps = 1e-05
root_half = 0.7071067811865476
inv_root_tau = 0.3989422804014327


BF = jnp.bfloat16
F32 = jnp.float32
ALL = ("sp", "ctx", "fsdp")
PLANE = ("ctx", "fsdp")


def layer_stats(values, gain_row, shift_row):
    centred = values - jnp.mean(values, axis=-1, keepdims=True)
    inv_std = lax.rsqrt(jnp.mean(centred * centred, axis=-1, keepdims=True) + norm_eps)
    unit_vals = centred * inv_std
    return (unit_vals * gain_row + shift_row, unit_vals, inv_std)


def layer_back(grad_vals, unit_vals, inv_std, gain_row):
    scaled = grad_vals * gain_row
    return inv_std * (
        scaled
        - jnp.mean(scaled, axis=-1, keepdims=True)
        - unit_vals * jnp.mean(scaled * unit_vals, axis=-1, keepdims=True)
    )


def angles(positions, head_size):
    half_size = head_size // 2
    inverse = jnp.exp(
        -math.log(10000.0) * (2.0 * jnp.arange(half_size, dtype=jnp.float32) / head_size)
    )
    phases = positions.astype(jnp.float32)[:, None] * inverse[None, :]
    return (jnp.cos(phases), jnp.sin(phases))


def rotate(values, cosine, sine, sign_flip):
    half_size = values.shape[-1] // 2
    first_half = values[..., :half_size]
    second_half = values[..., half_size:]
    return jnp.concatenate(
        [
            first_half * cosine - sign_flip * (second_half * sine),
            second_half * cosine + sign_flip * (first_half * sine),
        ],
        -1,
    )


def adam_update(weight, grad_vals, moment, square):
    moment_new = beta_one * moment + (1.0 - beta_one) * grad_vals
    square_new = beta_two * square + (1.0 - beta_two) * grad_vals * grad_vals
    moment_hat = moment_new / (1.0 - beta_one**STEP)
    square_hat = square_new / (1.0 - beta_two**STEP)
    step_vals = -learn_rate * (
        moment_hat / (jnp.sqrt(square_hat) + adam_eps) + decay_weight * weight
    )
    return (moment_new, square_new, step_vals)


def mm(a, b):
    return jnp.dot(a, b, preferred_element_type=F32)


def mm_t(a, b):
    return lax.dot_general(a, b, (((1,), (1,)), ((), ())), preferred_element_type=F32)


def mm_tn(a, b):
    return lax.dot_general(a, b, (((0,), (0,)), ((), ())), preferred_element_type=F32)


def ein(spec, a, b):
    return jnp.einsum(spec, a, b, preferred_element_type=F32)


MESH_ID = pl.DeviceIdType.MESH
ANY = pl.BlockSpec(memory_space=pl.ANY)
VM = pl.BlockSpec(memory_space=pltpu.VMEM)


def greet(peers):
    sem = pltpu.get_barrier_semaphore()
    for peer in peers:
        pl.semaphore_signal(sem, inc=1, device_id=peer, device_id_type=MESH_ID)
    pl.semaphore_wait(sem, len(peers))


def push(src, dst, send, recv, peer):
    copy = pltpu.make_async_remote_copy(
        src_ref=src, dst_ref=dst, send_sem=send, recv_sem=recv, device_id=peer, device_id_type=MESH_ID
    )
    copy.start()
    return copy


def arrived(dst, send, recv, peer):
    pltpu.make_async_remote_copy(
        src_ref=dst, dst_ref=dst, send_sem=send, recv_sem=recv, device_id=peer, device_id_type=MESH_ID
    ).wait_recv()


def beside(c):
    low = c + 1 - 2 * (c % 2)
    high = (c + 2) % 4
    return low, high, (low + 2) % 4


def params(ident):
    return pltpu.CompilerParams(collective_id=ident, has_side_effects=True)


def spread_kernel(sp_n, f_n, wp_in, wu_in, wo_in, wd_in, x_in, wp, wu, wo, wd, x, lsem, zs, zr, xs, xr, ps, pr, cs, cr):
    s, c, f = lax.axis_index("sp"), lax.axis_index("ctx"), lax.axis_index("fsdp")
    low, high, both = beside(c)
    lines = [lax.rem(s + j, sp_n) for j in range(sp_n)]
    cores = [lax.rem(f + k, f_n) for k in range(1, f_n)]
    greet(
        [{"sp": p} for p in lines[1:]]
        + [{"ctx": low}, {"ctx": high}]
        + [{"fsdp": p} for p in cores]
    )
    n_items = 2 * sp_n + 2
    waits = []

    def item_at(i, cc, ff):
        if i < 2:
            return (wo, wd)[i].at[cc, ff]
        j, a = (i - 2) // 2, (i - 2) % 2
        return (wp, wu)[a].at[cc, ff, lines[j]]

    def key(i):
        if i < 2:
            return i
        j, a = (i - 2) // 2, (i - 2) % 2
        return 2 + a * sp_n + lines[j]

    def own(i):
        if i < 2:
            return (wo_in, wd_in)[i]
        a = (i - 2) % 2
        return (wp_in, wu_in)[a].at[s]

    def start_local(n, src, dst):
        copy = pltpu.make_async_copy(src, dst, lsem.at[n])
        copy.start()
        return copy

    for j in range(1, sp_n):
        for a in range(2):
            src, dst = ((wp_in, wp), (wu_in, wu))[a]
            waits.append(
                push(src.at[lines[j]], dst.at[c, f, s], zs.at[a * sp_n + j], zr.at[a * sp_n + s], {"sp": lines[j]})
            )
    for j in range(1, sp_n):
        waits.append(push(x_in, x.at[s], xs.at[j], xr.at[s], {"sp": lines[j]}))
    local = [start_local(i, own(i), item_at(i, c, f)) for i in range(4)]
    local.append(start_local(4, x_in, x.at[s]))

    def to_cores(i, src, cc):
        for n, p in enumerate(cores):
            waits.append(
                push(
                    src,
                    item_at(i, cc, f),
                    cs.at[(n * 4 + cc) * n_items + i],
                    cr.at[(f * 4 + cc) * n_items + key(i)],
                    {"fsdp": p},
                )
            )

    def first(i):
        if i < 4:
            src = own(i)
        else:
            j, a = (i - 2) // 2, (i - 2) % 2
            arrived(item_at(i, c, f), zs.at[0], zr.at[a * sp_n + lines[j]], {"sp": lines[j]})
            src = item_at(i, c, f)
        for n, p in enumerate((low, high)):
            waits.append(
                push(src, item_at(i, c, f), ps.at[3 * i + n], pr.at[c * n_items + key(i)], {"ctx": p})
            )
        to_cores(i, src, c)

    def landed(i, cc):
        arrived(item_at(i, cc, f), ps.at[0], pr.at[cc * n_items + key(i)], {"ctx": cc})

    def second(i):
        landed(i, low)
        if i % 4 in (1, 2):
            waits.append(
                push(item_at(i, low, f), item_at(i, low, f), ps.at[3 * i + 2], pr.at[low * n_items + key(i)], {"ctx": high})
            )
        to_cores(i, item_at(i, low, f), low)
        landed(i, high)
        if i % 4 in (0, 3):
            waits.append(
                push(item_at(i, high, f), item_at(i, high, f), ps.at[3 * i + 2], pr.at[high * n_items + key(i)], {"ctx": low})
            )
        to_cores(i, item_at(i, high, f), high)

    def third(i):
        landed(i, both)
        to_cores(i, item_at(i, both, f), both)

    for i in range(n_items + 4):
        if i < n_items:
            first(i)
        if 2 <= i < n_items + 2:
            second(i - 2)
        if i >= 4:
            third(i - 4)
    for j in range(1, sp_n):
        arrived(x.at[lines[j]], xs.at[0], xr.at[lines[j]], {"sp": lines[j]})
    for p in cores:
        for cc in range(4):
            for i in range(n_items):
                arrived(item_at(i, cc, p), cs.at[0], cr.at[(p * 4 + cc) * n_items + key(i)], {"fsdp": p})
    for copy in waits:
        copy.wait_send()
    for copy in local:
        copy.wait()


def spread(wp_in, wu_in, wo_in, wd_in, x_in, sp_n, f_n, ident):
    rows = wp_in.shape[1]
    n_items = 2 * sp_n + 2
    shapes = [
        (4, f_n, sp_n, rows, wp_in.shape[2]),
        (4, f_n, sp_n, rows, wu_in.shape[2]),
        (4, f_n) + wo_in.shape,
        (4, f_n) + wd_in.shape,
        (sp_n,) + x_in.shape,
    ]
    dma = pltpu.SemaphoreType.DMA
    return pl.pallas_call(
        functools.partial(spread_kernel, sp_n, f_n),
        out_shape=[jax.ShapeDtypeStruct(v, BF) for v in shapes],
        in_specs=[VM] * 5,
        out_specs=[ANY] * 5,
        scratch_shapes=[
            dma((5,)),
            dma((2 * sp_n,)),
            dma((2 * sp_n,)),
            dma((sp_n,)),
            dma((sp_n,)),
            dma((3 * n_items,)),
            dma((4 * n_items,)),
            dma(((f_n - 1) * 4 * n_items,)),
            dma((f_n * 4 * n_items,)),
        ],
        compiler_params=params(ident),
        name="spread",
    )(wp_in, wu_in, wo_in, wd_in, x_in)


def line_gather_kernel(n, x_in, out, lsem, ss, rs):
    s = lax.axis_index("sp")
    greet([{"sp": lax.rem(s + j, n)} for j in range(1, n)])
    up_ok, down_ok = s + 1 < n, s > 0

    def desc(slot, way, peer, first):
        return pltpu.make_async_remote_copy(
            src_ref=x_in if first else out.at[slot],
            dst_ref=out.at[slot],
            send_sem=ss.at[way * n + slot],
            recv_sem=rs.at[slot],
            device_id={"sp": peer},
            device_id_type=MESH_ID,
        )

    local = pltpu.make_async_copy(x_in, out.at[s], lsem)
    for k in range(n - 1):

        @pl.when((s - k >= 0) & up_ok)
        def _():
            desc(s - k, 0, s + 1, k == 0).start()

        @pl.when((s + k < n) & down_ok)
        def _():
            desc(s + k, 1, s - 1, k == 0).start()

        if k == 0:
            local.start()

        @pl.when(s - 1 - k >= 0)
        def _():
            desc(s - 1 - k, 0, s - 1, False).wait_recv()

        @pl.when(s + 1 + k < n)
        def _():
            desc(s + 1 + k, 1, s + 1, False).wait_recv()

    for k in range(n - 1):

        @pl.when((s - k >= 0) & up_ok)
        def _():
            desc(s - k, 0, s + 1, k == 0).wait_send()

        @pl.when((s + k < n) & down_ok)
        def _():
            desc(s + k, 1, s - 1, k == 0).wait_send()

    local.wait()


def line_gather(x, n, ident):
    dma = pltpu.SemaphoreType.DMA
    out = pl.pallas_call(
        functools.partial(line_gather_kernel, n),
        out_shape=jax.ShapeDtypeStruct((n,) + x.shape, x.dtype),
        in_specs=[VM],
        out_specs=VM,
        scratch_shapes=[dma, dma((2 * n,)), dma((n,))],
        compiler_params=params(ident),
        name="line_gather",
    )(x)
    return out.reshape((n * x.shape[0],) + x.shape[1:])


def line_swap_kernel(n, x_in, out, lsem, ss, rs):
    s = lax.axis_index("sp")
    peers = [lax.rem(s + j, n) for j in range(1, n)]
    greet([{"sp": p} for p in peers])
    waits = [
        push(x_in.at[p], out.at[s], ss.at[j], rs.at[s], {"sp": p}) for j, p in enumerate(peers)
    ]
    local = pltpu.make_async_copy(x_in.at[s], out.at[s], lsem)
    local.start()
    for p in peers:
        arrived(out.at[p], ss.at[0], rs.at[p], {"sp": p})
    for copy in waits:
        copy.wait_send()
    local.wait()


def line_swap(x, n, ident):
    dma = pltpu.SemaphoreType.DMA
    return pl.pallas_call(
        functools.partial(line_swap_kernel, n),
        out_shape=jax.ShapeDtypeStruct(x.shape, x.dtype),
        in_specs=[VM],
        out_specs=VM,
        scratch_shapes=[dma, dma((n,)), dma((n,))],
        compiler_params=params(ident),
        name="line_swap",
    )(x)


def block_gather_kernel(n_items, x_in, out, lsem, ss, rs):
    c = lax.axis_index("ctx")
    low, high, both = beside(c)
    greet([{"ctx": low}, {"ctx": high}])
    waits = []
    for i in range(n_items):
        for n, p in enumerate((low, high)):
            waits.append(
                push(x_in.at[i], out.at[c, i], ss.at[3 * i + n], rs.at[c * n_items + i], {"ctx": p})
            )
    local = pltpu.make_async_copy(x_in, out.at[c], lsem)
    local.start()
    for i in range(n_items):
        for n, (came, goes) in enumerate(((low, high), (high, low))):
            arrived(out.at[came, i], ss.at[0], rs.at[came * n_items + i], {"ctx": came})
            if i % 2 == n:
                waits.append(
                    push(out.at[came, i], out.at[came, i], ss.at[3 * i + 2], rs.at[came * n_items + i], {"ctx": goes})
                )
    for i in range(n_items):
        arrived(out.at[both, i], ss.at[0], rs.at[both * n_items + i], {"ctx": both})
    for copy in waits:
        copy.wait_send()
    local.wait()


def block_gather(x, ident):
    n_items = x.shape[0]
    dma = pltpu.SemaphoreType.DMA
    return pl.pallas_call(
        functools.partial(block_gather_kernel, n_items),
        out_shape=jax.ShapeDtypeStruct((4,) + x.shape, x.dtype),
        in_specs=[VM],
        out_specs=VM,
        scratch_shapes=[dma, dma((3 * n_items,)), dma((4 * n_items,))],
        compiler_params=params(ident),
        name="block_gather",
    )(x)


def all_swap_kernel(sp_n, f_n, x_in, out, lsem, ss, rs):
    s, c, f = lax.axis_index("sp"), lax.axis_index("ctx"), lax.axis_index("fsdp")
    here = (s * 4 + c) * f_n + f
    peers = []
    for a in range(sp_n):
        for b in range(4):
            for d in range(f_n):
                if a or b or d:
                    peers.append((lax.rem(s + a, sp_n), lax.rem(c + b, 4), lax.rem(f + d, f_n)))
    ids = [{"sp": p, "ctx": q, "fsdp": r} for p, q, r in peers]
    flat = [(p * 4 + q) * f_n + r for p, q, r in peers]
    greet(ids)
    waits = [
        push(x_in.at[k], out.at[here], ss.at[n], rs.at[here], p)
        for n, (k, p) in enumerate(zip(flat, ids))
    ]
    local = pltpu.make_async_copy(x_in.at[here], out.at[here], lsem)
    local.start()
    for k, p in zip(flat, ids):
        arrived(out.at[k], ss.at[0], rs.at[k], p)
    for copy in waits:
        copy.wait_send()
    local.wait()


def all_swap(x, sp_n, f_n, ident):
    dma = pltpu.SemaphoreType.DMA
    n = x.shape[0]
    return pl.pallas_call(
        functools.partial(all_swap_kernel, sp_n, f_n),
        out_shape=jax.ShapeDtypeStruct(x.shape, x.dtype),
        in_specs=[VM],
        out_specs=VM,
        scratch_shapes=[dma, dma((n,)), dma((n,))],
        compiler_params=params(ident),
        name="all_swap",
    )(x)


def shards(
    block_input,
    cotangent,
    decay_rate,
    weight_in,
    weight_out,
    norm_gains,
    moment_in,
    square_in,
    moment_out,
    square_out,
    moment_norm,
    square_norm,
):
    tok_count = block_input.shape[2]
    width = block_input.shape[3]
    sp_n = lax.axis_size("sp")
    ctx_n, f_n = lax.axis_size("ctx"), lax.axis_size("fsdp")
    plane_n = ctx_n * f_n
    heads = H // sp_n
    block_len = tok_count * sp_n
    sp_i = lax.axis_index("sp")
    ctx_i = lax.axis_index("ctx")
    rows_in = weight_in.shape[0]
    qk_w, vd_w = QK // sp_n, VD // sp_n
    widths = (qk_w, qk_w, vd_w, vd_w, vd_w)
    starts = (0, QK, 2 * QK, 2 * QK + VD, 2 * QK + 2 * VD)
    cut = 2 * qk_w + 2 * vd_w

    def perm(v):
        return v.reshape(-1, sp_n, plane_n, rows_in).swapaxes(1, 2).reshape(v.shape)

    def unperm(v):
        return v.reshape(-1, plane_n, sp_n, rows_in).swapaxes(1, 2).reshape(v.shape)

    w_low = weight_in.astype(BF)
    slabs = jnp.concatenate(
        [w_low[:, o : o + sp_n * w].reshape(rows_in, sp_n, w) for o, w in zip(starts, widths)], 2
    )
    slabs = slabs.swapaxes(0, 1)
    o_low = weight_out.astype(BF)
    own_x = block_input.reshape(tok_count, width)
    own_xp = perm(own_x)
    w_proj, w_up, w_o, w_down, full_x = spread(
        slabs[:, :, :cut], slabs[:, :, cut:], o_low[:, :width], o_low[:, width:], own_xp, sp_n, f_n, 0
    )
    w_proj, w_up = w_proj.reshape(width, -1), w_up.reshape(width, -1)
    w_o, w_down = w_o.reshape(-1, width), w_down.reshape(-1, width)
    full_x = full_x.reshape(-1, width).astype(F32)
    n_dev = sp_n * plane_n
    gain_part = norm_gains.astype(BF).reshape(1, 4, -1)
    gain_part = jnp.broadcast_to(gain_part, (n_dev, 4, norm_gains.shape[1]))
    gains = all_swap(gain_part, sp_n, f_n, 1).swapaxes(0, 1).reshape(4, width).astype(F32)
    gains_p = perm(gains)

    grad_ffn_own = cotangent.reshape(tok_count, width)
    held_cot, full_x = lax.optimization_barrier((grad_ffn_own, full_x))
    grad_ffn = lax.all_gather(held_cot, "sp", axis=0, tiled=True)
    normed_a, _, _ = layer_stats(full_x, gains_p[0], gains_p[1])
    a_low = normed_a.astype(BF)
    proj = mm(a_low, w_proj)
    head_pos = ctx_i * block_len + jnp.arange(block_len, dtype=jnp.int32)
    cos_h, sin_h = angles(head_pos, DK)

    def split_heads(v, size):
        return v.reshape(block_len, heads, size).swapaxes(0, 1)

    def join_heads(v):
        return v.swapaxes(0, 1).reshape(block_len, -1)

    qs = rotate(split_heads(proj[:, :qk_w], DK), cos_h, sin_h, 1.0).astype(BF)
    ks = rotate(split_heads(proj[:, qk_w : 2 * qk_w], DK), cos_h, sin_h, 1.0).astype(BF)
    vs = split_heads(proj[:, 2 * qk_w : 2 * qk_w + vd_w], DV).astype(BF)
    gate = split_heads(proj[:, 2 * qk_w + vd_w :], DV)

    rates = lax.dynamic_slice_in_dim(decay_rate, sp_i * heads, heads)
    offs = jnp.arange(block_len, dtype=F32)
    spacing = offs[:, None] - offs[None, :]
    mask = jnp.where(
        spacing[None] >= 0.0, jnp.exp(-rates[:, None, None] * jnp.maximum(spacing, 0.0)[None]), 0.0
    )
    inward = jnp.exp(-rates[:, None] * (offs[None, :] + 1.0))[:, :, None]
    outward = jnp.exp(-rates[:, None] * (block_len - 1.0 - offs[None, :]))[:, :, None]
    blocks = jnp.arange(ctx_n)
    back_gap = (ctx_i - 1 - blocks).astype(F32)
    back_w = jnp.where(
        blocks[:, None] < ctx_i,
        jnp.exp(-rates[None, :] * block_len * jnp.maximum(back_gap, 0.0)[:, None]),
        0.0,
    )
    fore_gap = (blocks - ctx_i - 1).astype(F32)
    fore_w = jnp.where(
        blocks[:, None] > ctx_i,
        jnp.exp(-rates[None, :] * block_len * jnp.maximum(fore_gap, 0.0)[:, None]),
        0.0,
    )

    key_decayed = (ks * outward).astype(BF)
    own_state = ein("hjk,hjv->hkv", key_decayed, vs)
    states = block_gather(own_state.astype(BF), 2).astype(F32)
    state = jnp.sum(states * back_w[:, :, None, None], 0).astype(BF)
    scores = ein("hik,hjk->hij", qs, ks)
    probs = (scores * mask).astype(BF)
    mixed = (ein("hij,hjv->hiv", probs, vs) + ein("hik,hkv->hiv", qs, state) * inward).astype(BF)
    mixed_vals = mixed.astype(F32)
    centred = mixed_vals - jnp.mean(mixed_vals, axis=-1, keepdims=True)
    group_scale = lax.rsqrt(jnp.mean(centred * centred, axis=-1, keepdims=True) + norm_eps)
    unit_h = centred * group_scale
    gate_sig = jax.nn.sigmoid(gate)
    gate_act = gate * gate_sig
    gated = join_heads((gate_act * unit_h).astype(BF))

    def line_sum(v, ident, fine):
        v = v.reshape(sp_n, tok_count, width)
        main = lax.reduce_precision(v, 8, 7)
        parts = [main]
        if fine:
            parts.append(v[:, :fine] - main[:, :fine])
        got = line_swap(jnp.concatenate(parts, 1).astype(BF), sp_n, ident)
        total = jnp.sum(got.astype(F32), 0)
        if fine:
            rest = total[tok_count:]
            total = jnp.concatenate([total[:fine] + rest, total[fine:tok_count]], 0)
        return total

    branch = line_sum(mm(gated, w_o), 4, 16)
    hidden = own_x.astype(F32) + branch
    normed_b, unit_b, scale_b = layer_stats(hidden, gains[2], gains[3])
    b_low = line_gather(perm(normed_b.astype(BF)), sp_n, 5)
    up = mm(b_low, w_up)
    act_low = jax.nn.gelu(up, approximate=False).astype(BF)
    ffn_part = mm(act_low, w_down).astype(BF)

    grad_top = grad_ffn_own.astype(F32)
    grad_act = mm_t(grad_ffn, w_down)
    density = (
        0.5 * (1.0 + lax.erf(up * root_half)) + up * jnp.exp(-0.5 * up * up) * inv_root_tau
    )
    grad_up = (grad_act * density).astype(BF)
    grad_b = unperm(line_sum(mm_t(grad_up, w_up), 6, 16))
    grad_hidden = grad_top + layer_back(grad_b, unit_b, scale_b, gains[2])
    grad_branch = line_gather(grad_hidden.astype(BF), sp_n, 7)

    ffn_part, grad_branch = lax.optimization_barrier((ffn_part, grad_branch))
    ffn = lax.psum_scatter(ffn_part, "sp", scatter_dimension=0, tiled=True).astype(F32)
    block_out = (hidden + ffn).astype(BF).reshape(block_input.shape)

    def reduce_rows(v):
        return lax.psum_scatter(v.astype(BF), PLANE, scatter_dimension=0, tiled=True)

    sum_down = reduce_rows(mm_tn(act_low, grad_ffn))
    sum_up = reduce_rows(mm_tn(b_low, grad_up))
    sum_o = reduce_rows(mm_tn(gated, grad_branch))

    grad_gated = split_heads(mm_t(grad_branch, w_o), DV)
    grad_gate = (grad_gated * unit_h * gate_sig * (1.0 + gate * (1.0 - gate_sig))).astype(BF)
    grad_unit = grad_gated * gate_act
    grad_mixed = (
        group_scale
        * (
            grad_unit
            - jnp.mean(grad_unit, axis=-1, keepdims=True)
            - unit_h * jnp.mean(grad_unit * unit_h, axis=-1, keepdims=True)
        )
    ).astype(BF)
    grad_read = (grad_mixed * inward).astype(BF)
    own_reach = ein("hik,hiv->hkv", qs, grad_read)
    reaches = block_gather(own_reach.astype(BF), 3).astype(F32)
    reach = jnp.sum(reaches * fore_w[:, :, None, None], 0).astype(BF)
    grad_probs = ein("hiv,hjv->hij", grad_mixed, vs)
    grad_scores = (grad_probs * mask).astype(BF)
    grad_q = ein("hij,hjk->hik", grad_scores, ks) + ein("hiv,hkv->hik", grad_read, state)
    grad_k = ein("hij,hik->hjk", grad_scores, qs) + ein("hjv,hkv->hjk", vs, reach) * outward
    grad_v = ein("hij,hiv->hjv", probs, grad_mixed) + ein("hjk,hkv->hjv", key_decayed, reach)
    grad_proj = jnp.concatenate(
        [
            join_heads(rotate(grad_q, cos_h, sin_h, -1.0).astype(BF)),
            join_heads(rotate(grad_k, cos_h, sin_h, -1.0).astype(BF)),
            join_heads(grad_v.astype(BF)),
            join_heads(grad_gate),
        ],
        1,
    )
    grad_a = unperm(line_sum(mm_t(grad_proj, w_proj), 8, 0))
    sum_proj = reduce_rows(mm_tn(a_low, grad_proj))
    _, unit_a, scale_a = layer_stats(own_x.astype(F32), gains[0], gains[1])
    grad_rows = grad_hidden + layer_back(grad_a, unit_a, scale_a, gains[0])
    grad_x = grad_rows.astype(BF).reshape(block_input.shape)
    norm_terms = jnp.stack(
        [
            jnp.sum(grad_a * unit_a, 0),
            jnp.sum(grad_a, 0),
            jnp.sum(grad_b * unit_b, 0),
            jnp.sum(grad_b, 0),
        ]
    )
    norm_parts = norm_terms.reshape(4, n_dev, -1).swapaxes(0, 1)
    grad_gains = jnp.sum(all_swap(norm_parts, sp_n, f_n, 9), 0)

    def home(v):
        v = v.reshape(sp_n, rows_in, -1)
        return lax.all_to_all(v, "sp", split_axis=0, concat_axis=0, tiled=True)

    back_proj = home(sum_proj)
    back_up = home(sum_up)
    edges = (0, qk_w, 2 * qk_w, 2 * qk_w + vd_w, cut)
    parts = [back_proj[:, :, a:b] for a, b in zip(edges[:-1], edges[1:])] + [back_up]
    grad_first = jnp.concatenate(
        [p.swapaxes(0, 1).reshape(rows_in, -1) for p in parts], 1
    ).astype(F32)
    grad_second = jnp.concatenate([sum_o, sum_down], 1).astype(F32)
    first_m, first_v, first_step = adam_update(weight_in, grad_first, moment_in, square_in)
    second_m, second_v, second_step = adam_update(weight_out, grad_second, moment_out, square_out)
    gain_m, gain_v, gain_step = adam_update(norm_gains, grad_gains, moment_norm, square_norm)
    return (
        block_out,
        grad_x,
        grad_first,
        first_m,
        first_v,
        first_step,
        grad_second,
        second_m,
        second_v,
        second_step,
        grad_gains,
        gain_m,
        gain_v,
        gain_step,
    )


def solution(mesh):
    tokens = P("fsdp", "ctx", "sp", None)
    rows = P(ALL, None)
    cols = P(None, ALL)
    in_specs = (tokens, tokens, P(), rows, rows, cols, rows, rows, rows, rows, cols, cols)
    out_specs = (tokens, tokens) + (rows,) * 8 + (cols,) * 4
    return jax.shard_map(shards, mesh=mesh, in_specs=in_specs, out_specs=out_specs, check_vma=False)
```

```python
import functools
import math

import jax
import jax.numpy as jnp
from jax import lax
from jax.experimental import pallas as pl
from jax.experimental.pallas import tpu as pltpu
from jax.sharding import PartitionSpec as P

H = 8
DK = 256
DV = 512
SPAN = 512
STEP = 10
QK = 2048
VD = 4096

beta_one = 0.9
beta_two = 0.95
learn_rate = 0.01
decay_weight = 0.1
adam_eps = 1e-08
norm_eps = 1e-05
root_half = 0.7071067811865476
inv_root_tau = 0.3989422804014327


BF = jnp.bfloat16
F32 = jnp.float32
ALL = ("sp", "ctx", "fsdp")
PLANE = ("ctx", "fsdp")


def layer_stats(values, gain_row, shift_row):
    centred = values - jnp.mean(values, axis=-1, keepdims=True)
    inv_std = lax.rsqrt(jnp.mean(centred * centred, axis=-1, keepdims=True) + norm_eps)
    unit_vals = centred * inv_std
    return (unit_vals * gain_row + shift_row, unit_vals, inv_std)


def layer_back(grad_vals, unit_vals, inv_std, gain_row):
    scaled = grad_vals * gain_row
    return inv_std * (
        scaled
        - jnp.mean(scaled, axis=-1, keepdims=True)
        - unit_vals * jnp.mean(scaled * unit_vals, axis=-1, keepdims=True)
    )


def angles(positions, head_size):
    half_size = head_size // 2
    inverse = jnp.exp(
        -math.log(10000.0) * (2.0 * jnp.arange(half_size, dtype=jnp.float32) / head_size)
    )
    phases = positions.astype(jnp.float32)[:, None] * inverse[None, :]
    return (jnp.cos(phases), jnp.sin(phases))


def rotate(values, cosine, sine, sign_flip):
    half_size = values.shape[-1] // 2
    first_half = values[..., :half_size]
    second_half = values[..., half_size:]
    return jnp.concatenate(
        [
            first_half * cosine - sign_flip * (second_half * sine),
            second_half * cosine + sign_flip * (first_half * sine),
        ],
        -1,
    )


def adam_update(weight, grad_vals, moment, square):
    moment_new = beta_one * moment + (1.0 - beta_one) * grad_vals
    square_new = beta_two * square + (1.0 - beta_two) * grad_vals * grad_vals
    moment_hat = moment_new / (1.0 - beta_one**STEP)
    square_hat = square_new / (1.0 - beta_two**STEP)
    step_vals = -learn_rate * (
        moment_hat / (jnp.sqrt(square_hat) + adam_eps) + decay_weight * weight
    )
    return (moment_new, square_new, step_vals)


def mm(a, b):
    return jnp.dot(a, b, preferred_element_type=F32)


def mm_t(a, b):
    return lax.dot_general(a, b, (((1,), (1,)), ((), ())), preferred_element_type=F32)


def mm_tn(a, b):
    return lax.dot_general(a, b, (((0,), (0,)), ((), ())), preferred_element_type=F32)


def ein(spec, a, b):
    return jnp.einsum(spec, a, b, preferred_element_type=F32)


MESH_ID = pl.DeviceIdType.MESH
ANY = pl.BlockSpec(memory_space=pl.ANY)
VM = pl.BlockSpec(memory_space=pltpu.VMEM)


def greet(peers):
    sem = pltpu.get_barrier_semaphore()
    for peer in peers:
        pl.semaphore_signal(sem, inc=1, device_id=peer, device_id_type=MESH_ID)
    pl.semaphore_wait(sem, len(peers))


def push(src, dst, send, recv, peer):
    copy = pltpu.make_async_remote_copy(
        src_ref=src, dst_ref=dst, send_sem=send, recv_sem=recv, device_id=peer, device_id_type=MESH_ID
    )
    copy.start()
    return copy


def arrived(dst, send, recv, peer):
    pltpu.make_async_remote_copy(
        src_ref=dst, dst_ref=dst, send_sem=send, recv_sem=recv, device_id=peer, device_id_type=MESH_ID
    ).wait_recv()


def beside(c):
    low = c + 1 - 2 * (c % 2)
    high = (c + 2) % 4
    return low, high, (low + 2) % 4


def cost(micros):
    return pl.CostEstimate(flops=0, transcendentals=0, bytes_accessed=int(micros * 3.0e6))


def params(ident):
    return pltpu.CompilerParams(collective_id=ident, has_side_effects=True)


def others(s, c, f, sp_n, f_n):
    ids, flat = [], []
    for a in range(sp_n):
        for b in range(4):
            for d in range(f_n):
                if a or b or d:
                    p, q, r = lax.rem(s + a, sp_n), lax.rem(c + b, 4), lax.rem(f + d, f_n)
                    ids.append({"sp": p, "ctx": q, "fsdp": r})
                    flat.append((p * 4 + q) * f_n + r)
    return ids, flat


def spread_kernel(sp_n, f_n, wp_in, wu_in, wo_in, wd_in, x_in, g_in, wp, wu, wo, wd, x, g, gs, gr, lsem, zs, zr, xs, xr, ps, pr, cs, cr):
    s, c, f = lax.axis_index("sp"), lax.axis_index("ctx"), lax.axis_index("fsdp")
    low, high, both = beside(c)
    lines = [lax.rem(s + j, sp_n) for j in range(sp_n)]
    cores = [lax.rem(f + k, f_n) for k in range(1, f_n)]
    here = (s * 4 + c) * f_n + f
    ids, flat = others(s, c, f, sp_n, f_n)
    greet(ids)
    n_items = 2 * sp_n + 2
    waits = []

    def item_at(i, cc, ff):
        if i < 2:
            return (wo, wd)[i].at[cc, ff]
        j, a = (i - 2) // 2, (i - 2) % 2
        return (wp, wu)[a].at[cc, ff, lines[j]]

    def key(i):
        if i < 2:
            return i
        j, a = (i - 2) // 2, (i - 2) % 2
        return 2 + a * sp_n + lines[j]

    def own(i):
        if i < 2:
            return (wo_in, wd_in)[i]
        a = (i - 2) % 2
        return (wp_in, wu_in)[a].at[s]

    def start_local(n, src, dst):
        copy = pltpu.make_async_copy(src, dst, lsem.at[n])
        copy.start()
        return copy

    for n, p in enumerate(ids):
        waits.append(push(g_in, g.at[here], gs.at[n], gr.at[here], p))
    for j in range(1, sp_n):
        for a in range(2):
            src, dst = ((wp_in, wp), (wu_in, wu))[a]
            waits.append(
                push(src.at[lines[j]], dst.at[c, f, s], zs.at[a * sp_n + j], zr.at[a * sp_n + s], {"sp": lines[j]})
            )
    for j in range(1, sp_n):
        waits.append(push(x_in, x.at[s], xs.at[j], xr.at[s], {"sp": lines[j]}))
    local = [start_local(i, own(i), item_at(i, c, f)) for i in range(4)]
    local.append(start_local(4, x_in, x.at[s]))
    local.append(start_local(5, g_in, g.at[here]))

    def to_cores(i, src, cc):
        for n, p in enumerate(cores):
            waits.append(
                push(
                    src,
                    item_at(i, cc, f),
                    cs.at[(n * 4 + cc) * n_items + i],
                    cr.at[(f * 4 + cc) * n_items + key(i)],
                    {"fsdp": p},
                )
            )

    def first(i):
        if i < 4:
            src = own(i)
        else:
            j, a = (i - 2) // 2, (i - 2) % 2
            arrived(item_at(i, c, f), zs.at[0], zr.at[a * sp_n + lines[j]], {"sp": lines[j]})
            src = item_at(i, c, f)
        for n, p in enumerate((low, high)):
            waits.append(
                push(src, item_at(i, c, f), ps.at[3 * i + n], pr.at[c * n_items + key(i)], {"ctx": p})
            )
        to_cores(i, src, c)

    def landed(i, cc):
        arrived(item_at(i, cc, f), ps.at[0], pr.at[cc * n_items + key(i)], {"ctx": cc})

    def second(i):
        landed(i, low)
        if i % 4 in (1, 2):
            waits.append(
                push(item_at(i, low, f), item_at(i, low, f), ps.at[3 * i + 2], pr.at[low * n_items + key(i)], {"ctx": high})
            )
        to_cores(i, item_at(i, low, f), low)
        landed(i, high)
        if i % 4 in (0, 3):
            waits.append(
                push(item_at(i, high, f), item_at(i, high, f), ps.at[3 * i + 2], pr.at[high * n_items + key(i)], {"ctx": low})
            )
        to_cores(i, item_at(i, high, f), high)

    def third(i):
        landed(i, both)
        to_cores(i, item_at(i, both, f), both)

    for i in range(n_items + 4):
        if i < n_items:
            first(i)
        if 2 <= i < n_items + 2:
            second(i - 2)
        if i >= 4:
            third(i - 4)
    for j in range(1, sp_n):
        arrived(x.at[lines[j]], xs.at[0], xr.at[lines[j]], {"sp": lines[j]})
    for p in cores:
        for cc in range(4):
            for i in range(n_items):
                arrived(item_at(i, cc, p), cs.at[0], cr.at[(p * 4 + cc) * n_items + key(i)], {"fsdp": p})
    for k, p in zip(flat, ids):
        arrived(g.at[k], gs.at[0], gr.at[k], p)
    for copy in waits:
        copy.wait_send()
    for copy in local:
        copy.wait()


def spread(wp_in, wu_in, wo_in, wd_in, x_in, g_in, sp_n, f_n, ident):
    rows = wp_in.shape[1]
    n_items = 2 * sp_n + 2
    shapes = [
        (4, f_n, sp_n, rows, wp_in.shape[2]),
        (4, f_n, sp_n, rows, wu_in.shape[2]),
        (4, f_n) + wo_in.shape,
        (4, f_n) + wd_in.shape,
        (sp_n,) + x_in.shape,
        (sp_n * 4 * f_n,) + g_in.shape,
    ]
    dma = pltpu.SemaphoreType.DMA
    return pl.pallas_call(
        functools.partial(spread_kernel, sp_n, f_n),
        out_shape=[jax.ShapeDtypeStruct(v, BF) for v in shapes],
        in_specs=[VM] * 6,
        out_specs=[ANY] * 6,
        scratch_shapes=[
            dma((sp_n * 4 * f_n,)),
            dma((sp_n * 4 * f_n,)),
            dma((6,)),
            dma((2 * sp_n,)),
            dma((2 * sp_n,)),
            dma((sp_n,)),
            dma((sp_n,)),
            dma((3 * n_items,)),
            dma((4 * n_items,)),
            dma(((f_n - 1) * 4 * n_items,)),
            dma((f_n * 4 * n_items,)),
        ],
        compiler_params=params(ident),
        cost_estimate=cost(110),
        name="spread",
    )(wp_in, wu_in, wo_in, wd_in, x_in, g_in)


def line_gather_kernel(n, x_in, out, lsem, ss, rs):
    s = lax.axis_index("sp")
    greet([{"sp": lax.rem(s + j, n)} for j in range(1, n)])
    up_ok, down_ok = s + 1 < n, s > 0

    def desc(slot, way, peer, first):
        return pltpu.make_async_remote_copy(
            src_ref=x_in if first else out.at[slot],
            dst_ref=out.at[slot],
            send_sem=ss.at[way * n + slot],
            recv_sem=rs.at[slot],
            device_id={"sp": peer},
            device_id_type=MESH_ID,
        )

    local = pltpu.make_async_copy(x_in, out.at[s], lsem)
    for k in range(n - 1):

        @pl.when((s - k >= 0) & up_ok)
        def _():
            desc(s - k, 0, s + 1, k == 0).start()

        @pl.when((s + k < n) & down_ok)
        def _():
            desc(s + k, 1, s - 1, k == 0).start()

        if k == 0:
            local.start()

        @pl.when(s - 1 - k >= 0)
        def _():
            desc(s - 1 - k, 0, s - 1, False).wait_recv()

        @pl.when(s + 1 + k < n)
        def _():
            desc(s + 1 + k, 1, s + 1, False).wait_recv()

    for k in range(n - 1):

        @pl.when((s - k >= 0) & up_ok)
        def _():
            desc(s - k, 0, s + 1, k == 0).wait_send()

        @pl.when((s + k < n) & down_ok)
        def _():
            desc(s + k, 1, s - 1, k == 0).wait_send()

    local.wait()


def line_gather(x, n, ident):
    dma = pltpu.SemaphoreType.DMA
    out = pl.pallas_call(
        functools.partial(line_gather_kernel, n),
        out_shape=jax.ShapeDtypeStruct((n,) + x.shape, x.dtype),
        in_specs=[VM],
        out_specs=VM,
        scratch_shapes=[dma, dma((2 * n,)), dma((n,))],
        compiler_params=params(ident),
        cost_estimate=cost(40),
        name="line_gather",
    )(x)
    return out.reshape((n * x.shape[0],) + x.shape[1:])


def line_swap_kernel(n, m, *refs):
    ins, outs, (lsem, ss, rs) = refs[:m], refs[m : 2 * m], refs[2 * m :]
    s = lax.axis_index("sp")
    peers = [lax.rem(s + j, n) for j in range(1, n)]
    greet([{"sp": p} for p in peers])
    waits, local = [], []
    for k in range(m):
        for j, p in enumerate(peers):
            waits.append(
                push(ins[k].at[p], outs[k].at[s], ss.at[k * n + j], rs.at[k * n + s], {"sp": p})
            )
        copy = pltpu.make_async_copy(ins[k].at[s], outs[k].at[s], lsem.at[k])
        copy.start()
        local.append(copy)
    for k in range(m):
        for p in peers:
            arrived(outs[k].at[p], ss.at[0], rs.at[k * n + p], {"sp": p})
    for copy in waits:
        copy.wait_send()
    for copy in local:
        copy.wait()


def line_swap(xs, n, ident, micros):
    dma = pltpu.SemaphoreType.DMA
    m = len(xs)
    return pl.pallas_call(
        functools.partial(line_swap_kernel, n, m),
        out_shape=[jax.ShapeDtypeStruct(x.shape, x.dtype) for x in xs],
        in_specs=[VM] * m,
        out_specs=[VM] * m,
        scratch_shapes=[dma((m,)), dma((m * n,)), dma((m * n,))],
        compiler_params=params(ident),
        cost_estimate=cost(micros),
        name="line_swap",
    )(*xs)


def block_gather_kernel(n_items, x_in, out, lsem, ss, rs):
    c = lax.axis_index("ctx")
    low, high, both = beside(c)
    greet([{"ctx": low}, {"ctx": high}])
    waits = []
    for i in range(n_items):
        for n, p in enumerate((low, high)):
            waits.append(
                push(x_in.at[i], out.at[c, i], ss.at[3 * i + n], rs.at[c * n_items + i], {"ctx": p})
            )
    local = pltpu.make_async_copy(x_in, out.at[c], lsem)
    local.start()
    for i in range(n_items):
        for n, (came, goes) in enumerate(((low, high), (high, low))):
            arrived(out.at[came, i], ss.at[0], rs.at[came * n_items + i], {"ctx": came})
            if i % 2 == n:
                waits.append(
                    push(out.at[came, i], out.at[came, i], ss.at[3 * i + 2], rs.at[came * n_items + i], {"ctx": goes})
                )
    for i in range(n_items):
        arrived(out.at[both, i], ss.at[0], rs.at[both * n_items + i], {"ctx": both})
    for copy in waits:
        copy.wait_send()
    local.wait()


def block_gather(x, ident):
    n_items = x.shape[0]
    dma = pltpu.SemaphoreType.DMA
    return pl.pallas_call(
        functools.partial(block_gather_kernel, n_items),
        out_shape=jax.ShapeDtypeStruct((4,) + x.shape, x.dtype),
        in_specs=[VM],
        out_specs=VM,
        scratch_shapes=[dma, dma((3 * n_items,)), dma((4 * n_items,))],
        compiler_params=params(ident),
        cost_estimate=cost(22),
        name="block_gather",
    )(x)


def all_swap_kernel(sp_n, f_n, x_in, out, lsem, ss, rs):
    s, c, f = lax.axis_index("sp"), lax.axis_index("ctx"), lax.axis_index("fsdp")
    here = (s * 4 + c) * f_n + f
    ids, flat = others(s, c, f, sp_n, f_n)
    greet(ids)
    waits = [
        push(x_in.at[k], out.at[here], ss.at[n], rs.at[here], p)
        for n, (k, p) in enumerate(zip(flat, ids))
    ]
    local = pltpu.make_async_copy(x_in.at[here], out.at[here], lsem)
    local.start()
    for k, p in zip(flat, ids):
        arrived(out.at[k], ss.at[0], rs.at[k], p)
    for copy in waits:
        copy.wait_send()
    local.wait()


def all_swap(x, sp_n, f_n, ident):
    dma = pltpu.SemaphoreType.DMA
    n = x.shape[0]
    return pl.pallas_call(
        functools.partial(all_swap_kernel, sp_n, f_n),
        out_shape=jax.ShapeDtypeStruct(x.shape, x.dtype),
        in_specs=[VM],
        out_specs=VM,
        scratch_shapes=[dma, dma((n,)), dma((n,))],
        compiler_params=params(ident),
        cost_estimate=cost(10),
        name="all_swap",
    )(x)


def regroup(v, back):
    lane = lax.broadcasted_iota(jnp.int32, (v.shape[0], 128), 1) < 64
    piece = lambda k: v[:, 128 * k : 128 * k + 128]
    turn = lambda p: pltpu.roll(p, 64, 1)
    out = []
    for k in range(v.shape[1] // 128):
        if back:
            s, pair = k // 4, k % 4
            a, b, odd = 4 * pair + s // 2, 4 * pair + 2 + s // 2, s % 2
        else:
            cf, half = k // 2, k % 2
            a, b, odd = 8 * half + cf // 2, 8 * half + 4 + cf // 2, cf % 2
        if odd:
            out.append(jnp.where(lane, turn(piece(a)), piece(b)))
        else:
            out.append(jnp.where(lane, piece(a), turn(piece(b))))
    return jnp.concatenate(out, 1)


def added(main, lo):
    total = main[0].astype(F32)
    for k in range(1, main.shape[0]):
        total = total + main[k].astype(F32)
    if lo is not None:
        rest = lo[0].astype(F32)
        for k in range(1, lo.shape[0]):
            rest = rest + lo[k].astype(F32)
        total = total + jnp.where(pl.program_id(0) == 0, 1.0, 0.0) * rest
    return total


def tally(sums, grads, unit):
    @pl.when(pl.program_id(0) == 0)
    def _():
        sums[...] = jnp.zeros_like(sums)

    sums[0:1, :] += jnp.sum(grads * unit, 0, keepdims=True)
    sums[1:2, :] += jnp.sum(grads, 0, keepdims=True)


def ahead_kernel(group, main, lo, x, gains, hidden_out, bn_out):
    hidden = x[...].astype(F32) + added(main, lo)
    hidden_out[...] = hidden
    normed, _, _ = layer_stats(hidden, gains[2:3, :], gains[3:4, :])
    bn_out[...] = (regroup(normed, False) if group else normed).astype(BF)


def turn_kernel(group, main, lo, hidden, cot, gains, dh_out, dbr_out, sums):
    grads = added(main, lo)
    grads = regroup(grads, True) if group else grads
    _, unit, scale = layer_stats(hidden[...], gains[2:3, :], gains[3:4, :])
    dh = cot[...].astype(F32) + layer_back(grads, unit, scale, gains[2:3, :])
    dh_out[...] = dh
    dbr_out[...] = dh.astype(BF)
    tally(sums, grads, unit)


def last_kernel(group, main, x, dh, gains, gx_out, sums):
    grads = added(main, None)
    grads = regroup(grads, True) if group else grads
    _, unit, scale = layer_stats(x[...].astype(F32), gains[0:1, :], gains[1:2, :])
    gx_out[...] = (dh[...] + layer_back(grads, unit, scale, gains[0:1, :])).astype(BF)
    tally(sums, grads, unit)


def row_call(kernel, name, args, kinds, outs, rows, width, tile=16):
    n = args[0].shape[0]
    specs = {
        "main": pl.BlockSpec((n, tile, width), lambda i: (0, i, 0)),
        "lo": pl.BlockSpec((n, tile, width), lambda i: (0, rows // tile, 0)),
        "row": pl.BlockSpec((tile, width), lambda i: (i, 0)),
        "gains": pl.BlockSpec((4, width), lambda i: (0, 0)),
        "sums": pl.BlockSpec((8, width), lambda i: (0, 0)),
    }
    return pl.pallas_call(
        kernel,
        grid=(rows // tile,),
        in_specs=[specs[k] for k in kinds],
        out_specs=[specs["sums" if h == 8 else "row"] for h, _ in outs],
        out_shape=[jax.ShapeDtypeStruct((h, width), t) for h, t in outs],
        cost_estimate=cost(4),
        name=name,
    )(*args)


def shards(
    block_input,
    cotangent,
    decay_rate,
    weight_in,
    weight_out,
    norm_gains,
    moment_in,
    square_in,
    moment_out,
    square_out,
    moment_norm,
    square_norm,
):
    tok_count = block_input.shape[2]
    width = block_input.shape[3]
    sp_n = lax.axis_size("sp")
    ctx_n, f_n = lax.axis_size("ctx"), lax.axis_size("fsdp")
    plane_n = ctx_n * f_n
    heads = H // sp_n
    block_len = tok_count * sp_n
    sp_i = lax.axis_index("sp")
    ctx_i = lax.axis_index("ctx")
    rows_in = weight_in.shape[0]
    qk_w, vd_w = QK // sp_n, VD // sp_n
    widths = (qk_w, qk_w, vd_w, vd_w, vd_w)
    starts = (0, QK, 2 * QK, 2 * QK + VD, 2 * QK + 2 * VD)
    cut = 2 * qk_w + 2 * vd_w

    def perm(v):
        return v.reshape(-1, sp_n, plane_n, rows_in).swapaxes(1, 2).reshape(v.shape)

    def unperm(v):
        return v.reshape(-1, plane_n, sp_n, rows_in).swapaxes(1, 2).reshape(v.shape)

    w_low = weight_in.astype(BF)
    slabs = jnp.concatenate(
        [w_low[:, o : o + sp_n * w].reshape(rows_in, sp_n, w) for o, w in zip(starts, widths)], 2
    )
    slabs = slabs.swapaxes(0, 1)
    o_low = weight_out.astype(BF)
    own_x = block_input.reshape(tok_count, width)
    own_xp = perm(own_x)
    n_dev = sp_n * plane_n
    w_proj, w_up, w_o, w_down, full_x, gains = spread(
        slabs[:, :, :cut],
        slabs[:, :, cut:],
        o_low[:, :width],
        o_low[:, width:],
        own_xp,
        norm_gains.astype(BF),
        sp_n,
        f_n,
        0,
    )
    w_proj, w_up = w_proj.reshape(width, -1), w_up.reshape(width, -1)
    w_o, w_down = w_o.reshape(-1, width), w_down.reshape(-1, width)
    full_x = full_x.reshape(-1, width).astype(F32)
    gains = gains.swapaxes(0, 1).reshape(4, width).astype(F32)
    gains_p = perm(gains)

    grad_ffn_own = cotangent.reshape(tok_count, width)
    held_cot, full_x = lax.optimization_barrier((grad_ffn_own, full_x))
    grad_ffn = lax.all_gather(held_cot, "sp", axis=0, tiled=True)
    normed_a, _, _ = layer_stats(full_x, gains_p[0], gains_p[1])
    a_low = normed_a.astype(BF)
    proj = mm(a_low, w_proj)
    head_pos = ctx_i * block_len + jnp.arange(block_len, dtype=jnp.int32)
    cos_h, sin_h = angles(head_pos, DK)

    def split_heads(v, size):
        return v.reshape(block_len, heads, size).swapaxes(0, 1)

    def join_heads(v):
        return v.swapaxes(0, 1).reshape(block_len, -1)

    qs = rotate(split_heads(proj[:, :qk_w], DK), cos_h, sin_h, 1.0).astype(BF)
    ks = rotate(split_heads(proj[:, qk_w : 2 * qk_w], DK), cos_h, sin_h, 1.0).astype(BF)
    vs = split_heads(proj[:, 2 * qk_w : 2 * qk_w + vd_w], DV).astype(BF)
    gate = split_heads(proj[:, 2 * qk_w + vd_w :], DV)

    rates = lax.dynamic_slice_in_dim(decay_rate, sp_i * heads, heads)
    offs = jnp.arange(block_len, dtype=F32)
    spacing = offs[:, None] - offs[None, :]
    mask = jnp.where(
        spacing[None] >= 0.0, jnp.exp(-rates[:, None, None] * jnp.maximum(spacing, 0.0)[None]), 0.0
    )
    inward = jnp.exp(-rates[:, None] * (offs[None, :] + 1.0))[:, :, None]
    outward = jnp.exp(-rates[:, None] * (block_len - 1.0 - offs[None, :]))[:, :, None]
    blocks = jnp.arange(ctx_n)
    back_gap = (ctx_i - 1 - blocks).astype(F32)
    back_w = jnp.where(
        blocks[:, None] < ctx_i,
        jnp.exp(-rates[None, :] * block_len * jnp.maximum(back_gap, 0.0)[:, None]),
        0.0,
    )
    fore_gap = (blocks - ctx_i - 1).astype(F32)
    fore_w = jnp.where(
        blocks[:, None] > ctx_i,
        jnp.exp(-rates[None, :] * block_len * jnp.maximum(fore_gap, 0.0)[:, None]),
        0.0,
    )

    key_decayed = (ks * outward).astype(BF)
    own_state = ein("hjk,hjv->hkv", key_decayed, vs)
    states = block_gather(own_state.astype(BF), 2).astype(F32)
    state = jnp.sum(states * back_w[:, :, None, None], 0).astype(BF)
    scores = ein("hik,hjk->hij", qs, ks)
    probs = (scores * mask).astype(BF)
    mixed = (ein("hij,hjv->hiv", probs, vs) + ein("hik,hkv->hiv", qs, state) * inward).astype(BF)
    mixed_vals = mixed.astype(F32)
    centred = mixed_vals - jnp.mean(mixed_vals, axis=-1, keepdims=True)
    group_scale = lax.rsqrt(jnp.mean(centred * centred, axis=-1, keepdims=True) + norm_eps)
    unit_h = centred * group_scale
    gate_sig = jax.nn.sigmoid(gate)
    gate_act = gate * gate_sig
    gated = join_heads((gate_act * unit_h).astype(BF))

    group = rows_in == 64 and sp_n == 4 and plane_n == 8
    fine = 16

    def parts_of(v, fine):
        v = v.reshape(sp_n, tok_count, width)
        main = lax.reduce_precision(v, 8, 7)
        rest = [v[:, :fine] - main[:, :fine]] if fine else []
        return jnp.concatenate([main] + rest, 1).astype(BF)

    (got,) = line_swap([parts_of(mm(gated, w_o), fine)], sp_n, 4, 45)
    hidden, normed_b = row_call(
        functools.partial(ahead_kernel, group),
        "ahead",
        (got, got, own_x, gains),
        ("main", "lo", "row", "gains"),
        ((tok_count, F32), (tok_count, BF)),
        tok_count,
        width,
    )
    b_low = line_gather(normed_b if group else perm(normed_b), sp_n, 5)
    up = mm(b_low, w_up)
    act_low = jax.nn.gelu(up, approximate=False).astype(BF)
    ffn_part = mm(act_low, w_down).astype(BF)

    grad_act = mm_t(grad_ffn, w_down)
    density = (
        0.5 * (1.0 + lax.erf(up * root_half)) + up * jnp.exp(-0.5 * up * up) * inv_root_tau
    )
    grad_up = (grad_act * density).astype(BF)

    def reduce_rows(v):
        return lax.psum_scatter(v, PLANE, scatter_dimension=0, tiled=True)

    part_down = mm_tn(act_low, grad_ffn).astype(BF)
    part_up = mm_tn(b_low, grad_up).astype(BF)
    part_b = parts_of(mm_t(grad_up, w_up), fine)
    part_b, part_down, part_up = lax.optimization_barrier((part_b, part_down, part_up))
    sum_down = reduce_rows(part_down)
    sum_up = reduce_rows(part_up)
    (got,) = line_swap([part_b if group else unperm(part_b)], sp_n, 6, 45)
    grad_hidden, grad_branch, sums_b = row_call(
        functools.partial(turn_kernel, group),
        "turn",
        (got, got, hidden, grad_ffn_own, gains),
        ("main", "lo", "row", "row", "gains"),
        ((tok_count, F32), (tok_count, BF), (8, F32)),
        tok_count,
        width,
    )
    grad_branch = line_gather(grad_branch, sp_n, 7)
    ffn_part, grad_branch = lax.optimization_barrier((ffn_part, grad_branch))
    ffn = lax.psum_scatter(ffn_part, "sp", scatter_dimension=0, tiled=True).astype(F32)
    block_out = (hidden + ffn).astype(BF).reshape(block_input.shape)
    part_o = mm_tn(gated, grad_branch).astype(BF)

    grad_gated = split_heads(mm_t(grad_branch, w_o), DV)
    grad_gate = (grad_gated * unit_h * gate_sig * (1.0 + gate * (1.0 - gate_sig))).astype(BF)
    grad_unit = grad_gated * gate_act
    grad_mixed = (
        group_scale
        * (
            grad_unit
            - jnp.mean(grad_unit, axis=-1, keepdims=True)
            - unit_h * jnp.mean(grad_unit * unit_h, axis=-1, keepdims=True)
        )
    ).astype(BF)
    grad_read = (grad_mixed * inward).astype(BF)
    own_reach = ein("hik,hiv->hkv", qs, grad_read).astype(BF)
    grad_gate = join_heads(grad_gate)
    part_gate = mm_tn(a_low, grad_gate).astype(BF)
    own_reach, part_o, part_gate = lax.optimization_barrier((own_reach, part_o, part_gate))
    sum_o = reduce_rows(part_o)
    sum_gate = reduce_rows(part_gate)
    reaches = block_gather(own_reach, 3).astype(F32)
    reach = jnp.sum(reaches * fore_w[:, :, None, None], 0).astype(BF)
    grad_probs = ein("hiv,hjv->hij", grad_mixed, vs)
    grad_scores = (grad_probs * mask).astype(BF)
    grad_q = ein("hij,hjk->hik", grad_scores, ks) + ein("hiv,hkv->hik", grad_read, state)
    grad_k = ein("hij,hik->hjk", grad_scores, qs) + ein("hjv,hkv->hjk", vs, reach) * outward
    grad_v = ein("hij,hiv->hjv", probs, grad_mixed) + ein("hjk,hkv->hjv", key_decayed, reach)
    grad_qkv = jnp.concatenate(
        [
            join_heads(rotate(grad_q, cos_h, sin_h, -1.0).astype(BF)),
            join_heads(rotate(grad_k, cos_h, sin_h, -1.0).astype(BF)),
            join_heads(grad_v.astype(BF)),
        ],
        1,
    )
    part_qkv = mm_tn(a_low, grad_qkv).astype(BF)
    grad_proj = jnp.concatenate([grad_qkv, grad_gate], 1)
    part_a = parts_of(mm_t(grad_proj, w_proj), 0)
    part_a, part_qkv = lax.optimization_barrier((part_a, part_qkv))
    sum_qkv = reduce_rows(part_qkv)

    def home(v):
        return v.reshape(sp_n, rows_in, -1)

    got, back_up, back_gate = line_swap(
        [part_a if group else unperm(part_a), home(sum_up), home(sum_gate)], sp_n, 8, 65
    )
    grad_x, sums_a = row_call(
        functools.partial(last_kernel, group),
        "last",
        (got, own_x, grad_hidden, gains),
        ("main", "row", "row", "gains"),
        ((tok_count, BF), (8, F32)),
        tok_count,
        width,
    )
    grad_x = grad_x.reshape(block_input.shape)
    norm_terms = jnp.concatenate([sums_a[:2], sums_b[:2]], 0)
    norm_parts = norm_terms.reshape(4, n_dev, -1).swapaxes(0, 1)
    grad_gains = jnp.sum(all_swap(norm_parts, sp_n, f_n, 9), 0)
    (back_qkv,) = line_swap([home(sum_qkv)], sp_n, 10, 26)
    edges = (0, qk_w, 2 * qk_w, 2 * qk_w + vd_w)
    parts = [back_qkv[:, :, a:b] for a, b in zip(edges[:-1], edges[1:])] + [back_gate, back_up]
    grad_first = jnp.concatenate(
        [p.swapaxes(0, 1).reshape(rows_in, -1) for p in parts], 1
    ).astype(F32)
    grad_second = jnp.concatenate([sum_o, sum_down], 1).astype(F32)
    first_m, first_v, first_step = adam_update(weight_in, grad_first, moment_in, square_in)
    second_m, second_v, second_step = adam_update(weight_out, grad_second, moment_out, square_out)
    gain_m, gain_v, gain_step = adam_update(norm_gains, grad_gains, moment_norm, square_norm)
    return (
        block_out,
        grad_x,
        grad_first,
        first_m,
        first_v,
        first_step,
        grad_second,
        second_m,
        second_v,
        second_step,
        grad_gains,
        gain_m,
        gain_v,
        gain_step,
    )


def solution(mesh):
    tokens = P("fsdp", "ctx", "sp", None)
    rows = P(ALL, None)
    cols = P(None, ALL)
    in_specs = (tokens, tokens, P(), rows, rows, cols, rows, rows, rows, rows, cols, cols)
    out_specs = (tokens, tokens) + (rows,) * 8 + (cols,) * 4
    return jax.shard_map(shards, mesh=mesh, in_specs=in_specs, out_specs=out_specs, check_vma=False)
```

```python
import functools
import math

import jax
import jax.numpy as jnp
from jax import lax
from jax.experimental import pallas as pl
from jax.experimental.pallas import tpu as pltpu
from jax.sharding import PartitionSpec as P

H = 8
DK = 256
DV = 512
SPAN = 512
STEP = 10
QK = 2048
VD = 4096

beta_one = 0.9
beta_two = 0.95
learn_rate = 0.01
decay_weight = 0.1
adam_eps = 1e-08
norm_eps = 1e-05
root_half = 0.7071067811865476
inv_root_tau = 0.3989422804014327


BF = jnp.bfloat16
F32 = jnp.float32
ALL = ("sp", "ctx", "fsdp")
PLANE = ("ctx", "fsdp")


def layer_stats(values, gain_row, shift_row):
    centred = values - jnp.mean(values, axis=-1, keepdims=True)
    inv_std = lax.rsqrt(jnp.mean(centred * centred, axis=-1, keepdims=True) + norm_eps)
    unit_vals = centred * inv_std
    return (unit_vals * gain_row + shift_row, unit_vals, inv_std)


def layer_back(grad_vals, unit_vals, inv_std, gain_row):
    scaled = grad_vals * gain_row
    return inv_std * (
        scaled
        - jnp.mean(scaled, axis=-1, keepdims=True)
        - unit_vals * jnp.mean(scaled * unit_vals, axis=-1, keepdims=True)
    )


def angles(positions, head_size):
    half_size = head_size // 2
    inverse = jnp.exp(
        -math.log(10000.0) * (2.0 * jnp.arange(half_size, dtype=jnp.float32) / head_size)
    )
    phases = positions.astype(jnp.float32)[:, None] * inverse[None, :]
    return (jnp.cos(phases), jnp.sin(phases))


def rotate(values, cosine, sine, sign_flip):
    half_size = values.shape[-1] // 2
    first_half = values[..., :half_size]
    second_half = values[..., half_size:]
    return jnp.concatenate(
        [
            first_half * cosine - sign_flip * (second_half * sine),
            second_half * cosine + sign_flip * (first_half * sine),
        ],
        -1,
    )


def adam_update(weight, grad_vals, moment, square):
    moment_new = beta_one * moment + (1.0 - beta_one) * grad_vals
    square_new = beta_two * square + (1.0 - beta_two) * grad_vals * grad_vals
    moment_hat = moment_new / (1.0 - beta_one**STEP)
    square_hat = square_new / (1.0 - beta_two**STEP)
    step_vals = -learn_rate * (
        moment_hat / (jnp.sqrt(square_hat) + adam_eps) + decay_weight * weight
    )
    return (moment_new, square_new, step_vals)


def mm(a, b):
    return jnp.dot(a, b, preferred_element_type=F32)


def mm_t(a, b):
    return lax.dot_general(a, b, (((1,), (1,)), ((), ())), preferred_element_type=F32)


def mm_tn(a, b):
    return lax.dot_general(a, b, (((0,), (0,)), ((), ())), preferred_element_type=F32)


def ein(spec, a, b):
    return jnp.einsum(spec, a, b, preferred_element_type=F32)


MESH_ID = pl.DeviceIdType.MESH
ANY = pl.BlockSpec(memory_space=pl.ANY)
VM = pl.BlockSpec(memory_space=pltpu.VMEM)


def greet(peers):
    sem = pltpu.get_barrier_semaphore()
    for peer in peers:
        pl.semaphore_signal(sem, inc=1, device_id=peer, device_id_type=MESH_ID)
    pl.semaphore_wait(sem, len(peers))


def push(src, dst, send, recv, peer):
    copy = pltpu.make_async_remote_copy(
        src_ref=src, dst_ref=dst, send_sem=send, recv_sem=recv, device_id=peer, device_id_type=MESH_ID
    )
    copy.start()
    return copy


def arrived(dst, send, recv, peer):
    pltpu.make_async_remote_copy(
        src_ref=dst, dst_ref=dst, send_sem=send, recv_sem=recv, device_id=peer, device_id_type=MESH_ID
    ).wait_recv()


def beside(c):
    low = c + 1 - 2 * (c % 2)
    high = (c + 2) % 4
    return low, high, (low + 2) % 4


def cost(micros):
    return pl.CostEstimate(flops=0, transcendentals=0, bytes_accessed=int(micros * 3.0e6))


def along(s, n):
    if n == 4:
        return [s, s + 1 - 2 * (s % 2), (s + 2) % 4, 3 - s]
    return [lax.rem(s + j, n) for j in range(n)]


def params(ident):
    return pltpu.CompilerParams(collective_id=ident, has_side_effects=True)


def others(s, c, f, sp_n, f_n):
    ids, flat = [], []
    for a in range(sp_n):
        for b in range(4):
            for d in range(f_n):
                if a or b or d:
                    p, q, r = lax.rem(s + a, sp_n), lax.rem(c + b, 4), lax.rem(f + d, f_n)
                    ids.append({"sp": p, "ctx": q, "fsdp": r})
                    flat.append((p * 4 + q) * f_n + r)
    return ids, flat


def spread_kernel(sp_n, f_n, wp_in, wu_in, wo_in, wd_in, x_in, g_in, wp, wu, wo, wd, x, g, gs, gr, lsem, zs, zr, xs, xr, ps, pr, cs, cr):
    s, c, f = lax.axis_index("sp"), lax.axis_index("ctx"), lax.axis_index("fsdp")
    low, high, both = beside(c)
    lines = along(s, sp_n)
    cores = [lax.rem(f + k, f_n) for k in range(1, f_n)]
    here = (s * 4 + c) * f_n + f
    ids, flat = others(s, c, f, sp_n, f_n)
    greet(ids)
    n_items = 2 * sp_n + 2
    waits = []

    def item_at(i, cc, ff):
        if i < 2:
            return (wo, wd)[i].at[cc, ff]
        j, a = (i - 2) // 2, (i - 2) % 2
        return (wp, wu)[a].at[cc, ff, lines[j]]

    def key(i):
        if i < 2:
            return i
        j, a = (i - 2) // 2, (i - 2) % 2
        return 2 + a * sp_n + lines[j]

    def own(i):
        if i < 2:
            return (wo_in, wd_in)[i]
        a = (i - 2) % 2
        return (wp_in, wu_in)[a].at[s]

    def start_local(n, src, dst):
        copy = pltpu.make_async_copy(src, dst, lsem.at[n])
        copy.start()
        return copy

    for n, p in enumerate(ids):
        waits.append(push(g_in, g.at[here], gs.at[n], gr.at[here], p))
    for j in range(1, sp_n):
        for a in range(2):
            src, dst = ((wp_in, wp), (wu_in, wu))[a]
            waits.append(
                push(src.at[lines[j]], dst.at[c, f, s], zs.at[a * sp_n + j], zr.at[a * sp_n + s], {"sp": lines[j]})
            )
    for j in range(1, sp_n):
        waits.append(push(x_in, x.at[s], xs.at[j], xr.at[s], {"sp": lines[j]}))
    local = [start_local(i, own(i), item_at(i, c, f)) for i in range(4)]
    local.append(start_local(4, x_in, x.at[s]))
    local.append(start_local(5, g_in, g.at[here]))

    def to_cores(i, src, cc):
        for n, p in enumerate(cores):
            waits.append(
                push(
                    src,
                    item_at(i, cc, f),
                    cs.at[(n * 4 + cc) * n_items + i],
                    cr.at[(f * 4 + cc) * n_items + key(i)],
                    {"fsdp": p},
                )
            )

    def first(i):
        if i < 4:
            src = own(i)
        else:
            j, a = (i - 2) // 2, (i - 2) % 2
            arrived(item_at(i, c, f), zs.at[0], zr.at[a * sp_n + lines[j]], {"sp": lines[j]})
            src = item_at(i, c, f)
        for n, p in enumerate((low, high)):
            waits.append(
                push(src, item_at(i, c, f), ps.at[3 * i + n], pr.at[c * n_items + key(i)], {"ctx": p})
            )
        to_cores(i, src, c)

    def landed(i, cc):
        arrived(item_at(i, cc, f), ps.at[0], pr.at[cc * n_items + key(i)], {"ctx": cc})

    def second(i):
        landed(i, low)
        if i % 4 in (1, 2):
            waits.append(
                push(item_at(i, low, f), item_at(i, low, f), ps.at[3 * i + 2], pr.at[low * n_items + key(i)], {"ctx": high})
            )
        to_cores(i, item_at(i, low, f), low)
        landed(i, high)
        if i % 4 in (0, 3):
            waits.append(
                push(item_at(i, high, f), item_at(i, high, f), ps.at[3 * i + 2], pr.at[high * n_items + key(i)], {"ctx": low})
            )
        to_cores(i, item_at(i, high, f), high)

    def third(i):
        landed(i, both)
        to_cores(i, item_at(i, both, f), both)

    for i in range(n_items + 4):
        if i < n_items:
            first(i)
        if 2 <= i < n_items + 2:
            second(i - 2)
        if i >= 4:
            third(i - 4)
    for j in range(1, sp_n):
        arrived(x.at[lines[j]], xs.at[0], xr.at[lines[j]], {"sp": lines[j]})
    for p in cores:
        for cc in range(4):
            for i in range(n_items):
                arrived(item_at(i, cc, p), cs.at[0], cr.at[(p * 4 + cc) * n_items + key(i)], {"fsdp": p})
    for k, p in zip(flat, ids):
        arrived(g.at[k], gs.at[0], gr.at[k], p)
    for copy in waits:
        copy.wait_send()
    for copy in local:
        copy.wait()


def spread(wp_in, wu_in, wo_in, wd_in, x_in, g_in, sp_n, f_n, ident):
    rows = wp_in.shape[1]
    n_items = 2 * sp_n + 2
    shapes = [
        (4, f_n, sp_n, rows, wp_in.shape[2]),
        (4, f_n, sp_n, rows, wu_in.shape[2]),
        (4, f_n) + wo_in.shape,
        (4, f_n) + wd_in.shape,
        (sp_n,) + x_in.shape,
        (sp_n * 4 * f_n,) + g_in.shape,
    ]
    dma = pltpu.SemaphoreType.DMA
    return pl.pallas_call(
        functools.partial(spread_kernel, sp_n, f_n),
        out_shape=[jax.ShapeDtypeStruct(v, BF) for v in shapes],
        in_specs=[VM] * 6,
        out_specs=[ANY] * 6,
        scratch_shapes=[
            dma((sp_n * 4 * f_n,)),
            dma((sp_n * 4 * f_n,)),
            dma((6,)),
            dma((2 * sp_n,)),
            dma((2 * sp_n,)),
            dma((sp_n,)),
            dma((sp_n,)),
            dma((3 * n_items,)),
            dma((4 * n_items,)),
            dma(((f_n - 1) * 4 * n_items,)),
            dma((f_n * 4 * n_items,)),
        ],
        compiler_params=params(ident),
        cost_estimate=cost(110),
        name="spread",
    )(wp_in, wu_in, wo_in, wd_in, x_in, g_in)


def line_gather_kernel(n, x_in, out, lsem, ss, rs):
    s = lax.axis_index("sp")
    greet([{"sp": lax.rem(s + j, n)} for j in range(1, n)])
    up_ok, down_ok = s + 1 < n, s > 0

    def desc(slot, way, peer, first):
        return pltpu.make_async_remote_copy(
            src_ref=x_in if first else out.at[slot],
            dst_ref=out.at[slot],
            send_sem=ss.at[way * n + slot],
            recv_sem=rs.at[slot],
            device_id={"sp": peer},
            device_id_type=MESH_ID,
        )

    local = pltpu.make_async_copy(x_in, out.at[s], lsem)
    for k in range(n - 1):

        @pl.when((s - k >= 0) & up_ok)
        def _():
            desc(s - k, 0, s + 1, k == 0).start()

        @pl.when((s + k < n) & down_ok)
        def _():
            desc(s + k, 1, s - 1, k == 0).start()

        if k == 0:
            local.start()

        @pl.when(s - 1 - k >= 0)
        def _():
            desc(s - 1 - k, 0, s - 1, False).wait_recv()

        @pl.when(s + 1 + k < n)
        def _():
            desc(s + 1 + k, 1, s + 1, False).wait_recv()

    for k in range(n - 1):

        @pl.when((s - k >= 0) & up_ok)
        def _():
            desc(s - k, 0, s + 1, k == 0).wait_send()

        @pl.when((s + k < n) & down_ok)
        def _():
            desc(s + k, 1, s - 1, k == 0).wait_send()

    local.wait()


def line_gather(x, n, ident):
    dma = pltpu.SemaphoreType.DMA
    out = pl.pallas_call(
        functools.partial(line_gather_kernel, n),
        out_shape=jax.ShapeDtypeStruct((n,) + x.shape, x.dtype),
        in_specs=[VM],
        out_specs=VM,
        scratch_shapes=[dma, dma((2 * n,)), dma((n,))],
        compiler_params=params(ident),
        cost_estimate=cost(40),
        name="line_gather",
    )(x)
    return out.reshape((n * x.shape[0],) + x.shape[1:])


def line_swap_kernel(n, m, *refs):
    ins, outs, (lsem, ss, rs) = refs[:m], refs[m : 2 * m], refs[2 * m :]
    s = lax.axis_index("sp")
    peers = along(s, n)[1:]
    greet([{"sp": p} for p in peers])
    waits, local = [], []
    for k in range(m):
        for j, p in enumerate(peers):
            waits.append(
                push(ins[k].at[p], outs[k].at[s], ss.at[k * n + j], rs.at[k * n + s], {"sp": p})
            )
        copy = pltpu.make_async_copy(ins[k].at[s], outs[k].at[s], lsem.at[k])
        copy.start()
        local.append(copy)
    for k in range(m):
        for p in peers:
            arrived(outs[k].at[p], ss.at[0], rs.at[k * n + p], {"sp": p})
    for copy in waits:
        copy.wait_send()
    for copy in local:
        copy.wait()


def line_swap(xs, n, ident, micros):
    dma = pltpu.SemaphoreType.DMA
    m = len(xs)
    return pl.pallas_call(
        functools.partial(line_swap_kernel, n, m),
        out_shape=[jax.ShapeDtypeStruct(x.shape, x.dtype) for x in xs],
        in_specs=[VM] * m,
        out_specs=[VM] * m,
        scratch_shapes=[dma((m,)), dma((m * n,)), dma((m * n,))],
        compiler_params=params(ident),
        cost_estimate=cost(micros),
        name="line_swap",
    )(*xs)


def block_gather_kernel(n_items, x_in, out, lsem, ss, rs):
    c = lax.axis_index("ctx")
    low, high, both = beside(c)
    greet([{"ctx": low}, {"ctx": high}])
    waits = []
    for i in range(n_items):
        for n, p in enumerate((low, high)):
            waits.append(
                push(x_in.at[i], out.at[c, i], ss.at[3 * i + n], rs.at[c * n_items + i], {"ctx": p})
            )
    local = pltpu.make_async_copy(x_in, out.at[c], lsem)
    local.start()
    for i in range(n_items):
        for n, (came, goes) in enumerate(((low, high), (high, low))):
            arrived(out.at[came, i], ss.at[0], rs.at[came * n_items + i], {"ctx": came})
            if i % 2 == n:
                waits.append(
                    push(out.at[came, i], out.at[came, i], ss.at[3 * i + 2], rs.at[came * n_items + i], {"ctx": goes})
                )
    for i in range(n_items):
        arrived(out.at[both, i], ss.at[0], rs.at[both * n_items + i], {"ctx": both})
    for copy in waits:
        copy.wait_send()
    local.wait()


def block_gather(x, ident):
    n_items = x.shape[0]
    dma = pltpu.SemaphoreType.DMA
    return pl.pallas_call(
        functools.partial(block_gather_kernel, n_items),
        out_shape=jax.ShapeDtypeStruct((4,) + x.shape, x.dtype),
        in_specs=[VM],
        out_specs=VM,
        scratch_shapes=[dma, dma((3 * n_items,)), dma((4 * n_items,))],
        compiler_params=params(ident),
        cost_estimate=cost(22),
        name="block_gather",
    )(x)


def all_swap_kernel(sp_n, f_n, x_in, out, lsem, ss, rs):
    s, c, f = lax.axis_index("sp"), lax.axis_index("ctx"), lax.axis_index("fsdp")
    here = (s * 4 + c) * f_n + f
    ids, flat = others(s, c, f, sp_n, f_n)
    greet(ids)
    waits = [
        push(x_in.at[k], out.at[here], ss.at[n], rs.at[here], p)
        for n, (k, p) in enumerate(zip(flat, ids))
    ]
    local = pltpu.make_async_copy(x_in.at[here], out.at[here], lsem)
    local.start()
    for k, p in zip(flat, ids):
        arrived(out.at[k], ss.at[0], rs.at[k], p)
    for copy in waits:
        copy.wait_send()
    local.wait()


def all_swap(x, sp_n, f_n, ident):
    dma = pltpu.SemaphoreType.DMA
    n = x.shape[0]
    return pl.pallas_call(
        functools.partial(all_swap_kernel, sp_n, f_n),
        out_shape=jax.ShapeDtypeStruct(x.shape, x.dtype),
        in_specs=[VM],
        out_specs=VM,
        scratch_shapes=[dma, dma((n,)), dma((n,))],
        compiler_params=params(ident),
        cost_estimate=cost(10),
        name="all_swap",
    )(x)


def regroup(v, back):
    lane = lax.broadcasted_iota(jnp.int32, (v.shape[0], 128), 1) < 64
    piece = lambda k: v[:, 128 * k : 128 * k + 128]
    turn = lambda p: pltpu.roll(p, 64, 1)
    out = []
    for k in range(v.shape[1] // 128):
        if back:
            s, pair = k // 4, k % 4
            a, b, odd = 4 * pair + s // 2, 4 * pair + 2 + s // 2, s % 2
        else:
            cf, half = k // 2, k % 2
            a, b, odd = 8 * half + cf // 2, 8 * half + 4 + cf // 2, cf % 2
        if odd:
            out.append(jnp.where(lane, turn(piece(a)), piece(b)))
        else:
            out.append(jnp.where(lane, piece(a), turn(piece(b))))
    return jnp.concatenate(out, 1)


def added(main, lo):
    total = main[0].astype(F32)
    for k in range(1, main.shape[0]):
        total = total + main[k].astype(F32)
    if lo is not None:
        rest = lo[0].astype(F32)
        for k in range(1, lo.shape[0]):
            rest = rest + lo[k].astype(F32)
        total = total + jnp.where(pl.program_id(0) == 0, 1.0, 0.0) * rest
    return total


def tally(sums, grads, unit):
    @pl.when(pl.program_id(0) == 0)
    def _():
        sums[...] = jnp.zeros_like(sums)

    sums[0:1, :] += jnp.sum(grads * unit, 0, keepdims=True)
    sums[1:2, :] += jnp.sum(grads, 0, keepdims=True)


def ahead_kernel(group, main, lo, x, gains, hidden_out, bn_out):
    hidden = x[...].astype(F32) + added(main, lo)
    hidden_out[...] = hidden
    normed, _, _ = layer_stats(hidden, gains[2:3, :], gains[3:4, :])
    bn_out[...] = (regroup(normed, False) if group else normed).astype(BF)


def turn_kernel(group, main, lo, hidden, cot, gains, dh_out, dbr_out, sums):
    grads = added(main, lo)
    grads = regroup(grads, True) if group else grads
    _, unit, scale = layer_stats(hidden[...], gains[2:3, :], gains[3:4, :])
    dh = cot[...].astype(F32) + layer_back(grads, unit, scale, gains[2:3, :])
    dh_out[...] = dh
    dbr_out[...] = dh.astype(BF)
    tally(sums, grads, unit)


def last_kernel(group, main, x, dh, gains, gx_out, sums):
    grads = added(main, None)
    grads = regroup(grads, True) if group else grads
    _, unit, scale = layer_stats(x[...].astype(F32), gains[0:1, :], gains[1:2, :])
    gx_out[...] = (dh[...] + layer_back(grads, unit, scale, gains[0:1, :])).astype(BF)
    tally(sums, grads, unit)


def row_call(kernel, name, args, kinds, outs, rows, width, tile=16):
    n = args[0].shape[0]
    specs = {
        "main": pl.BlockSpec((n, tile, width), lambda i: (0, i, 0)),
        "lo": pl.BlockSpec((n, tile, width), lambda i: (0, rows // tile, 0)),
        "row": pl.BlockSpec((tile, width), lambda i: (i, 0)),
        "gains": pl.BlockSpec((4, width), lambda i: (0, 0)),
        "sums": pl.BlockSpec((8, width), lambda i: (0, 0)),
    }
    return pl.pallas_call(
        kernel,
        grid=(rows // tile,),
        in_specs=[specs[k] for k in kinds],
        out_specs=[specs["sums" if h == 8 else "row"] for h, _ in outs],
        out_shape=[jax.ShapeDtypeStruct((h, width), t) for h, t in outs],
        cost_estimate=cost(4),
        name=name,
    )(*args)


def shards(
    block_input,
    cotangent,
    decay_rate,
    weight_in,
    weight_out,
    norm_gains,
    moment_in,
    square_in,
    moment_out,
    square_out,
    moment_norm,
    square_norm,
):
    tok_count = block_input.shape[2]
    width = block_input.shape[3]
    sp_n = lax.axis_size("sp")
    ctx_n, f_n = lax.axis_size("ctx"), lax.axis_size("fsdp")
    plane_n = ctx_n * f_n
    heads = H // sp_n
    block_len = tok_count * sp_n
    sp_i = lax.axis_index("sp")
    ctx_i = lax.axis_index("ctx")
    rows_in = weight_in.shape[0]
    qk_w, vd_w = QK // sp_n, VD // sp_n
    widths = (qk_w, qk_w, vd_w, vd_w, vd_w)
    starts = (0, QK, 2 * QK, 2 * QK + VD, 2 * QK + 2 * VD)
    cut = 2 * qk_w + 2 * vd_w

    def perm(v):
        return v.reshape(-1, sp_n, plane_n, rows_in).swapaxes(1, 2).reshape(v.shape)

    def unperm(v):
        return v.reshape(-1, plane_n, sp_n, rows_in).swapaxes(1, 2).reshape(v.shape)

    w_low = weight_in.astype(BF)
    slabs = jnp.concatenate(
        [w_low[:, o : o + sp_n * w].reshape(rows_in, sp_n, w) for o, w in zip(starts, widths)], 2
    )
    slabs = slabs.swapaxes(0, 1)
    o_low = weight_out.astype(BF)
    own_x = block_input.reshape(tok_count, width)
    own_xp = perm(own_x)
    n_dev = sp_n * plane_n
    w_proj, w_up, w_o, w_down, full_x, gains = spread(
        slabs[:, :, :cut],
        slabs[:, :, cut:],
        o_low[:, :width],
        o_low[:, width:],
        own_xp,
        norm_gains.astype(BF),
        sp_n,
        f_n,
        0,
    )
    w_proj, w_up = w_proj.reshape(width, -1), w_up.reshape(width, -1)
    w_o, w_down = w_o.reshape(-1, width), w_down.reshape(-1, width)
    full_x = full_x.reshape(-1, width).astype(F32)
    gains = gains.swapaxes(0, 1).reshape(4, width).astype(F32)
    gains_p = perm(gains)

    grad_ffn_own = cotangent.reshape(tok_count, width)
    held_cot, full_x = lax.optimization_barrier((grad_ffn_own, full_x))
    grad_ffn = lax.all_gather(held_cot, "sp", axis=0, tiled=True)
    normed_a, _, _ = layer_stats(full_x, gains_p[0], gains_p[1])
    a_low = normed_a.astype(BF)
    proj = mm(a_low, w_proj)
    head_pos = ctx_i * block_len + jnp.arange(block_len, dtype=jnp.int32)
    cos_h, sin_h = angles(head_pos, DK)

    def split_heads(v, size):
        return v.reshape(block_len, heads, size).swapaxes(0, 1)

    def join_heads(v):
        return v.swapaxes(0, 1).reshape(block_len, -1)

    qs = rotate(split_heads(proj[:, :qk_w], DK), cos_h, sin_h, 1.0).astype(BF)
    ks = rotate(split_heads(proj[:, qk_w : 2 * qk_w], DK), cos_h, sin_h, 1.0).astype(BF)
    vs = split_heads(proj[:, 2 * qk_w : 2 * qk_w + vd_w], DV).astype(BF)
    gate = split_heads(proj[:, 2 * qk_w + vd_w :], DV)

    rates = lax.dynamic_slice_in_dim(decay_rate, sp_i * heads, heads)
    offs = jnp.arange(block_len, dtype=F32)
    spacing = offs[:, None] - offs[None, :]
    mask = jnp.where(
        spacing[None] >= 0.0, jnp.exp(-rates[:, None, None] * jnp.maximum(spacing, 0.0)[None]), 0.0
    )
    inward = jnp.exp(-rates[:, None] * (offs[None, :] + 1.0))[:, :, None]
    outward = jnp.exp(-rates[:, None] * (block_len - 1.0 - offs[None, :]))[:, :, None]
    blocks = jnp.arange(ctx_n)
    back_gap = (ctx_i - 1 - blocks).astype(F32)
    back_w = jnp.where(
        blocks[:, None] < ctx_i,
        jnp.exp(-rates[None, :] * block_len * jnp.maximum(back_gap, 0.0)[:, None]),
        0.0,
    )
    fore_gap = (blocks - ctx_i - 1).astype(F32)
    fore_w = jnp.where(
        blocks[:, None] > ctx_i,
        jnp.exp(-rates[None, :] * block_len * jnp.maximum(fore_gap, 0.0)[:, None]),
        0.0,
    )

    key_decayed = (ks * outward).astype(BF)
    own_state = ein("hjk,hjv->hkv", key_decayed, vs)
    states = block_gather(own_state.astype(BF), 2).astype(F32)
    state = jnp.sum(states * back_w[:, :, None, None], 0).astype(BF)
    scores = ein("hik,hjk->hij", qs, ks)
    probs = (scores * mask).astype(BF)
    mixed = (ein("hij,hjv->hiv", probs, vs) + ein("hik,hkv->hiv", qs, state) * inward).astype(BF)
    mixed_vals = mixed.astype(F32)
    centred = mixed_vals - jnp.mean(mixed_vals, axis=-1, keepdims=True)
    group_scale = lax.rsqrt(jnp.mean(centred * centred, axis=-1, keepdims=True) + norm_eps)
    unit_h = centred * group_scale
    gate_sig = jax.nn.sigmoid(gate)
    gate_act = gate * gate_sig
    gated = join_heads((gate_act * unit_h).astype(BF))

    group = rows_in == 64 and sp_n == 4 and plane_n == 8
    fine = 16

    def parts_of(v, fine):
        v = v.reshape(sp_n, tok_count, width)
        main = lax.reduce_precision(v, 8, 7)
        rest = [v[:, :fine] - main[:, :fine]] if fine else []
        return jnp.concatenate([main] + rest, 1).astype(BF)

    (got,) = line_swap([parts_of(mm(gated, w_o), fine)], sp_n, 4, 45)
    hidden, normed_b = row_call(
        functools.partial(ahead_kernel, group),
        "ahead",
        (got, got, own_x, gains),
        ("main", "lo", "row", "gains"),
        ((tok_count, F32), (tok_count, BF)),
        tok_count,
        width,
    )
    b_low = line_gather(normed_b if group else perm(normed_b), sp_n, 5)
    up = mm(b_low, w_up)
    act_low = jax.nn.gelu(up, approximate=False).astype(BF)
    ffn_part = mm(act_low, w_down).astype(BF)
    ffn_part, grad_ffn = lax.optimization_barrier((ffn_part, grad_ffn))
    ffn = lax.psum_scatter(ffn_part, "sp", scatter_dimension=0, tiled=True)

    grad_act = mm_t(grad_ffn, w_down)
    density = (
        0.5 * (1.0 + lax.erf(up * root_half)) + up * jnp.exp(-0.5 * up * up) * inv_root_tau
    )
    grad_up = (grad_act * density).astype(BF)

    def reduce_rows(v):
        return lax.psum_scatter(v, PLANE, scatter_dimension=0, tiled=True)

    part_down = mm_tn(act_low, grad_ffn).astype(BF)
    part_up = mm_tn(b_low, grad_up).astype(BF)
    part_b = parts_of(mm_t(grad_up, w_up), fine)
    part_b, part_down, part_up = lax.optimization_barrier((part_b, part_down, part_up))
    sum_down = reduce_rows(part_down)
    sum_up = reduce_rows(part_up)
    (got,) = line_swap([part_b if group else unperm(part_b)], sp_n, 6, 45)
    got, ffn = lax.optimization_barrier((got, ffn))
    grad_hidden, grad_branch, sums_b = row_call(
        functools.partial(turn_kernel, group),
        "turn",
        (got, got, hidden, grad_ffn_own, gains),
        ("main", "lo", "row", "row", "gains"),
        ((tok_count, F32), (tok_count, BF), (8, F32)),
        tok_count,
        width,
    )
    grad_branch = line_gather(grad_branch, sp_n, 7)
    block_out = (hidden + ffn.astype(F32)).astype(BF).reshape(block_input.shape)
    part_o = mm_tn(gated, grad_branch).astype(BF)

    grad_gated = split_heads(mm_t(grad_branch, w_o), DV)
    grad_gate = (grad_gated * unit_h * gate_sig * (1.0 + gate * (1.0 - gate_sig))).astype(BF)
    grad_unit = grad_gated * gate_act
    grad_mixed = (
        group_scale
        * (
            grad_unit
            - jnp.mean(grad_unit, axis=-1, keepdims=True)
            - unit_h * jnp.mean(grad_unit * unit_h, axis=-1, keepdims=True)
        )
    ).astype(BF)
    grad_read = (grad_mixed * inward).astype(BF)
    own_reach = ein("hik,hiv->hkv", qs, grad_read).astype(BF)
    grad_gate = join_heads(grad_gate)
    grad_probs = ein("hiv,hjv->hij", grad_mixed, vs)
    grad_scores = (grad_probs * mask).astype(BF)
    grad_q = ein("hij,hjk->hik", grad_scores, ks) + ein("hiv,hkv->hik", grad_read, state)
    grad_gq = jnp.concatenate([grad_gate, join_heads(rotate(grad_q, cos_h, sin_h, -1.0).astype(BF))], 1)
    part_gq = mm_tn(a_low, grad_gq).astype(BF)
    own_reach, part_o, part_gq, sum_down, sum_up = lax.optimization_barrier(
        (own_reach, part_o, part_gq, sum_down, sum_up)
    )
    sum_o = reduce_rows(part_o)
    sum_gq = reduce_rows(part_gq)
    reaches = block_gather(own_reach, 3).astype(F32)
    reach = jnp.sum(reaches * fore_w[:, :, None, None], 0).astype(BF)
    grad_k = ein("hij,hik->hjk", grad_scores, qs) + ein("hjv,hkv->hjk", vs, reach) * outward
    grad_v = ein("hij,hiv->hjv", probs, grad_mixed) + ein("hjk,hkv->hjv", key_decayed, reach)
    grad_kv = jnp.concatenate(
        [join_heads(rotate(grad_k, cos_h, sin_h, -1.0).astype(BF)), join_heads(grad_v.astype(BF))], 1
    )
    part_kv = mm_tn(a_low, grad_kv).astype(BF)
    grad_proj = jnp.concatenate([grad_gq[:, vd_w:], grad_kv, grad_gate], 1)
    part_a = parts_of(mm_t(grad_proj, w_proj), 0)
    part_a, part_kv = lax.optimization_barrier((part_a, part_kv))
    sum_kv = reduce_rows(part_kv)

    def home(v):
        return v.reshape(sp_n, rows_in, -1)

    got, back_up = line_swap([part_a if group else unperm(part_a), home(sum_up)], sp_n, 8, 58)
    grad_x, sums_a = row_call(
        functools.partial(last_kernel, group),
        "last",
        (got, own_x, grad_hidden, gains),
        ("main", "row", "row", "gains"),
        ((tok_count, BF), (8, F32)),
        tok_count,
        width,
    )
    grad_x = grad_x.reshape(block_input.shape)
    norm_terms = jnp.concatenate([sums_a[:2], sums_b[:2]], 0)
    norm_parts = norm_terms.reshape(4, n_dev, -1).swapaxes(0, 1)
    grad_gains = jnp.sum(all_swap(norm_parts, sp_n, f_n, 9), 0)
    back_gq, back_kv = line_swap([home(sum_gq), home(sum_kv)], sp_n, 10, 38)
    parts = [back_gq[:, :, vd_w:], back_kv[:, :, :qk_w], back_kv[:, :, qk_w:], back_gq[:, :, :vd_w], back_up]
    grad_first = jnp.concatenate(
        [p.swapaxes(0, 1).reshape(rows_in, -1) for p in parts], 1
    ).astype(F32)
    grad_second = jnp.concatenate([sum_o, sum_down], 1).astype(F32)
    first_m, first_v, first_step = adam_update(weight_in, grad_first, moment_in, square_in)
    second_m, second_v, second_step = adam_update(weight_out, grad_second, moment_out, square_out)
    gain_m, gain_v, gain_step = adam_update(norm_gains, grad_gains, moment_norm, square_norm)
    return (
        block_out,
        grad_x,
        grad_first,
        first_m,
        first_v,
        first_step,
        grad_second,
        second_m,
        second_v,
        second_step,
        grad_gains,
        gain_m,
        gain_v,
        gain_step,
    )


def solution(mesh):
    tokens = P("fsdp", "ctx", "sp", None)
    rows = P(ALL, None)
    cols = P(None, ALL)
    in_specs = (tokens, tokens, P(), rows, rows, cols, rows, rows, rows, rows, cols, cols)
    out_specs = (tokens, tokens) + (rows,) * 8 + (cols,) * 4
    return jax.shard_map(shards, mesh=mesh, in_specs=in_specs, out_specs=out_specs, check_vma=False)
```

```python
import functools
import math

import jax
import jax.numpy as jnp
from jax import lax
from jax.experimental import pallas as pl
from jax.experimental.pallas import tpu as pltpu
from jax.sharding import PartitionSpec as P

H = 8
DK = 256
DV = 512
SPAN = 512
STEP = 10
QK = 2048
VD = 4096

beta_one = 0.9
beta_two = 0.95
learn_rate = 0.01
decay_weight = 0.1
adam_eps = 1e-08
norm_eps = 1e-05
root_half = 0.7071067811865476
inv_root_tau = 0.3989422804014327


BF = jnp.bfloat16
F32 = jnp.float32
ALL = ("sp", "ctx", "fsdp")
PLANE = ("ctx", "fsdp")


def layer_stats(values, gain_row, shift_row):
    centred = values - jnp.mean(values, axis=-1, keepdims=True)
    inv_std = lax.rsqrt(jnp.mean(centred * centred, axis=-1, keepdims=True) + norm_eps)
    unit_vals = centred * inv_std
    return (unit_vals * gain_row + shift_row, unit_vals, inv_std)


def layer_back(grad_vals, unit_vals, inv_std, gain_row):
    scaled = grad_vals * gain_row
    return inv_std * (
        scaled
        - jnp.mean(scaled, axis=-1, keepdims=True)
        - unit_vals * jnp.mean(scaled * unit_vals, axis=-1, keepdims=True)
    )


def angles(positions, head_size):
    half_size = head_size // 2
    inverse = jnp.exp(
        -math.log(10000.0) * (2.0 * jnp.arange(half_size, dtype=jnp.float32) / head_size)
    )
    phases = positions.astype(jnp.float32)[:, None] * inverse[None, :]
    return (jnp.cos(phases), jnp.sin(phases))


def rotate(values, cosine, sine, sign_flip):
    half_size = values.shape[-1] // 2
    first_half = values[..., :half_size]
    second_half = values[..., half_size:]
    return jnp.concatenate(
        [
            first_half * cosine - sign_flip * (second_half * sine),
            second_half * cosine + sign_flip * (first_half * sine),
        ],
        -1,
    )


def adam_update(weight, grad_vals, moment, square):
    moment_new = beta_one * moment + (1.0 - beta_one) * grad_vals
    square_new = beta_two * square + (1.0 - beta_two) * grad_vals * grad_vals
    moment_hat = moment_new / (1.0 - beta_one**STEP)
    square_hat = square_new / (1.0 - beta_two**STEP)
    step_vals = -learn_rate * (
        moment_hat / (jnp.sqrt(square_hat) + adam_eps) + decay_weight * weight
    )
    return (moment_new, square_new, step_vals)


def mm(a, b):
    return jnp.dot(a, b, preferred_element_type=F32)


def mm_t(a, b):
    return lax.dot_general(a, b, (((1,), (1,)), ((), ())), preferred_element_type=F32)


def mm_tn(a, b):
    return lax.dot_general(a, b, (((0,), (0,)), ((), ())), preferred_element_type=F32)


def ein(spec, a, b):
    return jnp.einsum(spec, a, b, preferred_element_type=F32)


MESH_ID = pl.DeviceIdType.MESH
ANY = pl.BlockSpec(memory_space=pl.ANY)
VM = pl.BlockSpec(memory_space=pltpu.VMEM)


def greet(peers):
    sem = pltpu.get_barrier_semaphore()
    for peer in peers:
        pl.semaphore_signal(sem, inc=1, device_id=peer, device_id_type=MESH_ID)
    pl.semaphore_wait(sem, len(peers))


def push(src, dst, send, recv, peer):
    copy = pltpu.make_async_remote_copy(
        src_ref=src, dst_ref=dst, send_sem=send, recv_sem=recv, device_id=peer, device_id_type=MESH_ID
    )
    copy.start()
    return copy


def arrived(dst, send, recv, peer):
    pltpu.make_async_remote_copy(
        src_ref=dst, dst_ref=dst, send_sem=send, recv_sem=recv, device_id=peer, device_id_type=MESH_ID
    ).wait_recv()


def beside(c):
    low = c + 1 - 2 * (c % 2)
    high = (c + 2) % 4
    return low, high, (low + 2) % 4


def cost(micros):
    return pl.CostEstimate(flops=0, transcendentals=0, bytes_accessed=int(micros * 3.0e6))


def along(s, n):
    if n == 4:
        return [s, s + 1 - 2 * (s % 2), (s + 2) % 4, 3 - s]
    return [lax.rem(s + j, n) for j in range(n)]


def params(ident):
    return pltpu.CompilerParams(collective_id=ident, has_side_effects=True)


def others(s, c, f, sp_n, f_n):
    ids, flat = [], []
    for a in range(sp_n):
        for b in range(4):
            for d in range(f_n):
                if a or b or d:
                    p, q, r = lax.rem(s + a, sp_n), lax.rem(c + b, 4), lax.rem(f + d, f_n)
                    ids.append({"sp": p, "ctx": q, "fsdp": r})
                    flat.append((p * 4 + q) * f_n + r)
    return ids, flat


def spread_kernel(sp_n, f_n, wp_in, wo_in, x_in, g_in, wp, wo, x, g, gs, gr, lsem, zs, zr, xs, xr, ps, pr, cs, cr):
    s, c, f = lax.axis_index("sp"), lax.axis_index("ctx"), lax.axis_index("fsdp")
    low, high, both = beside(c)
    lines = along(s, sp_n)
    cores = [lax.rem(f + k, f_n) for k in range(1, f_n)]
    here = (s * 4 + c) * f_n + f
    ids, flat = others(s, c, f, sp_n, f_n)
    greet(ids)
    n_items = sp_n + 1
    waits = []

    def item_at(i, cc, ff):
        return wp.at[cc, ff, lines[i - 1]] if i else wo.at[cc, ff]

    def key(i):
        return 1 + lines[i - 1] if i else 0

    def start_local(n, src, dst):
        copy = pltpu.make_async_copy(src, dst, lsem.at[n])
        copy.start()
        return copy

    for n, p in enumerate(ids):
        waits.append(push(g_in, g.at[here], gs.at[n], gr.at[here], p))
    for j in range(1, sp_n):
        waits.append(push(wp_in.at[lines[j]], wp.at[c, f, s], zs.at[j], zr.at[s], {"sp": lines[j]}))
    for j in range(1, sp_n):
        waits.append(push(x_in, x.at[s], xs.at[j], xr.at[s], {"sp": lines[j]}))
    own = (wo_in, wp_in.at[s])
    local = [start_local(i, own[i], item_at(i, c, f)) for i in range(2)]
    local.append(start_local(2, x_in, x.at[s]))
    local.append(start_local(3, g_in, g.at[here]))

    def to_cores(i, src, cc):
        for n, p in enumerate(cores):
            waits.append(
                push(
                    src,
                    item_at(i, cc, f),
                    cs.at[(n * 4 + cc) * n_items + i],
                    cr.at[(f * 4 + cc) * n_items + key(i)],
                    {"fsdp": p},
                )
            )

    def first(i):
        if i < 2:
            src = own[i]
        else:
            src = item_at(i, c, f)
            arrived(src, zs.at[0], zr.at[lines[i - 1]], {"sp": lines[i - 1]})
        for n, p in enumerate((low, high)):
            waits.append(
                push(src, item_at(i, c, f), ps.at[3 * i + n], pr.at[c * n_items + key(i)], {"ctx": p})
            )
        to_cores(i, src, c)

    def landed(i, cc):
        arrived(item_at(i, cc, f), ps.at[0], pr.at[cc * n_items + key(i)], {"ctx": cc})

    def second(i):
        for n, (came, goes) in enumerate(((low, high), (high, low))):
            landed(i, came)
            at = item_at(i, came, f)
            if i % 2 == n:
                waits.append(push(at, at, ps.at[3 * i + 2], pr.at[came * n_items + key(i)], {"ctx": goes}))
            to_cores(i, at, came)

    def third(i):
        landed(i, both)
        to_cores(i, item_at(i, both, f), both)

    for i in range(n_items + 2):
        if i < n_items:
            first(i)
        if 1 <= i < n_items + 1:
            second(i - 1)
        if i >= 2:
            third(i - 2)
    for j in range(1, sp_n):
        arrived(x.at[lines[j]], xs.at[0], xr.at[lines[j]], {"sp": lines[j]})
    for p in cores:
        for cc in range(4):
            for i in range(n_items):
                arrived(item_at(i, cc, p), cs.at[0], cr.at[(p * 4 + cc) * n_items + key(i)], {"fsdp": p})
    for k, p in zip(flat, ids):
        arrived(g.at[k], gs.at[0], gr.at[k], p)
    for copy in waits:
        copy.wait_send()
    for copy in local:
        copy.wait()


def spread(wp_in, wo_in, x_in, g_in, sp_n, f_n, ident):
    n_items, n_dev = sp_n + 1, sp_n * 4 * f_n
    shapes = [
        (4, f_n) + wp_in.shape,
        (4, f_n) + wo_in.shape,
        (sp_n,) + x_in.shape,
        (n_dev,) + g_in.shape,
    ]
    dma = pltpu.SemaphoreType.DMA
    return pl.pallas_call(
        functools.partial(spread_kernel, sp_n, f_n),
        out_shape=[jax.ShapeDtypeStruct(v, BF) for v in shapes],
        in_specs=[VM] * 4,
        out_specs=[ANY] * 4,
        scratch_shapes=[
            dma((n_dev,)),
            dma((n_dev,)),
            dma((4,)),
            dma((sp_n,)),
            dma((sp_n,)),
            dma((sp_n,)),
            dma((sp_n,)),
            dma((3 * n_items,)),
            dma((4 * n_items,)),
            dma(((f_n - 1) * 4 * n_items,)),
            dma((f_n * 4 * n_items,)),
        ],
        compiler_params=params(ident),
        cost_estimate=cost(85),
        name="spread",
    )(wp_in, wo_in, x_in, g_in)


def exchange_kernel(plan, sp_n, f_n, *refs):
    m = len(plan)
    ins, outs, (ls, ss, rs) = refs[:m], refs[m : 2 * m], refs[2 * m :]
    s, c, f = lax.axis_index("sp"), lax.axis_index("ctx"), lax.axis_index("fsdp")
    low, high, both = beside(c)
    line = along(s, sp_n)[1:]
    cores = [lax.rem(f + k, f_n) for k in range(1, f_n)]
    kinds = set(plan)
    peers = []
    if kinds & {"swap", "gather"}:
        peers += [{"sp": p} for p in line]
    if kinds & {"ctx_swap"}:
        peers += [{"ctx": p} for p in (low, high, both)]
    elif kinds & {"block", "plane"}:
        peers += [{"ctx": p} for p in (low, high)]
    if kinds & {"core", "plane"}:
        peers += [{"fsdp": p} for p in cores]
    greet(peers)
    sends, local, steps, ends = [], [], [], []
    used = [0, 0, 0]

    def take(k, n):
        used[k] += n
        return used[k] - n

    def send(src, dst, r, peer):
        sends.append(push(src, dst, ss.at[take(1, 1)], rs.at[r], peer))

    def keep(src, dst):
        copy = pltpu.make_async_copy(src, dst, ls.at[take(0, 1)])
        copy.start()
        local.append(copy)

    def got(dst, r, peer):
        arrived(dst, ss.at[0], rs.at[r], peer)

    def swap(x, o):
        r = take(2, sp_n)
        for p in line:
            send(x.at[p], o.at[s], r + s, {"sp": p})
        keep(x.at[s], o.at[s])
        ends.append(lambda: [got(o.at[p], r + p, {"sp": p}) for p in line])

    def ctx_swap(x, o):
        r = take(2, 3)
        for p in (low, high, both):
            k = lax.rem(c - p + 4, 4) - 1
            send(x.at[p], o.at[k], r + k, {"ctx": p})
        ends.append(lambda: [got(o.at[k], r + k, {"ctx": low}) for k in range(3)])

    def core(x, o):
        r = take(2, f_n - 1)
        for p in cores:
            k = lax.rem(f - p + f_n, f_n) - 1
            send(x.at[:, p], o.at[k], r + k, {"fsdp": p})
        ends.append(lambda: [got(o.at[k], r + k, {"fsdp": cores[0]}) for k in range(f_n - 1)])

    def plane(x, o, wide):
        n = x.shape[0]
        r, rc = take(2, 4 * n), take(2, f_n * 4 * n) if wide else 0
        at = lambda cc, ff, i: o.at[cc, ff, i] if wide else o.at[cc, i]

        def across(src, cc, i):
            if wide:
                for p in cores:
                    send(src, at(cc, f, i), rc + (f * 4 + cc) * n + i, {"fsdp": p})

        for i in range(n):
            for p in (low, high):
                send(x.at[i], at(c, f, i), r + c * n + i, {"ctx": p})
            across(x.at[i], c, i)
        keep(x, o.at[c, f] if wide else o.at[c])

        def near(i):
            for k, (came, goes) in enumerate(((low, high), (high, low))):
                got(at(came, f, i), r + came * n + i, {"ctx": came})
                if i % 2 == k:
                    send(at(came, f, i), at(came, f, i), r + came * n + i, {"ctx": goes})
                across(at(came, f, i), came, i)

        def far(i):
            got(at(both, f, i), r + both * n + i, {"ctx": both})
            across(at(both, f, i), both, i)

        def close():
            for p in cores if wide else ():
                for cc in range(4):
                    for i in range(n):
                        got(at(cc, p, i), rc + (p * 4 + cc) * n + i, {"fsdp": p})

        steps.extend([functools.partial(near, i) for i in range(n)])
        steps.extend([functools.partial(far, i) for i in range(n)])
        ends.append(close)

    def gather(x, o):
        n = sp_n
        r, q = take(2, n), take(1, 2 * n)
        up_ok, down_ok = s + 1 < n, s > 0

        def desc(slot, way, peer, first):
            return pltpu.make_async_remote_copy(
                src_ref=x if first else o.at[slot],
                dst_ref=o.at[slot],
                send_sem=ss.at[q + way * n + slot],
                recv_sem=rs.at[r + slot],
                device_id={"sp": peer},
                device_id_type=MESH_ID,
            )

        def out_going(k, act):
            @pl.when((s - k >= 0) & up_ok)
            def _():
                act(desc(s - k, 0, s + 1, k == 0))

            @pl.when((s + k < n) & down_ok)
            def _():
                act(desc(s + k, 1, s - 1, k == 0))

        def incoming(k):
            @pl.when(s - 1 - k >= 0)
            def _():
                desc(s - 1 - k, 0, s - 1, False).wait_recv()

            @pl.when(s + 1 + k < n)
            def _():
                desc(s + 1 + k, 1, s + 1, False).wait_recv()

        def step(k):
            incoming(k)
            if k + 1 < n - 1:
                out_going(k + 1, lambda d: d.start())

        def close():
            for k in range(n - 1):
                out_going(k, lambda d: d.wait_send())

        out_going(0, lambda d: d.start())
        keep(x, o.at[s])
        steps.extend([functools.partial(step, k) for k in range(n - 1)])
        ends.append(close)

    for kind, x, o in zip(plan, ins, outs):
        if kind == "swap":
            swap(x, o)
        elif kind == "ctx_swap":
            ctx_swap(x, o)
        elif kind == "core":
            core(x, o)
        elif kind == "gather":
            gather(x, o)
        else:
            plane(x, o, kind == "plane")
    for step in steps:
        step()
    for end in ends:
        end()
    for copy in sends:
        copy.wait_send()
    for copy in local:
        copy.wait()


def exchange(ops, sp_n, f_n, ident, micros):
    plan = tuple(kind for kind, _ in ops)
    outs, n_send, n_recv = [], 0, 0
    for kind, x in ops:
        n = x.shape[0]
        if kind == "swap":
            shape, a, b = x.shape, sp_n - 1, sp_n
        elif kind == "ctx_swap":
            shape, a, b = (3,) + x.shape[1:], 3, 3
        elif kind == "core":
            shape, a, b = (f_n - 1, x.shape[0]) + x.shape[2:], f_n - 1, f_n - 1
        elif kind == "gather":
            shape, a, b = (sp_n,) + x.shape, 2 * sp_n, sp_n
        elif kind == "block":
            shape, a, b = (4,) + x.shape, 3 * n, 4 * n
        else:
            shape, a, b = (4, f_n) + x.shape, 3 * n + 4 * n * (f_n - 1), 4 * n * (f_n + 1)
        outs.append(jax.ShapeDtypeStruct(shape, x.dtype))
        n_send, n_recv = n_send + a, n_recv + b
    dma = pltpu.SemaphoreType.DMA
    far = ("core", "ctx_swap")
    return pl.pallas_call(
        functools.partial(exchange_kernel, plan, sp_n, f_n),
        out_shape=outs,
        in_specs=[ANY if kind in far else VM for kind in plan],
        out_specs=[ANY if kind in far + ("plane",) else VM for kind in plan],
        scratch_shapes=[dma((len(ops),)), dma((n_send,)), dma((n_recv,))],
        compiler_params=params(ident),
        cost_estimate=cost(micros),
        name="exchange_" + "_".join(plan),
    )(*[x for _, x in ops])


def all_swap_kernel(sp_n, f_n, x_in, out, lsem, ss, rs):
    s, c, f = lax.axis_index("sp"), lax.axis_index("ctx"), lax.axis_index("fsdp")
    here = (s * 4 + c) * f_n + f
    ids, flat = others(s, c, f, sp_n, f_n)
    greet(ids)
    waits = [
        push(x_in.at[k], out.at[here], ss.at[n], rs.at[here], p)
        for n, (k, p) in enumerate(zip(flat, ids))
    ]
    local = pltpu.make_async_copy(x_in.at[here], out.at[here], lsem)
    local.start()
    for k, p in zip(flat, ids):
        arrived(out.at[k], ss.at[0], rs.at[k], p)
    for copy in waits:
        copy.wait_send()
    local.wait()


def all_swap(x, sp_n, f_n, ident):
    dma = pltpu.SemaphoreType.DMA
    n = x.shape[0]
    return pl.pallas_call(
        functools.partial(all_swap_kernel, sp_n, f_n),
        out_shape=jax.ShapeDtypeStruct(x.shape, x.dtype),
        in_specs=[VM],
        out_specs=VM,
        scratch_shapes=[dma, dma((n,)), dma((n,))],
        compiler_params=params(ident),
        cost_estimate=cost(10),
        name="all_swap",
    )(x)


def regroup(v, back):
    lane = lax.broadcasted_iota(jnp.int32, (v.shape[0], 128), 1) < 64
    piece = lambda k: v[:, 128 * k : 128 * k + 128]
    turn = lambda p: pltpu.roll(p, 64, 1)
    out = []
    for k in range(v.shape[1] // 128):
        if back:
            s, pair = k // 4, k % 4
            a, b, odd = 4 * pair + s // 2, 4 * pair + 2 + s // 2, s % 2
        else:
            cf, half = k // 2, k % 2
            a, b, odd = 8 * half + cf // 2, 8 * half + 4 + cf // 2, cf % 2
        if odd:
            out.append(jnp.where(lane, turn(piece(a)), piece(b)))
        else:
            out.append(jnp.where(lane, piece(a), turn(piece(b))))
    return jnp.concatenate(out, 1)


def added(main, lo):
    total = main[0].astype(F32)
    for k in range(1, main.shape[0]):
        total = total + main[k].astype(F32)
    if lo is not None:
        rest = lo[0].astype(F32)
        for k in range(1, lo.shape[0]):
            rest = rest + lo[k].astype(F32)
        total = total + jnp.where(pl.program_id(0) == 0, 1.0, 0.0) * rest
    return total


def tally(sums, grads, unit):
    @pl.when(pl.program_id(0) == 0)
    def _():
        sums[...] = jnp.zeros_like(sums)

    sums[0:1, :] += jnp.sum(grads * unit, 0, keepdims=True)
    sums[1:2, :] += jnp.sum(grads, 0, keepdims=True)


def ahead_kernel(group, main, lo, x, gains, hidden_out, bn_out):
    hidden = x[...].astype(F32) + added(main, lo)
    hidden_out[...] = hidden
    normed, _, _ = layer_stats(hidden, gains[2:3, :], gains[3:4, :])
    bn_out[...] = (regroup(normed, False) if group else normed).astype(BF)


def turn_kernel(group, main, lo, hidden, cot, gains, dh_out, dbr_out, sums):
    grads = added(main, lo)
    grads = regroup(grads, True) if group else grads
    _, unit, scale = layer_stats(hidden[...], gains[2:3, :], gains[3:4, :])
    dh = cot[...].astype(F32) + layer_back(grads, unit, scale, gains[2:3, :])
    dh_out[...] = dh
    dbr_out[...] = dh.astype(BF)
    tally(sums, grads, unit)


def last_kernel(group, main, x, dh, gains, gx_out, sums):
    grads = added(main, None)
    grads = regroup(grads, True) if group else grads
    _, unit, scale = layer_stats(x[...].astype(F32), gains[0:1, :], gains[1:2, :])
    gx_out[...] = (dh[...] + layer_back(grads, unit, scale, gains[0:1, :])).astype(BF)
    tally(sums, grads, unit)


def row_call(kernel, name, args, kinds, outs, rows, width, tile=16):
    n = args[0].shape[0]
    specs = {
        "main": pl.BlockSpec((n, tile, width), lambda i: (0, i, 0)),
        "lo": pl.BlockSpec((n, tile, width), lambda i: (0, rows // tile, 0)),
        "row": pl.BlockSpec((tile, width), lambda i: (i, 0)),
        "gains": pl.BlockSpec((4, width), lambda i: (0, 0)),
        "sums": pl.BlockSpec((8, width), lambda i: (0, 0)),
    }
    return pl.pallas_call(
        kernel,
        grid=(rows // tile,),
        in_specs=[specs[k] for k in kinds],
        out_specs=[specs["sums" if h == 8 else "row"] for h, _ in outs],
        out_shape=[jax.ShapeDtypeStruct((h, width), t) for h, t in outs],
        cost_estimate=cost(4),
        name=name,
    )(*args)


def shards(
    block_input,
    cotangent,
    decay_rate,
    weight_in,
    weight_out,
    norm_gains,
    moment_in,
    square_in,
    moment_out,
    square_out,
    moment_norm,
    square_norm,
):
    tok_count = block_input.shape[2]
    width = block_input.shape[3]
    sp_n = lax.axis_size("sp")
    ctx_n, f_n = lax.axis_size("ctx"), lax.axis_size("fsdp")
    plane_n = ctx_n * f_n
    heads = H // sp_n
    block_len = tok_count * sp_n
    sp_i = lax.axis_index("sp")
    ctx_i = lax.axis_index("ctx")
    rows_in = weight_in.shape[0]
    qk_w, vd_w = QK // sp_n, VD // sp_n
    widths = (qk_w, qk_w, vd_w, vd_w, vd_w)
    starts = (0, QK, 2 * QK, 2 * QK + VD, 2 * QK + 2 * VD)
    cut = 2 * qk_w + 2 * vd_w

    def perm(v):
        return v.reshape(-1, sp_n, plane_n, rows_in).swapaxes(1, 2).reshape(v.shape)

    def unperm(v):
        return v.reshape(-1, plane_n, sp_n, rows_in).swapaxes(1, 2).reshape(v.shape)

    w_low = weight_in.astype(BF)
    slabs = jnp.concatenate(
        [w_low[:, o : o + sp_n * w].reshape(rows_in, sp_n, w) for o, w in zip(starts, widths)], 2
    )
    slabs = slabs.swapaxes(0, 1)
    o_low = weight_out.astype(BF)
    own_x = block_input.reshape(tok_count, width)
    own_xp = perm(own_x)
    n_dev = sp_n * plane_n
    w_proj, w_o, full_x, gains = spread(
        slabs[:, :, :cut], o_low[:, :width], own_xp, norm_gains.astype(BF), sp_n, f_n, 0
    )
    w_proj, w_o = w_proj.reshape(width, -1), w_o.reshape(-1, width)
    full_x = full_x.reshape(-1, width).astype(F32)
    gains = gains.swapaxes(0, 1).reshape(4, width).astype(F32)
    gains_p = perm(gains)

    grad_ffn_own = cotangent.reshape(tok_count, width)
    held_cot, full_x = lax.optimization_barrier((grad_ffn_own, full_x))
    grad_ffn = lax.all_gather(held_cot, "sp", axis=0, tiled=True)
    normed_a, _, _ = layer_stats(full_x, gains_p[0], gains_p[1])
    a_low = normed_a.astype(BF)
    proj = mm(a_low, w_proj)
    head_pos = ctx_i * block_len + jnp.arange(block_len, dtype=jnp.int32)
    cos_h, sin_h = angles(head_pos, DK)

    def split_heads(v, size):
        return v.reshape(block_len, heads, size).swapaxes(0, 1)

    def join_heads(v):
        return v.swapaxes(0, 1).reshape(block_len, -1)

    qs = rotate(split_heads(proj[:, :qk_w], DK), cos_h, sin_h, 1.0).astype(BF)
    ks = rotate(split_heads(proj[:, qk_w : 2 * qk_w], DK), cos_h, sin_h, 1.0).astype(BF)
    vs = split_heads(proj[:, 2 * qk_w : 2 * qk_w + vd_w], DV).astype(BF)
    gate = split_heads(proj[:, 2 * qk_w + vd_w :], DV)

    rates = lax.dynamic_slice_in_dim(decay_rate, sp_i * heads, heads)
    offs = jnp.arange(block_len, dtype=F32)
    spacing = offs[:, None] - offs[None, :]
    mask = jnp.where(
        spacing[None] >= 0.0, jnp.exp(-rates[:, None, None] * jnp.maximum(spacing, 0.0)[None]), 0.0
    )
    inward = jnp.exp(-rates[:, None] * (offs[None, :] + 1.0))[:, :, None]
    outward = jnp.exp(-rates[:, None] * (block_len - 1.0 - offs[None, :]))[:, :, None]
    blocks = jnp.arange(ctx_n)
    back_gap = (ctx_i - 1 - blocks).astype(F32)
    back_w = jnp.where(
        blocks[:, None] < ctx_i,
        jnp.exp(-rates[None, :] * block_len * jnp.maximum(back_gap, 0.0)[:, None]),
        0.0,
    )
    fore_gap = (blocks - ctx_i - 1).astype(F32)
    fore_w = jnp.where(
        blocks[:, None] > ctx_i,
        jnp.exp(-rates[None, :] * block_len * jnp.maximum(fore_gap, 0.0)[:, None]),
        0.0,
    )

    key_decayed = (ks * outward).astype(BF)
    own_state = ein("hjk,hjv->hkv", key_decayed, vs)
    states, up_rows = exchange(
        [("block", own_state.astype(BF)), ("swap", slabs[:, :, cut:])], sp_n, f_n, 2, 25
    )
    states = states.astype(F32)
    state = jnp.sum(states * back_w[:, :, None, None], 0).astype(BF)
    scores = ein("hik,hjk->hij", qs, ks)
    probs = (scores * mask).astype(BF)
    mixed = (ein("hij,hjv->hiv", probs, vs) + ein("hik,hkv->hiv", qs, state) * inward).astype(BF)
    mixed_vals = mixed.astype(F32)
    centred = mixed_vals - jnp.mean(mixed_vals, axis=-1, keepdims=True)
    group_scale = lax.rsqrt(jnp.mean(centred * centred, axis=-1, keepdims=True) + norm_eps)
    unit_h = centred * group_scale
    gate_sig = jax.nn.sigmoid(gate)
    gate_act = gate * gate_sig
    gated = join_heads((gate_act * unit_h).astype(BF))

    group = rows_in == 64 and sp_n == 4 and plane_n == 8
    fine = 16

    def parts_of(v, fine):
        v = v.reshape(sp_n, tok_count, width)
        main = lax.reduce_precision(v, 8, 7)
        rest = [v[:, :fine] - main[:, :fine]] if fine else []
        return jnp.concatenate([main] + rest, 1).astype(BF)

    down_rows = o_low[:, width:].reshape(2, -1, width)
    got, w_up, w_down = exchange(
        [("swap", parts_of(mm(gated, w_o), fine)), ("plane", up_rows), ("plane", down_rows)], sp_n, f_n, 4, 50
    )
    w_up, w_down = w_up.reshape(width, -1), w_down.reshape(-1, width)
    hidden, normed_b = row_call(
        functools.partial(ahead_kernel, group),
        "ahead",
        (got, got, own_x, gains),
        ("main", "lo", "row", "gains"),
        ((tok_count, F32), (tok_count, BF)),
        tok_count,
        width,
    )
    (b_low,) = exchange([("gather", normed_b if group else perm(normed_b))], sp_n, f_n, 5, 40)
    b_low = b_low.reshape(block_len, width)
    up = mm(b_low, w_up)
    act_low = jax.nn.gelu(up, approximate=False).astype(BF)
    ffn_part = mm(act_low, w_down).astype(BF)

    grad_act = mm_t(grad_ffn, w_down)
    density = (
        0.5 * (1.0 + lax.erf(up * root_half)) + up * jnp.exp(-0.5 * up * up) * inv_root_tau
    )
    grad_up = (grad_act * density).astype(BF)

    def reduce_rows(v):
        return lax.psum_scatter(v, PLANE, scatter_dimension=0, tiled=True)

    part_down = mm_tn(act_low, grad_ffn).astype(BF)
    part_up = mm_tn(b_low, grad_up).astype(BF)
    part_b = parts_of(mm_t(grad_up, w_up), fine)
    part_b, part_down, part_up = lax.optimization_barrier((part_b, part_down, part_up))
    sum_down = reduce_rows(part_down)
    ctx_own = lambda v: lax.dynamic_index_in_dim(v, ctx_i, 0, False).astype(F32)

    def core_sum(v, others):
        mine = lax.dynamic_index_in_dim(v, lax.axis_index("fsdp"), 1, False)
        return (mine.astype(F32) + jnp.sum(others.astype(F32), 0)).astype(BF)

    part_up = part_up.reshape(ctx_n, f_n, -1, part_up.shape[1])
    got, up_others = exchange(
        [("swap", part_b if group else unperm(part_b)), ("core", part_up)], sp_n, f_n, 6, 50
    )
    up_half = core_sum(part_up, up_others)
    grad_hidden, grad_branch, sums_b = row_call(
        functools.partial(turn_kernel, group),
        "turn",
        (got, got, hidden, grad_ffn_own, gains),
        ("main", "lo", "row", "row", "gains"),
        ((tok_count, F32), (tok_count, BF), (8, F32)),
        tok_count,
        width,
    )
    grad_branch, up_blocks = exchange([("gather", grad_branch), ("ctx_swap", up_half)], sp_n, f_n, 7, 40)
    grad_branch = grad_branch.reshape(block_len, width)
    sum_up = (ctx_own(up_half) + jnp.sum(up_blocks.astype(F32), 0)).astype(BF)
    ffn_part, grad_branch = lax.optimization_barrier((ffn_part, grad_branch))
    ffn = lax.psum_scatter(ffn_part, "sp", scatter_dimension=0, tiled=True)
    block_out = (hidden + ffn.astype(F32)).astype(BF).reshape(block_input.shape)
    part_o = mm_tn(gated, grad_branch).astype(BF)

    grad_gated = split_heads(mm_t(grad_branch, w_o), DV)
    grad_gate = (grad_gated * unit_h * gate_sig * (1.0 + gate * (1.0 - gate_sig))).astype(BF)
    grad_unit = grad_gated * gate_act
    grad_mixed = (
        group_scale
        * (
            grad_unit
            - jnp.mean(grad_unit, axis=-1, keepdims=True)
            - unit_h * jnp.mean(grad_unit * unit_h, axis=-1, keepdims=True)
        )
    ).astype(BF)
    grad_read = (grad_mixed * inward).astype(BF)
    own_reach = ein("hik,hiv->hkv", qs, grad_read).astype(BF)
    grad_gate = join_heads(grad_gate)
    grad_probs = ein("hiv,hjv->hij", grad_mixed, vs)
    grad_scores = (grad_probs * mask).astype(BF)
    grad_q = ein("hij,hjk->hik", grad_scores, ks) + ein("hiv,hkv->hik", grad_read, state)
    grad_gq = jnp.concatenate([grad_gate, join_heads(rotate(grad_q, cos_h, sin_h, -1.0).astype(BF))], 1)
    part_gq = mm_tn(a_low, grad_gq).astype(BF)
    own_reach, part_o, part_gq, sum_down = lax.optimization_barrier(
        (own_reach, part_o, part_gq, sum_down)
    )
    sum_gq = reduce_rows(part_gq)
    part_o = part_o.reshape(ctx_n, f_n, -1, width)

    def home(v):
        return v.reshape(sp_n, rows_in, -1)

    reaches, o_others, back_up = exchange(
        [("block", own_reach), ("core", part_o), ("swap", home(sum_up))], sp_n, f_n, 3, 25
    )
    o_half = core_sum(part_o, o_others)
    reaches = reaches.astype(F32)
    reach = jnp.sum(reaches * fore_w[:, :, None, None], 0).astype(BF)
    grad_k = ein("hij,hik->hjk", grad_scores, qs) + ein("hjv,hkv->hjk", vs, reach) * outward
    grad_v = ein("hij,hiv->hjv", probs, grad_mixed) + ein("hjk,hkv->hjv", key_decayed, reach)
    grad_kv = jnp.concatenate(
        [join_heads(rotate(grad_k, cos_h, sin_h, -1.0).astype(BF)), join_heads(grad_v.astype(BF))], 1
    )
    part_kv = mm_tn(a_low, grad_kv).astype(BF)
    grad_proj = jnp.concatenate([grad_gq[:, vd_w:], grad_kv, grad_gate], 1)
    part_a = parts_of(mm_t(grad_proj, w_proj), 0)
    part_a, part_kv = lax.optimization_barrier((part_a, part_kv))
    sum_kv = reduce_rows(part_kv)

    got, o_blocks = exchange(
        [("swap", part_a if group else unperm(part_a)), ("ctx_swap", o_half)], sp_n, f_n, 8, 50
    )
    sum_o = ctx_own(o_half) + jnp.sum(o_blocks.astype(F32), 0)
    grad_x, sums_a = row_call(
        functools.partial(last_kernel, group),
        "last",
        (got, own_x, grad_hidden, gains),
        ("main", "row", "row", "gains"),
        ((tok_count, BF), (8, F32)),
        tok_count,
        width,
    )
    grad_x = grad_x.reshape(block_input.shape)
    norm_terms = jnp.concatenate([sums_a[:2], sums_b[:2]], 0)
    norm_parts = norm_terms.reshape(4, n_dev, -1).swapaxes(0, 1)
    grad_gains = jnp.sum(all_swap(norm_parts, sp_n, f_n, 9), 0)
    back_gq, back_kv = exchange([("swap", home(sum_gq)), ("swap", home(sum_kv))], sp_n, f_n, 10, 38)
    parts = [back_gq[:, :, vd_w:], back_kv[:, :, :qk_w], back_kv[:, :, qk_w:], back_gq[:, :, :vd_w], back_up]
    grad_first = jnp.concatenate(
        [p.swapaxes(0, 1).reshape(rows_in, -1) for p in parts], 1
    ).astype(F32)
    grad_second = jnp.concatenate([sum_o, sum_down.astype(F32)], 1)
    first_m, first_v, first_step = adam_update(weight_in, grad_first, moment_in, square_in)
    second_m, second_v, second_step = adam_update(weight_out, grad_second, moment_out, square_out)
    gain_m, gain_v, gain_step = adam_update(norm_gains, grad_gains, moment_norm, square_norm)
    return (
        block_out,
        grad_x,
        grad_first,
        first_m,
        first_v,
        first_step,
        grad_second,
        second_m,
        second_v,
        second_step,
        grad_gains,
        gain_m,
        gain_v,
        gain_step,
    )


def solution(mesh):
    tokens = P("fsdp", "ctx", "sp", None)
    rows = P(ALL, None)
    cols = P(None, ALL)
    in_specs = (tokens, tokens, P(), rows, rows, cols, rows, rows, rows, rows, cols, cols)
    out_specs = (tokens, tokens) + (rows,) * 8 + (cols,) * 4
    return jax.shard_map(shards, mesh=mesh, in_specs=in_specs, out_specs=out_specs, check_vma=False)
```

```python
import functools
import math

import jax
import jax.numpy as jnp
from jax import lax
from jax.experimental import pallas as pl
from jax.experimental.pallas import tpu as pltpu
from jax.sharding import PartitionSpec as P

H = 8
DK = 256
DV = 512
SPAN = 512
STEP = 10
QK = 2048
VD = 4096

beta_one = 0.9
beta_two = 0.95
learn_rate = 0.01
decay_weight = 0.1
adam_eps = 1e-08
norm_eps = 1e-05
root_half = 0.7071067811865476
inv_root_tau = 0.3989422804014327


BF = jnp.bfloat16
F32 = jnp.float32
ALL = ("sp", "ctx", "fsdp")
PLANE = ("ctx", "fsdp")


def layer_stats(values, gain_row, shift_row):
    centred = values - jnp.mean(values, axis=-1, keepdims=True)
    inv_std = lax.rsqrt(jnp.mean(centred * centred, axis=-1, keepdims=True) + norm_eps)
    unit_vals = centred * inv_std
    return (unit_vals * gain_row + shift_row, unit_vals, inv_std)


def layer_back(grad_vals, unit_vals, inv_std, gain_row):
    scaled = grad_vals * gain_row
    return inv_std * (
        scaled
        - jnp.mean(scaled, axis=-1, keepdims=True)
        - unit_vals * jnp.mean(scaled * unit_vals, axis=-1, keepdims=True)
    )


def angles(positions, head_size):
    half_size = head_size // 2
    inverse = jnp.exp(
        -math.log(10000.0) * (2.0 * jnp.arange(half_size, dtype=jnp.float32) / head_size)
    )
    phases = positions.astype(jnp.float32)[:, None] * inverse[None, :]
    return (jnp.cos(phases), jnp.sin(phases))


def rotate(values, cosine, sine, sign_flip):
    half_size = values.shape[-1] // 2
    first_half = values[..., :half_size]
    second_half = values[..., half_size:]
    return jnp.concatenate(
        [
            first_half * cosine - sign_flip * (second_half * sine),
            second_half * cosine + sign_flip * (first_half * sine),
        ],
        -1,
    )


def adam_update(weight, grad_vals, moment, square):
    moment_new = beta_one * moment + (1.0 - beta_one) * grad_vals
    square_new = beta_two * square + (1.0 - beta_two) * grad_vals * grad_vals
    moment_hat = moment_new / (1.0 - beta_one**STEP)
    square_hat = square_new / (1.0 - beta_two**STEP)
    step_vals = -learn_rate * (
        moment_hat / (jnp.sqrt(square_hat) + adam_eps) + decay_weight * weight
    )
    return (moment_new, square_new, step_vals)


def mm(a, b):
    return jnp.dot(a, b, preferred_element_type=F32)


def mm_t(a, b):
    return lax.dot_general(a, b, (((1,), (1,)), ((), ())), preferred_element_type=F32)


def mm_tn(a, b):
    return lax.dot_general(a, b, (((0,), (0,)), ((), ())), preferred_element_type=F32)


def ein(spec, a, b):
    return jnp.einsum(spec, a, b, preferred_element_type=F32)


MESH_ID = pl.DeviceIdType.MESH
ANY = pl.BlockSpec(memory_space=pl.ANY)
VM = pl.BlockSpec(memory_space=pltpu.VMEM)


def greet(peers):
    sem = pltpu.get_barrier_semaphore()
    for peer in peers:
        pl.semaphore_signal(sem, inc=1, device_id=peer, device_id_type=MESH_ID)
    pl.semaphore_wait(sem, len(peers))


def push(src, dst, send, recv, peer):
    copy = pltpu.make_async_remote_copy(
        src_ref=src, dst_ref=dst, send_sem=send, recv_sem=recv, device_id=peer, device_id_type=MESH_ID
    )
    copy.start()
    return copy


def arrived(dst, send, recv, peer):
    pltpu.make_async_remote_copy(
        src_ref=dst, dst_ref=dst, send_sem=send, recv_sem=recv, device_id=peer, device_id_type=MESH_ID
    ).wait_recv()


def beside(c):
    low = c + 1 - 2 * (c % 2)
    high = (c + 2) % 4
    return low, high, (low + 2) % 4


def cost(micros):
    return pl.CostEstimate(flops=0, transcendentals=0, bytes_accessed=int(micros * 3.0e6))


def along(s, n):
    if n == 4:
        return [s, s + 1 - 2 * (s % 2), (s + 2) % 4, 3 - s]
    return [lax.rem(s + j, n) for j in range(n)]


def params(ident):
    return pltpu.CompilerParams(collective_id=ident, has_side_effects=True)


def others(s, c, f, sp_n, f_n):
    ids, flat = [], []
    for a in range(sp_n):
        for b in range(4):
            for d in range(f_n):
                if a or b or d:
                    p, q, r = lax.rem(s + a, sp_n), lax.rem(c + b, 4), lax.rem(f + d, f_n)
                    ids.append({"sp": p, "ctx": q, "fsdp": r})
                    flat.append((p * 4 + q) * f_n + r)
    return ids, flat


def spread_kernel(sp_n, f_n, wp_in, wo_in, x_in, g_in, wp, wo, x, g, gs, gr, lsem, zs, zr, xs, xr, ps, pr, cs, cr):
    s, c, f = lax.axis_index("sp"), lax.axis_index("ctx"), lax.axis_index("fsdp")
    low, high, both = beside(c)
    lines = along(s, sp_n)
    cores = [lax.rem(f + k, f_n) for k in range(1, f_n)]
    here = (s * 4 + c) * f_n + f
    ids, flat = others(s, c, f, sp_n, f_n)
    greet(ids)
    n_items = sp_n + 1
    waits = []

    def item_at(i, cc, ff):
        return wp.at[cc, ff, lines[i - 1]] if i else wo.at[cc, ff]

    def key(i):
        return 1 + lines[i - 1] if i else 0

    def start_local(n, src, dst):
        copy = pltpu.make_async_copy(src, dst, lsem.at[n])
        copy.start()
        return copy

    for n, p in enumerate(ids):
        waits.append(push(g_in, g.at[here], gs.at[n], gr.at[here], p))
    for j in range(1, sp_n):
        waits.append(push(wp_in.at[lines[j]], wp.at[c, f, s], zs.at[j], zr.at[s], {"sp": lines[j]}))
    up_ok, down_ok = s + 1 < sp_n, s > 0

    def x_copy(slot, way, peer, first):
        return pltpu.make_async_remote_copy(
            src_ref=x_in if first else x.at[slot],
            dst_ref=x.at[slot],
            send_sem=xs.at[way * sp_n + slot],
            recv_sem=xr.at[slot],
            device_id={"sp": peer},
            device_id_type=MESH_ID,
        )

    def x_out(k, act):
        @pl.when((s - k >= 0) & up_ok)
        def _():
            act(x_copy(s - k, 0, s + 1, k == 0))

        @pl.when((s + k < sp_n) & down_ok)
        def _():
            act(x_copy(s + k, 1, s - 1, k == 0))

    def x_step(k):
        @pl.when(s - 1 - k >= 0)
        def _():
            x_copy(s - 1 - k, 0, s - 1, False).wait_recv()

        @pl.when(s + 1 + k < sp_n)
        def _():
            x_copy(s + 1 + k, 1, s + 1, False).wait_recv()

        if k + 1 < sp_n - 1:
            x_out(k + 1, lambda d: d.start())

    x_out(0, lambda d: d.start())
    own = (wo_in, wp_in.at[s])
    local = [start_local(i, own[i], item_at(i, c, f)) for i in range(2)]
    local.append(start_local(2, x_in, x.at[s]))
    local.append(start_local(3, g_in, g.at[here]))

    def to_cores(i, src, cc):
        for n, p in enumerate(cores):
            waits.append(
                push(
                    src,
                    item_at(i, cc, f),
                    cs.at[(n * 4 + cc) * n_items + i],
                    cr.at[(f * 4 + cc) * n_items + key(i)],
                    {"fsdp": p},
                )
            )

    def first(i):
        if i < 2:
            src = own[i]
        else:
            src = item_at(i, c, f)
            arrived(src, zs.at[0], zr.at[lines[i - 1]], {"sp": lines[i - 1]})
        for n, p in enumerate((low, high)):
            waits.append(
                push(src, item_at(i, c, f), ps.at[3 * i + n], pr.at[c * n_items + key(i)], {"ctx": p})
            )
        to_cores(i, src, c)

    def landed(i, cc):
        arrived(item_at(i, cc, f), ps.at[0], pr.at[cc * n_items + key(i)], {"ctx": cc})

    def second(i):
        for n, (came, goes) in enumerate(((low, high), (high, low))):
            landed(i, came)
            at = item_at(i, came, f)
            if i % 2 == n:
                waits.append(push(at, at, ps.at[3 * i + 2], pr.at[came * n_items + key(i)], {"ctx": goes}))
            to_cores(i, at, came)

    def third(i):
        landed(i, both)
        to_cores(i, item_at(i, both, f), both)

    for i in range(n_items + 2):
        if i < n_items:
            first(i)
        if 1 <= i < n_items + 1:
            second(i - 1)
        if i >= 2:
            third(i - 2)
        if i == n_items - 1:
            x_step(0)
    for k in range(1, sp_n - 1):
        x_step(k)
    for k in range(sp_n - 1):
        x_out(k, lambda d: d.wait_send())
    for p in cores:
        for cc in range(4):
            for i in range(n_items):
                arrived(item_at(i, cc, p), cs.at[0], cr.at[(p * 4 + cc) * n_items + key(i)], {"fsdp": p})
    for k, p in zip(flat, ids):
        arrived(g.at[k], gs.at[0], gr.at[k], p)
    for copy in waits:
        copy.wait_send()
    for copy in local:
        copy.wait()


def spread(wp_in, wo_in, x_in, g_in, sp_n, f_n, ident):
    n_items, n_dev = sp_n + 1, sp_n * 4 * f_n
    shapes = [
        (4, f_n) + wp_in.shape,
        (4, f_n) + wo_in.shape,
        (sp_n,) + x_in.shape,
        (n_dev,) + g_in.shape,
    ]
    dma = pltpu.SemaphoreType.DMA
    return pl.pallas_call(
        functools.partial(spread_kernel, sp_n, f_n),
        out_shape=[jax.ShapeDtypeStruct(v, BF) for v in shapes],
        in_specs=[VM] * 4,
        out_specs=[ANY] * 4,
        scratch_shapes=[
            dma((n_dev,)),
            dma((n_dev,)),
            dma((4,)),
            dma((sp_n,)),
            dma((sp_n,)),
            dma((2 * sp_n,)),
            dma((sp_n,)),
            dma((3 * n_items,)),
            dma((4 * n_items,)),
            dma(((f_n - 1) * 4 * n_items,)),
            dma((f_n * 4 * n_items,)),
        ],
        compiler_params=params(ident),
        cost_estimate=cost(85),
        name="spread",
    )(wp_in, wo_in, x_in, g_in)


def exchange_kernel(plan, sp_n, f_n, *refs):
    m = len(plan)
    ins, outs, (ls, ss, rs) = refs[:m], refs[m : 2 * m], refs[2 * m :]
    s, c, f = lax.axis_index("sp"), lax.axis_index("ctx"), lax.axis_index("fsdp")
    low, high, both = beside(c)
    line = along(s, sp_n)[1:]
    cores = [lax.rem(f + k, f_n) for k in range(1, f_n)]
    kinds = set(plan)
    here = (s * 4 + c) * f_n + f
    ids, flat = others(s, c, f, sp_n, f_n)
    peers = []
    if kinds & {"swap", "gather"}:
        peers += [{"sp": p} for p in line]
    if kinds & {"ctx_swap"}:
        peers += [{"ctx": p} for p in (low, high, both)]
    elif kinds & {"block", "plane"}:
        peers += [{"ctx": p} for p in (low, high)]
    if kinds & {"core", "plane"}:
        peers += [{"fsdp": p} for p in cores]
    greet(ids if "all" in kinds else peers)
    sends, local, steps, ends = [], [], [], []
    used = [0, 0, 0]

    def take(k, n):
        used[k] += n
        return used[k] - n

    def send(src, dst, r, peer):
        sends.append(push(src, dst, ss.at[take(1, 1)], rs.at[r], peer))

    def keep(src, dst):
        copy = pltpu.make_async_copy(src, dst, ls.at[take(0, 1)])
        copy.start()
        local.append(copy)

    def got(dst, r, peer):
        arrived(dst, ss.at[0], rs.at[r], peer)

    def swap(x, o):
        r = take(2, sp_n)
        for p in line:
            send(x.at[p], o.at[s], r + s, {"sp": p})
        keep(x.at[s], o.at[s])
        ends.append(lambda: [got(o.at[p], r + p, {"sp": p}) for p in line])

    def every(x, o):
        r = take(2, len(ids) + 1)
        for k, p in zip(flat, ids):
            send(x.at[k], o.at[here], r + here, p)
        keep(x.at[here], o.at[here])
        ends.append(lambda: [got(o.at[k], r + k, p) for k, p in zip(flat, ids)])

    def ctx_swap(x, o):
        r = take(2, 3)
        for p in (low, high, both):
            k = lax.rem(c - p + 4, 4) - 1
            send(x.at[p], o.at[k], r + k, {"ctx": p})
        ends.append(lambda: [got(o.at[k], r + k, {"ctx": low}) for k in range(3)])

    def core(x, o):
        r = take(2, f_n - 1)
        for p in cores:
            k = lax.rem(f - p + f_n, f_n) - 1
            send(x.at[:, p], o.at[k], r + k, {"fsdp": p})
        ends.append(lambda: [got(o.at[k], r + k, {"fsdp": cores[0]}) for k in range(f_n - 1)])

    def plane(x, o, wide):
        n = x.shape[0]
        r, rc = take(2, 4 * n), take(2, f_n * 4 * n) if wide else 0
        at = lambda cc, ff, i: o.at[cc, ff, i] if wide else o.at[cc, i]

        def across(src, cc, i):
            if wide:
                for p in cores:
                    send(src, at(cc, f, i), rc + (f * 4 + cc) * n + i, {"fsdp": p})

        for i in range(n):
            for p in (low, high):
                send(x.at[i], at(c, f, i), r + c * n + i, {"ctx": p})
            across(x.at[i], c, i)
        keep(x, o.at[c, f] if wide else o.at[c])

        def near(i):
            for k, (came, goes) in enumerate(((low, high), (high, low))):
                got(at(came, f, i), r + came * n + i, {"ctx": came})
                if i % 2 == k:
                    send(at(came, f, i), at(came, f, i), r + came * n + i, {"ctx": goes})
                across(at(came, f, i), came, i)

        def far(i):
            got(at(both, f, i), r + both * n + i, {"ctx": both})
            across(at(both, f, i), both, i)

        def close():
            for p in cores if wide else ():
                for cc in range(4):
                    for i in range(n):
                        got(at(cc, p, i), rc + (p * 4 + cc) * n + i, {"fsdp": p})

        steps.extend([functools.partial(near, i) for i in range(n)])
        steps.extend([functools.partial(far, i) for i in range(n)])
        ends.append(close)

    def gather(x, o):
        n = sp_n
        r, q = take(2, n), take(1, 2 * n)
        up_ok, down_ok = s + 1 < n, s > 0

        def desc(slot, way, peer, first):
            return pltpu.make_async_remote_copy(
                src_ref=x if first else o.at[slot],
                dst_ref=o.at[slot],
                send_sem=ss.at[q + way * n + slot],
                recv_sem=rs.at[r + slot],
                device_id={"sp": peer},
                device_id_type=MESH_ID,
            )

        def out_going(k, act):
            @pl.when((s - k >= 0) & up_ok)
            def _():
                act(desc(s - k, 0, s + 1, k == 0))

            @pl.when((s + k < n) & down_ok)
            def _():
                act(desc(s + k, 1, s - 1, k == 0))

        def incoming(k):
            @pl.when(s - 1 - k >= 0)
            def _():
                desc(s - 1 - k, 0, s - 1, False).wait_recv()

            @pl.when(s + 1 + k < n)
            def _():
                desc(s + 1 + k, 1, s + 1, False).wait_recv()

        def step(k):
            incoming(k)
            if k + 1 < n - 1:
                out_going(k + 1, lambda d: d.start())

        def close():
            for k in range(n - 1):
                out_going(k, lambda d: d.wait_send())

        out_going(0, lambda d: d.start())
        keep(x, o.at[s])
        steps.extend([functools.partial(step, k) for k in range(n - 1)])
        ends.append(close)

    for kind, x, o in zip(plan, ins, outs):
        if kind == "swap":
            swap(x, o)
        elif kind == "all":
            every(x, o)
        elif kind == "ctx_swap":
            ctx_swap(x, o)
        elif kind == "core":
            core(x, o)
        elif kind == "gather":
            gather(x, o)
        else:
            plane(x, o, kind == "plane")
    for step in steps:
        step()
    for end in ends:
        end()
    for copy in sends:
        copy.wait_send()
    for copy in local:
        copy.wait()


def exchange(ops, sp_n, f_n, ident, micros):
    plan = tuple(kind for kind, _ in ops)
    outs, n_send, n_recv = [], 0, 0
    for kind, x in ops:
        n = x.shape[0]
        if kind == "swap":
            shape, a, b = x.shape, sp_n - 1, sp_n
        elif kind == "all":
            shape, a, b = x.shape, n, n
        elif kind == "ctx_swap":
            shape, a, b = (3,) + x.shape[1:], 3, 3
        elif kind == "core":
            shape, a, b = (f_n - 1, x.shape[0]) + x.shape[2:], f_n - 1, f_n - 1
        elif kind == "gather":
            shape, a, b = (sp_n,) + x.shape, 2 * sp_n, sp_n
        elif kind == "block":
            shape, a, b = (4,) + x.shape, 3 * n, 4 * n
        else:
            shape, a, b = (4, f_n) + x.shape, 3 * n + 4 * n * (f_n - 1), 4 * n * (f_n + 1)
        outs.append(jax.ShapeDtypeStruct(shape, x.dtype))
        n_send, n_recv = n_send + a, n_recv + b
    dma = pltpu.SemaphoreType.DMA
    far = ("core", "ctx_swap")
    return pl.pallas_call(
        functools.partial(exchange_kernel, plan, sp_n, f_n),
        out_shape=outs,
        in_specs=[ANY if kind in far else VM for kind in plan],
        out_specs=[ANY if kind in far + ("plane",) else VM for kind in plan],
        scratch_shapes=[dma((len(ops),)), dma((n_send,)), dma((n_recv,))],
        compiler_params=params(ident),
        cost_estimate=cost(micros),
        name="exchange_" + "_".join(plan),
    )(*[x for _, x in ops])


def regroup(v, back):
    lane = lax.broadcasted_iota(jnp.int32, (v.shape[0], 128), 1) < 64
    piece = lambda k: v[:, 128 * k : 128 * k + 128]
    turn = lambda p: pltpu.roll(p, 64, 1)
    out = []
    for k in range(v.shape[1] // 128):
        if back:
            s, pair = k // 4, k % 4
            a, b, odd = 4 * pair + s // 2, 4 * pair + 2 + s // 2, s % 2
        else:
            cf, half = k // 2, k % 2
            a, b, odd = 8 * half + cf // 2, 8 * half + 4 + cf // 2, cf % 2
        if odd:
            out.append(jnp.where(lane, turn(piece(a)), piece(b)))
        else:
            out.append(jnp.where(lane, piece(a), turn(piece(b))))
    return jnp.concatenate(out, 1)


def added(main, lo):
    total = main[0].astype(F32)
    for k in range(1, main.shape[0]):
        total = total + main[k].astype(F32)
    if lo is not None:
        rest = lo[0].astype(F32)
        for k in range(1, lo.shape[0]):
            rest = rest + lo[k].astype(F32)
        total = total + jnp.where(pl.program_id(0) == 0, 1.0, 0.0) * rest
    return total


def tally(sums, grads, unit):
    @pl.when(pl.program_id(0) == 0)
    def _():
        sums[...] = jnp.zeros_like(sums)

    sums[0:1, :] += jnp.sum(grads * unit, 0, keepdims=True)
    sums[1:2, :] += jnp.sum(grads, 0, keepdims=True)


def ahead_kernel(group, main, lo, x, gains, hidden_out, bn_out):
    hidden = x[...].astype(F32) + added(main, lo)
    hidden_out[...] = hidden
    normed, _, _ = layer_stats(hidden, gains[2:3, :], gains[3:4, :])
    bn_out[...] = (regroup(normed, False) if group else normed).astype(BF)


def turn_kernel(group, main, lo, hidden, cot, gains, dh_out, dbr_out, sums):
    grads = added(main, lo)
    grads = regroup(grads, True) if group else grads
    _, unit, scale = layer_stats(hidden[...], gains[2:3, :], gains[3:4, :])
    dh = cot[...].astype(F32) + layer_back(grads, unit, scale, gains[2:3, :])
    dh_out[...] = dh
    dbr_out[...] = dh.astype(BF)
    tally(sums, grads, unit)


def last_kernel(group, main, x, dh, gains, gx_out, sums):
    grads = added(main, None)
    grads = regroup(grads, True) if group else grads
    _, unit, scale = layer_stats(x[...].astype(F32), gains[0:1, :], gains[1:2, :])
    gx_out[...] = (dh[...] + layer_back(grads, unit, scale, gains[0:1, :])).astype(BF)
    tally(sums, grads, unit)


def row_call(kernel, name, args, kinds, outs, rows, width, tile=16):
    n = args[0].shape[0]
    specs = {
        "main": pl.BlockSpec((n, tile, width), lambda i: (0, i, 0)),
        "lo": pl.BlockSpec((n, tile, width), lambda i: (0, rows // tile, 0)),
        "row": pl.BlockSpec((tile, width), lambda i: (i, 0)),
        "gains": pl.BlockSpec((4, width), lambda i: (0, 0)),
        "sums": pl.BlockSpec((8, width), lambda i: (0, 0)),
    }
    return pl.pallas_call(
        kernel,
        grid=(rows // tile,),
        in_specs=[specs[k] for k in kinds],
        out_specs=[specs["sums" if h == 8 else "row"] for h, _ in outs],
        out_shape=[jax.ShapeDtypeStruct((h, width), t) for h, t in outs],
        cost_estimate=cost(4),
        name=name,
    )(*args)


def first_kernel(x, gains, out):
    normed, _, _ = layer_stats(x[...].astype(F32), gains[0:1, :], gains[1:2, :])
    out[...] = normed.astype(BF)


def turned(x, cos, sin, sign):
    half = x.shape[1] // 2
    a, b = x[:, :half], x[:, half:]
    return jnp.concatenate([a * cos - sign * (b * sin), b * cos + sign * (a * sin)], 1)


def heads_kernel(q, k, v, cos, sin, outw, qs, ks, vs, kw, own):
    qs[0] = turned(q[...], cos[...], sin[...], 1.0).astype(BF)
    key = turned(k[...], cos[...], sin[...], 1.0).astype(BF)
    val = v[...].astype(BF)
    late = (key.astype(F32) * outw[0]).astype(BF)
    ks[0], vs[0], kw[0] = key, val, late
    own[0] = mm_tn(late, val).astype(BF)


def weighted(parts, weights):
    h = pl.program_id(0)
    total = parts[0, 0].astype(F32) * weights[0, h]
    for k in range(1, parts.shape[0]):
        total = total + parts[k, 0].astype(F32) * weights[k, h]
    return total.astype(BF)


def unit_of(mixed):
    vals = mixed.astype(F32)
    centred = vals - jnp.mean(vals, axis=-1, keepdims=True)
    scale = lax.rsqrt(jnp.mean(centred * centred, axis=-1, keepdims=True) + norm_eps)
    return centred * scale, scale


def retain_kernel(weights, states, qs, ks, vs, gate, mask, inw, state_out, probs_out, mixed_out, gated):
    state = weighted(states, weights)
    state_out[0] = state
    probs = (mm_t(qs[0], ks[0]) * mask[0]).astype(BF)
    probs_out[0] = probs
    mixed = (mm(probs, vs[0]) + mm(qs[0], state) * inw[0]).astype(BF)
    mixed_out[0] = mixed
    unit, _ = unit_of(mixed)
    pre = gate[...]
    gated[...] = (pre * jax.nn.sigmoid(pre) * unit).astype(BF)


def back_kernel(grads, gate, mixed, qs, ks, vs, state, mask, inw, cos, sin, dgate, dos_out, reach, dsc_out, dq):
    unit, scale = unit_of(mixed[0])
    pre, g = gate[...], grads[...]
    sig = jax.nn.sigmoid(pre)
    dgate[...] = (g * unit * sig * (1.0 + pre * (1.0 - sig))).astype(BF)
    gu = g * (pre * sig)
    lean = jnp.mean(gu * unit, axis=-1, keepdims=True)
    dos = (scale * (gu - jnp.mean(gu, axis=-1, keepdims=True) - unit * lean)).astype(BF)
    dos_out[0] = dos
    read = (dos.astype(F32) * inw[0]).astype(BF)
    reach[0] = mm_tn(qs[0], read).astype(BF)
    dsc = (mm_t(dos, vs[0]) * mask[0]).astype(BF)
    dsc_out[0] = dsc
    dq[...] = turned(mm(dsc, ks[0]) + mm_t(read, state[0]), cos[...], sin[...], -1.0).astype(BF)


def later_kernel(weights, reaches, dsc, qs, vs, probs, dos, kw, outw, cos, sin, dk, dv):
    after = weighted(reaches, weights)
    grad = mm_tn(dsc[0], qs[0]) + mm_t(vs[0], after) * outw[0]
    dk[...] = turned(grad, cos[...], sin[...], -1.0).astype(BF)
    dv[...] = (mm_tn(probs[0], dos[0]) + mm(kw[0], after)).astype(BF)


def head_call(kernel, name, heads, args, specs, outs):
    def spec(v, k):
        if k == "scalar":
            return pl.BlockSpec(memory_space=pltpu.SMEM)
        if k == "all":
            return pl.BlockSpec(v.shape, lambda h: (0,) * len(v.shape))
        if k == "head":
            return pl.BlockSpec((1,) + v.shape[1:], lambda h: (h, 0, 0))
        if k == "parts":
            return pl.BlockSpec((v.shape[0], 1) + v.shape[2:], lambda h: (0, h, 0, 0))
        size, first = k
        return pl.BlockSpec((v.shape[0], size), lambda h: (0, first + h))

    outs = [(jax.ShapeDtypeStruct(shape, BF), k) for shape, k in outs]
    return pl.pallas_call(
        kernel,
        grid=(heads,),
        in_specs=[spec(v, k) for v, k in zip(args, specs)],
        out_specs=[spec(v, k) for v, k in outs],
        out_shape=[v for v, _ in outs],
        cost_estimate=cost(5),
        name=name,
    )(*args)


def shards(
    block_input,
    cotangent,
    decay_rate,
    weight_in,
    weight_out,
    norm_gains,
    moment_in,
    square_in,
    moment_out,
    square_out,
    moment_norm,
    square_norm,
):
    tok_count = block_input.shape[2]
    width = block_input.shape[3]
    sp_n = lax.axis_size("sp")
    ctx_n, f_n = lax.axis_size("ctx"), lax.axis_size("fsdp")
    plane_n = ctx_n * f_n
    heads = H // sp_n
    block_len = tok_count * sp_n
    sp_i = lax.axis_index("sp")
    ctx_i = lax.axis_index("ctx")
    rows_in = weight_in.shape[0]
    qk_w, vd_w = QK // sp_n, VD // sp_n
    widths = (qk_w, qk_w, vd_w, vd_w, vd_w)
    starts = (0, QK, 2 * QK, 2 * QK + VD, 2 * QK + 2 * VD)
    cut = 2 * qk_w + 2 * vd_w

    def perm(v):
        return v.reshape(-1, sp_n, plane_n, rows_in).swapaxes(1, 2).reshape(v.shape)

    def unperm(v):
        return v.reshape(-1, plane_n, sp_n, rows_in).swapaxes(1, 2).reshape(v.shape)

    w_low = weight_in.astype(BF)
    slabs = jnp.concatenate(
        [w_low[:, o : o + sp_n * w].reshape(rows_in, sp_n, w) for o, w in zip(starts, widths)], 2
    )
    slabs = slabs.swapaxes(0, 1)
    o_low = weight_out.astype(BF)
    own_x = block_input.reshape(tok_count, width)
    own_xp = perm(own_x)
    n_dev = sp_n * plane_n
    w_proj, w_o, full_x, gains = spread(
        slabs[:, :, :cut], o_low[:, :width], own_xp, norm_gains.astype(BF), sp_n, f_n, 0
    )
    w_proj, w_o = w_proj.reshape(width, -1), w_o.reshape(-1, width)
    full_x = full_x.reshape(-1, width)
    gains = gains.swapaxes(0, 1).reshape(4, width).astype(F32)
    gains_p = perm(gains)

    grad_ffn_own = cotangent.reshape(tok_count, width)
    held_cot, full_x = lax.optimization_barrier((grad_ffn_own, full_x))
    grad_ffn = lax.all_gather(held_cot, "sp", axis=0, tiled=True)
    (a_low,) = row_call(
        first_kernel, "first", (full_x, gains_p), ("row", "gains"), ((block_len, BF),), block_len, width, 64
    )
    proj = mm(a_low, w_proj)
    head_pos = ctx_i * block_len + jnp.arange(block_len, dtype=jnp.int32)
    cos_h, sin_h = angles(head_pos, DK)

    rates = lax.dynamic_slice_in_dim(decay_rate, sp_i * heads, heads)
    offs = jnp.arange(block_len, dtype=F32)
    spacing = offs[:, None] - offs[None, :]
    mask = jnp.where(
        spacing[None] >= 0.0, jnp.exp(-rates[:, None, None] * jnp.maximum(spacing, 0.0)[None]), 0.0
    )
    inward = jnp.exp(-rates[:, None] * (offs[None, :] + 1.0))[:, :, None]
    outward = jnp.exp(-rates[:, None] * (block_len - 1.0 - offs[None, :]))[:, :, None]
    blocks = jnp.arange(ctx_n)
    back_gap = (ctx_i - 1 - blocks).astype(F32)
    back_w = jnp.where(
        blocks[:, None] < ctx_i,
        jnp.exp(-rates[None, :] * block_len * jnp.maximum(back_gap, 0.0)[:, None]),
        0.0,
    )
    fore_gap = (blocks - ctx_i - 1).astype(F32)
    fore_w = jnp.where(
        blocks[:, None] > ctx_i,
        jnp.exp(-rates[None, :] * block_len * jnp.maximum(fore_gap, 0.0)[:, None]),
        0.0,
    )

    wide, small = (heads, block_len, DV), (heads, block_len, DK)
    corner = (heads, DK, DV)
    qs, ks, vs, kw, own_state = head_call(
        heads_kernel,
        "heads",
        heads,
        (proj, proj, proj, cos_h, sin_h, outward),
        ((DK, 0), (DK, heads), (DV, heads), "all", "all", "head"),
        ((small, "head"), (small, "head"), (wide, "head"), (small, "head"), (corner, "head")),
    )
    states, up_rows = exchange(
        [("block", own_state), ("swap", slabs[:, :, cut:])], sp_n, f_n, 2, 25
    )
    gate_at = (DV, 2 * heads)
    square = (heads, block_len, block_len)
    state, probs, mixed, gated = head_call(
        retain_kernel,
        "retain",
        heads,
        (back_w, states, qs, ks, vs, proj, mask, inward),
        ("scalar", "parts", "head", "head", "head", gate_at, "head", "head"),
        ((corner, "head"), (square, "head"), (wide, "head"), ((block_len, vd_w), (DV, 0))),
    )
    group = rows_in == 64 and sp_n == 4 and plane_n == 8
    fine = 16

    def parts_of(v, fine):
        v = v.reshape(sp_n, tok_count, width)
        main = lax.reduce_precision(v, 8, 7)
        rest = [v[:, :fine] - main[:, :fine]] if fine else []
        return jnp.concatenate([main] + rest, 1).astype(BF)

    down_rows = o_low[:, width:].reshape(2, -1, width)
    got, w_up, w_down = exchange(
        [("swap", parts_of(mm(gated, w_o), fine)), ("plane", up_rows), ("plane", down_rows)], sp_n, f_n, 4, 50
    )
    w_up, w_down = w_up.reshape(width, -1), w_down.reshape(-1, width)
    hidden, normed_b = row_call(
        functools.partial(ahead_kernel, group),
        "ahead",
        (got, got, own_x, gains),
        ("main", "lo", "row", "gains"),
        ((tok_count, F32), (tok_count, BF)),
        tok_count,
        width,
    )
    (b_low,) = exchange([("gather", normed_b if group else perm(normed_b))], sp_n, f_n, 5, 40)
    b_low = b_low.reshape(block_len, width)
    up = mm(b_low, w_up)
    act_low = jax.nn.gelu(up, approximate=False).astype(BF)
    ffn_part = mm(act_low, w_down).astype(BF)

    grad_act = mm_t(grad_ffn, w_down)
    density = (
        0.5 * (1.0 + lax.erf(up * root_half)) + up * jnp.exp(-0.5 * up * up) * inv_root_tau
    )
    grad_up = (grad_act * density).astype(BF)

    def reduce_rows(v):
        return lax.psum_scatter(v, PLANE, scatter_dimension=0, tiled=True)

    part_down = mm_tn(act_low, grad_ffn).astype(BF)
    part_up = mm_tn(b_low, grad_up).astype(BF)
    part_b = parts_of(mm_t(grad_up, w_up), fine)
    part_b, part_down, part_up = lax.optimization_barrier((part_b, part_down, part_up))
    sum_down = reduce_rows(part_down)
    ctx_own = lambda v: lax.dynamic_index_in_dim(v, ctx_i, 0, False).astype(F32)

    def core_sum(v, others):
        mine = lax.dynamic_index_in_dim(v, lax.axis_index("fsdp"), 1, False)
        return (mine.astype(F32) + jnp.sum(others.astype(F32), 0)).astype(BF)

    part_up = part_up.reshape(ctx_n, f_n, -1, part_up.shape[1])
    got, up_others = exchange(
        [("swap", part_b if group else unperm(part_b)), ("core", part_up)], sp_n, f_n, 6, 50
    )
    up_half = core_sum(part_up, up_others)
    grad_hidden, grad_branch, sums_b = row_call(
        functools.partial(turn_kernel, group),
        "turn",
        (got, got, hidden, grad_ffn_own, gains),
        ("main", "lo", "row", "row", "gains"),
        ((tok_count, F32), (tok_count, BF), (8, F32)),
        tok_count,
        width,
    )
    grad_branch, up_blocks = exchange([("gather", grad_branch), ("ctx_swap", up_half)], sp_n, f_n, 7, 40)
    grad_branch = grad_branch.reshape(block_len, width)
    sum_up = (ctx_own(up_half) + jnp.sum(up_blocks.astype(F32), 0)).astype(BF)
    ffn_part, grad_branch = lax.optimization_barrier((ffn_part, grad_branch))
    ffn = lax.psum_scatter(ffn_part, "sp", scatter_dimension=0, tiled=True)
    block_out = (hidden + ffn.astype(F32)).astype(BF).reshape(block_input.shape)
    part_o = mm_tn(gated, grad_branch).astype(BF)

    grad_gate, grad_mixed, own_reach, grad_scores, grad_q = head_call(
        back_kernel,
        "back",
        heads,
        (mm_t(grad_branch, w_o), proj, mixed, qs, ks, vs, state, mask, inward, cos_h, sin_h),
        ((DV, 0), gate_at) + ("head",) * 7 + ("all", "all"),
        (
            ((block_len, vd_w), (DV, 0)),
            (wide, "head"),
            (corner, "head"),
            (square, "head"),
            ((block_len, qk_w), (DK, 0)),
        ),
    )
    grad_gq = jnp.concatenate([grad_gate, grad_q], 1)
    part_gq = mm_tn(a_low, grad_gq).astype(BF)
    own_reach, part_o, part_gq, sum_down = lax.optimization_barrier(
        (own_reach, part_o, part_gq, sum_down)
    )
    sum_gq = reduce_rows(part_gq)
    part_o = part_o.reshape(ctx_n, f_n, -1, width)

    def home(v):
        return v.reshape(sp_n, rows_in, -1)

    reaches, o_others, back_up = exchange(
        [("block", own_reach), ("core", part_o), ("swap", home(sum_up))], sp_n, f_n, 3, 25
    )
    o_half = core_sum(part_o, o_others)
    grad_k, grad_v = head_call(
        later_kernel,
        "later",
        heads,
        (fore_w, reaches, grad_scores, qs, vs, probs, grad_mixed, kw, outward, cos_h, sin_h),
        ("scalar", "parts") + ("head",) * 7 + ("all", "all"),
        (((block_len, qk_w), (DK, 0)), ((block_len, vd_w), (DV, 0))),
    )
    grad_kv = jnp.concatenate([grad_k, grad_v], 1)
    part_kv = mm_tn(a_low, grad_kv).astype(BF)
    grad_proj = jnp.concatenate([grad_gq[:, vd_w:], grad_kv, grad_gate], 1)
    part_a = parts_of(mm_t(grad_proj, w_proj), 0)
    part_a, part_kv = lax.optimization_barrier((part_a, part_kv))
    sum_kv = reduce_rows(part_kv)

    got, o_blocks = exchange(
        [("swap", part_a if group else unperm(part_a)), ("ctx_swap", o_half)], sp_n, f_n, 8, 50
    )
    sum_o = ctx_own(o_half) + jnp.sum(o_blocks.astype(F32), 0)
    grad_x, sums_a = row_call(
        functools.partial(last_kernel, group),
        "last",
        (got, own_x, grad_hidden, gains),
        ("main", "row", "row", "gains"),
        ((tok_count, BF), (8, F32)),
        tok_count,
        width,
    )
    grad_x = grad_x.reshape(block_input.shape)
    norm_terms = jnp.concatenate([sums_a[:2], sums_b[:2]], 0)
    norm_parts = norm_terms.reshape(4, n_dev, -1).swapaxes(0, 1)
    norm_sums, back_gq = exchange([("all", norm_parts), ("swap", home(sum_gq))], sp_n, f_n, 9, 20)
    grad_gains = jnp.sum(norm_sums, 0)
    (back_kv,) = exchange([("swap", home(sum_kv))], sp_n, f_n, 10, 22)
    parts = [back_gq[:, :, vd_w:], back_kv[:, :, :qk_w], back_kv[:, :, qk_w:], back_gq[:, :, :vd_w], back_up]
    grad_first = jnp.concatenate(
        [p.swapaxes(0, 1).reshape(rows_in, -1) for p in parts], 1
    ).astype(F32)
    grad_second = jnp.concatenate([sum_o, sum_down.astype(F32)], 1)
    first_m, first_v, first_step = adam_update(weight_in, grad_first, moment_in, square_in)
    second_m, second_v, second_step = adam_update(weight_out, grad_second, moment_out, square_out)
    gain_m, gain_v, gain_step = adam_update(norm_gains, grad_gains, moment_norm, square_norm)
    return (
        block_out,
        grad_x,
        grad_first,
        first_m,
        first_v,
        first_step,
        grad_second,
        second_m,
        second_v,
        second_step,
        grad_gains,
        gain_m,
        gain_v,
        gain_step,
    )


def solution(mesh):
    tokens = P("fsdp", "ctx", "sp", None)
    rows = P(ALL, None)
    cols = P(None, ALL)
    in_specs = (tokens, tokens, P(), rows, rows, cols, rows, rows, rows, rows, cols, cols)
    out_specs = (tokens, tokens) + (rows,) * 8 + (cols,) * 4
    return jax.shard_map(shards, mesh=mesh, in_specs=in_specs, out_specs=out_specs, check_vma=False)
```

```python
import functools
import math

import jax
import jax.numpy as jnp
from jax import lax
from jax.experimental import pallas as pl
from jax.experimental.pallas import tpu as pltpu
from jax.sharding import PartitionSpec as P

H = 8
DK = 256
DV = 512
SPAN = 512
STEP = 10
QK = 2048
VD = 4096

beta_one = 0.9
beta_two = 0.95
learn_rate = 0.01
decay_weight = 0.1
adam_eps = 1e-08
norm_eps = 1e-05
root_half = 0.7071067811865476
inv_root_tau = 0.3989422804014327


BF = jnp.bfloat16
F32 = jnp.float32
ALL = ("sp", "ctx", "fsdp")
PLANE = ("ctx", "fsdp")


def layer_stats(values, gain_row, shift_row):
    centred = values - jnp.mean(values, axis=-1, keepdims=True)
    inv_std = lax.rsqrt(jnp.mean(centred * centred, axis=-1, keepdims=True) + norm_eps)
    unit_vals = centred * inv_std
    return (unit_vals * gain_row + shift_row, unit_vals, inv_std)


def layer_back(grad_vals, unit_vals, inv_std, gain_row):
    scaled = grad_vals * gain_row
    return inv_std * (
        scaled
        - jnp.mean(scaled, axis=-1, keepdims=True)
        - unit_vals * jnp.mean(scaled * unit_vals, axis=-1, keepdims=True)
    )


def angles(positions, head_size):
    half_size = head_size // 2
    inverse = jnp.exp(
        -math.log(10000.0) * (2.0 * jnp.arange(half_size, dtype=jnp.float32) / head_size)
    )
    phases = positions.astype(jnp.float32)[:, None] * inverse[None, :]
    return (jnp.cos(phases), jnp.sin(phases))


def rotate(values, cosine, sine, sign_flip):
    half_size = values.shape[-1] // 2
    first_half = values[..., :half_size]
    second_half = values[..., half_size:]
    return jnp.concatenate(
        [
            first_half * cosine - sign_flip * (second_half * sine),
            second_half * cosine + sign_flip * (first_half * sine),
        ],
        -1,
    )


def adam_update(weight, grad_vals, moment, square):
    moment_new = beta_one * moment + (1.0 - beta_one) * grad_vals
    square_new = beta_two * square + (1.0 - beta_two) * grad_vals * grad_vals
    moment_hat = moment_new / (1.0 - beta_one**STEP)
    square_hat = square_new / (1.0 - beta_two**STEP)
    step_vals = -learn_rate * (
        moment_hat / (jnp.sqrt(square_hat) + adam_eps) + decay_weight * weight
    )
    return (moment_new, square_new, step_vals)


def mm(a, b):
    return jnp.dot(a, b, preferred_element_type=F32)


def mm_t(a, b):
    return lax.dot_general(a, b, (((1,), (1,)), ((), ())), preferred_element_type=F32)


def mm_tn(a, b):
    return lax.dot_general(a, b, (((0,), (0,)), ((), ())), preferred_element_type=F32)


def ein(spec, a, b):
    return jnp.einsum(spec, a, b, preferred_element_type=F32)


MESH_ID = pl.DeviceIdType.MESH
ANY = pl.BlockSpec(memory_space=pl.ANY)
VM = pl.BlockSpec(memory_space=pltpu.VMEM)


def greet(peers):
    sem = pltpu.get_barrier_semaphore()
    for peer in peers:
        pl.semaphore_signal(sem, inc=1, device_id=peer, device_id_type=MESH_ID)
    pl.semaphore_wait(sem, len(peers))


def push(src, dst, send, recv, peer):
    copy = pltpu.make_async_remote_copy(
        src_ref=src, dst_ref=dst, send_sem=send, recv_sem=recv, device_id=peer, device_id_type=MESH_ID
    )
    copy.start()
    return copy


def arrived(dst, send, recv, peer):
    pltpu.make_async_remote_copy(
        src_ref=dst, dst_ref=dst, send_sem=send, recv_sem=recv, device_id=peer, device_id_type=MESH_ID
    ).wait_recv()


def beside(c):
    low = c + 1 - 2 * (c % 2)
    high = (c + 2) % 4
    return low, high, (low + 2) % 4


def cost(micros):
    return pl.CostEstimate(flops=0, transcendentals=0, bytes_accessed=int(micros * 3.0e6))


def along(s, n):
    if n == 4:
        return [s, s + 1 - 2 * (s % 2), (s + 2) % 4, 3 - s]
    return [lax.rem(s + j, n) for j in range(n)]


def params(ident):
    return pltpu.CompilerParams(collective_id=ident, has_side_effects=True)


def others(s, c, f, sp_n, f_n):
    ids, flat = [], []
    for a in range(sp_n):
        for b in range(4):
            for d in range(f_n):
                if a or b or d:
                    p, q, r = lax.rem(s + a, sp_n), lax.rem(c + b, 4), lax.rem(f + d, f_n)
                    ids.append({"sp": p, "ctx": q, "fsdp": r})
                    flat.append((p * 4 + q) * f_n + r)
    return ids, flat


def spread_kernel(sp_n, f_n, wp_in, wo_in, x_in, g_in, wp, wo, x, g, gs, gr, lsem, zs, zr, xs, xr, ps, pr, cs, cr):
    s, c, f = lax.axis_index("sp"), lax.axis_index("ctx"), lax.axis_index("fsdp")
    low, high, both = beside(c)
    lines = along(s, sp_n)
    cores = [lax.rem(f + k, f_n) for k in range(1, f_n)]
    here = (s * 4 + c) * f_n + f
    ids, flat = others(s, c, f, sp_n, f_n)
    greet(ids)
    n_items = sp_n + 1
    waits = []

    def item_at(i, cc, ff):
        return wp.at[cc, ff, lines[i - 1]] if i else wo.at[cc, ff]

    def key(i):
        return 1 + lines[i - 1] if i else 0

    def start_local(n, src, dst):
        copy = pltpu.make_async_copy(src, dst, lsem.at[n])
        copy.start()
        return copy

    for n, p in enumerate(ids):
        waits.append(push(g_in, g.at[here], gs.at[n], gr.at[here], p))
    for j in range(1, sp_n):
        waits.append(push(wp_in.at[lines[j]], wp.at[c, f, s], zs.at[j], zr.at[s], {"sp": lines[j]}))
    for j in range(1, sp_n):
        waits.append(push(x_in, x.at[s], xs.at[j], xr.at[s], {"sp": lines[j]}))
    own = (wo_in, wp_in.at[s])
    local = [start_local(i, own[i], item_at(i, c, f)) for i in range(2)]
    local.append(start_local(2, x_in, x.at[s]))
    local.append(start_local(3, g_in, g.at[here]))

    def to_cores(i, src, cc):
        for n, p in enumerate(cores):
            waits.append(
                push(
                    src,
                    item_at(i, cc, f),
                    cs.at[(n * 4 + cc) * n_items + i],
                    cr.at[(f * 4 + cc) * n_items + key(i)],
                    {"fsdp": p},
                )
            )

    def first(i):
        if i < 2:
            src = own[i]
        else:
            src = item_at(i, c, f)
            arrived(src, zs.at[0], zr.at[lines[i - 1]], {"sp": lines[i - 1]})
        for n, p in enumerate((low, high)):
            waits.append(
                push(src, item_at(i, c, f), ps.at[3 * i + n], pr.at[c * n_items + key(i)], {"ctx": p})
            )
        to_cores(i, src, c)

    def landed(i, cc):
        arrived(item_at(i, cc, f), ps.at[0], pr.at[cc * n_items + key(i)], {"ctx": cc})

    def second(i):
        for n, (came, goes) in enumerate(((low, high), (high, low))):
            landed(i, came)
            at = item_at(i, came, f)
            if i % 2 == n:
                waits.append(push(at, at, ps.at[3 * i + 2], pr.at[came * n_items + key(i)], {"ctx": goes}))
            to_cores(i, at, came)

    def third(i):
        landed(i, both)
        to_cores(i, item_at(i, both, f), both)

    for i in range(n_items + 2):
        if i < n_items:
            first(i)
        if 1 <= i < n_items + 1:
            second(i - 1)
        if i >= 2:
            third(i - 2)
    for j in range(1, sp_n):
        arrived(x.at[lines[j]], xs.at[0], xr.at[lines[j]], {"sp": lines[j]})
    for p in cores:
        for cc in range(4):
            for i in range(n_items):
                arrived(item_at(i, cc, p), cs.at[0], cr.at[(p * 4 + cc) * n_items + key(i)], {"fsdp": p})
    for k, p in zip(flat, ids):
        arrived(g.at[k], gs.at[0], gr.at[k], p)
    for copy in waits:
        copy.wait_send()
    for copy in local:
        copy.wait()


def spread(wp_in, wo_in, x_in, g_in, sp_n, f_n, ident):
    n_items, n_dev = sp_n + 1, sp_n * 4 * f_n
    shapes = [
        (4, f_n) + wp_in.shape,
        (4, f_n) + wo_in.shape,
        (sp_n,) + x_in.shape,
        (n_dev,) + g_in.shape,
    ]
    dma = pltpu.SemaphoreType.DMA
    return pl.pallas_call(
        functools.partial(spread_kernel, sp_n, f_n),
        out_shape=[jax.ShapeDtypeStruct(v, BF) for v in shapes],
        in_specs=[VM] * 4,
        out_specs=[ANY] * 4,
        scratch_shapes=[
            dma((n_dev,)),
            dma((n_dev,)),
            dma((4,)),
            dma((sp_n,)),
            dma((sp_n,)),
            dma((sp_n,)),
            dma((sp_n,)),
            dma((3 * n_items,)),
            dma((4 * n_items,)),
            dma(((f_n - 1) * 4 * n_items,)),
            dma((f_n * 4 * n_items,)),
        ],
        compiler_params=params(ident),
        cost_estimate=cost(85),
        name="spread",
    )(wp_in, wo_in, x_in, g_in)


def exchange_kernel(plan, sp_n, f_n, *refs):
    m = len(plan)
    ins, outs, (ls, ss, rs) = refs[:m], refs[m : 2 * m], refs[2 * m :]
    s, c, f = lax.axis_index("sp"), lax.axis_index("ctx"), lax.axis_index("fsdp")
    low, high, both = beside(c)
    line = along(s, sp_n)[1:]
    cores = [lax.rem(f + k, f_n) for k in range(1, f_n)]
    kinds = set(plan)
    here = (s * 4 + c) * f_n + f
    ids, flat = others(s, c, f, sp_n, f_n)
    peers = []
    if kinds & {"swap", "gather", "lead"}:
        peers += [{"sp": p} for p in line]
    if kinds & {"ctx_swap"}:
        peers += [{"ctx": p} for p in (low, high, both)]
    elif kinds & {"block", "plane"}:
        peers += [{"ctx": p} for p in (low, high)]
    if kinds & {"core", "plane"}:
        peers += [{"fsdp": p} for p in cores]
    greet(ids if "all" in kinds else peers)
    sends, local, steps, ends = [], [], [], []
    used = [0, 0, 0]

    def take(k, n):
        used[k] += n
        return used[k] - n

    def send(src, dst, r, peer):
        sends.append(push(src, dst, ss.at[take(1, 1)], rs.at[r], peer))

    def keep(src, dst):
        copy = pltpu.make_async_copy(src, dst, ls.at[take(0, 1)])
        copy.start()
        local.append(copy)

    def got(dst, r, peer):
        arrived(dst, ss.at[0], rs.at[r], peer)

    def swap(x, o):
        r = take(2, sp_n)
        for p in line:
            send(x.at[p], o.at[s], r + s, {"sp": p})
        keep(x.at[s], o.at[s])
        ends.append(lambda: [got(o.at[p], r + p, {"sp": p}) for p in line])

    def every(x, o):
        r = take(2, len(ids) + 1)
        for k, p in zip(flat, ids):
            send(x.at[k], o.at[here], r + here, p)
        keep(x.at[here], o.at[here])
        ends.append(lambda: [got(o.at[k], r + k, p) for k, p in zip(flat, ids)])

    def ctx_swap(x, o):
        r = take(2, 3)
        for p in (low, high, both):
            k = lax.rem(c - p + 4, 4) - 1
            send(x.at[p], o.at[k], r + k, {"ctx": p})
        ends.append(lambda: [got(o.at[k], r + k, {"ctx": low}) for k in range(3)])

    def core(x, o):
        r = take(2, f_n - 1)
        for p in cores:
            k = lax.rem(f - p + f_n, f_n) - 1
            send(x.at[:, p], o.at[k], r + k, {"fsdp": p})
        ends.append(lambda: [got(o.at[k], r + k, {"fsdp": cores[0]}) for k in range(f_n - 1)])

    def plane(x, o, wide):
        n = x.shape[0]
        r, rc = take(2, 4 * n), take(2, f_n * 4 * n) if wide else 0
        at = lambda cc, ff, i: o.at[cc, ff, i] if wide else o.at[cc, i]

        def across(src, cc, i):
            if wide:
                for p in cores:
                    send(src, at(cc, f, i), rc + (f * 4 + cc) * n + i, {"fsdp": p})

        for i in range(n):
            for p in (low, high):
                send(x.at[i], at(c, f, i), r + c * n + i, {"ctx": p})
            across(x.at[i], c, i)
        keep(x, o.at[c, f] if wide else o.at[c])

        def near(i):
            for k, (came, goes) in enumerate(((low, high), (high, low))):
                got(at(came, f, i), r + came * n + i, {"ctx": came})
                if i % 2 == k:
                    send(at(came, f, i), at(came, f, i), r + came * n + i, {"ctx": goes})
                across(at(came, f, i), came, i)

        def far(i):
            got(at(both, f, i), r + both * n + i, {"ctx": both})
            across(at(both, f, i), both, i)

        def close():
            for p in cores if wide else ():
                for cc in range(4):
                    for i in range(n):
                        got(at(cc, p, i), rc + (p * 4 + cc) * n + i, {"fsdp": p})

        steps.extend([functools.partial(near, i) for i in range(n)])
        steps.extend([functools.partial(far, i) for i in range(n)])
        ends.append(close)

    def gather(x, o):
        n = sp_n
        r, q = take(2, n), take(1, 2 * n)
        up_ok, down_ok = s + 1 < n, s > 0

        def desc(slot, way, peer, first):
            return pltpu.make_async_remote_copy(
                src_ref=x if first else o.at[slot],
                dst_ref=o.at[slot],
                send_sem=ss.at[q + way * n + slot],
                recv_sem=rs.at[r + slot],
                device_id={"sp": peer},
                device_id_type=MESH_ID,
            )

        def out_going(k, act):
            @pl.when((s - k >= 0) & up_ok)
            def _():
                act(desc(s - k, 0, s + 1, k == 0))

            @pl.when((s + k < n) & down_ok)
            def _():
                act(desc(s + k, 1, s - 1, k == 0))

        def incoming(k):
            @pl.when(s - 1 - k >= 0)
            def _():
                desc(s - 1 - k, 0, s - 1, False).wait_recv()

            @pl.when(s + 1 + k < n)
            def _():
                desc(s + 1 + k, 1, s + 1, False).wait_recv()

        def step(k):
            incoming(k)
            if k + 1 < n - 1:
                out_going(k + 1, lambda d: d.start())

        def close():
            for k in range(n - 1):
                out_going(k, lambda d: d.wait_send())

        out_going(0, lambda d: d.start())
        keep(x, o.at[s])
        steps.extend([functools.partial(step, k) for k in range(n - 1)])
        ends.append(close)

    def lead(x, o):
        r, q = take(2, sp_n), take(1, 1)
        goes, comes = (c == 0) & (s > 0), (c == 0) & (s == 0)

        def desc(k):
            return pltpu.make_async_remote_copy(
                src_ref=x.at[0],
                dst_ref=o.at[k],
                send_sem=ss.at[q],
                recv_sem=rs.at[r + k],
                device_id={"sp": 0},
                device_id_type=MESH_ID,
            )

        @pl.when(goes)
        def _():
            desc(s).start()

        keep(x.at[0], o.at[0])

        def close():
            @pl.when(comes)
            def _():
                for k in range(1, sp_n):
                    desc(k).wait_recv()

            @pl.when(goes)
            def _():
                desc(s).wait_send()

        ends.append(close)

    for kind, x, o in zip(plan, ins, outs):
        if kind == "swap":
            swap(x, o)
        elif kind == "lead":
            lead(x, o)
        elif kind == "all":
            every(x, o)
        elif kind == "ctx_swap":
            ctx_swap(x, o)
        elif kind == "core":
            core(x, o)
        elif kind == "gather":
            gather(x, o)
        else:
            plane(x, o, kind == "plane")
    for step in steps:
        step()
    for end in ends:
        end()
    for copy in sends:
        copy.wait_send()
    for copy in local:
        copy.wait()


def exchange(ops, sp_n, f_n, ident, micros):
    plan = tuple(kind for kind, _ in ops)
    outs, n_send, n_recv = [], 0, 0
    for kind, x in ops:
        n = x.shape[0]
        if kind == "swap":
            shape, a, b = x.shape, sp_n - 1, sp_n
        elif kind == "lead":
            shape, a, b = x.shape, 1, sp_n
        elif kind == "all":
            shape, a, b = x.shape, n, n
        elif kind == "ctx_swap":
            shape, a, b = (3,) + x.shape[1:], 3, 3
        elif kind == "core":
            shape, a, b = (f_n - 1, x.shape[0]) + x.shape[2:], f_n - 1, f_n - 1
        elif kind == "gather":
            shape, a, b = (sp_n,) + x.shape, 2 * sp_n, sp_n
        elif kind == "block":
            shape, a, b = (4,) + x.shape, 3 * n, 4 * n
        else:
            shape, a, b = (4, f_n) + x.shape, 3 * n + 4 * n * (f_n - 1), 4 * n * (f_n + 1)
        outs.append(jax.ShapeDtypeStruct(shape, x.dtype))
        n_send, n_recv = n_send + a, n_recv + b
    dma = pltpu.SemaphoreType.DMA
    far = ("core", "ctx_swap")
    return pl.pallas_call(
        functools.partial(exchange_kernel, plan, sp_n, f_n),
        out_shape=outs,
        in_specs=[ANY if kind in far else VM for kind in plan],
        out_specs=[ANY if kind in far + ("plane",) else VM for kind in plan],
        scratch_shapes=[dma((len(ops),)), dma((n_send,)), dma((n_recv,))],
        compiler_params=params(ident),
        cost_estimate=cost(micros),
        name="exchange_" + "_".join(plan),
    )(*[x for _, x in ops])


def regroup(v, back):
    lane = lax.broadcasted_iota(jnp.int32, (v.shape[0], 128), 1) < 64
    piece = lambda k: v[:, 128 * k : 128 * k + 128]
    turn = lambda p: pltpu.roll(p, 64, 1)
    out = []
    for k in range(v.shape[1] // 128):
        if back:
            s, pair = k // 4, k % 4
            a, b, odd = 4 * pair + s // 2, 4 * pair + 2 + s // 2, s % 2
        else:
            cf, half = k // 2, k % 2
            a, b, odd = 8 * half + cf // 2, 8 * half + 4 + cf // 2, cf % 2
        if odd:
            out.append(jnp.where(lane, turn(piece(a)), piece(b)))
        else:
            out.append(jnp.where(lane, piece(a), turn(piece(b))))
    return jnp.concatenate(out, 1)


def added(main, lead):
    total = main[0].astype(F32)
    for k in range(1, main.shape[0]):
        total = total + main[k].astype(F32)
    if lead is not None:
        lo, begins = lead
        rest = lo[0].astype(F32)
        for k in range(1, lo.shape[0]):
            rest = rest + lo[k].astype(F32)
        total = total + jnp.where((pl.program_id(0) == 0) & (begins[0] == 1), rest, 0.0)
    return total


def tally(sums, grads, unit):
    @pl.when(pl.program_id(0) == 0)
    def _():
        sums[...] = jnp.zeros_like(sums)

    sums[0:1, :] += jnp.sum(grads * unit, 0, keepdims=True)
    sums[1:2, :] += jnp.sum(grads, 0, keepdims=True)


def ahead_kernel(group, begins, main, lo, x, gains, hidden_out, bn_out):
    hidden = x[...].astype(F32) + added(main, (lo, begins))
    hidden_out[...] = hidden
    normed, _, _ = layer_stats(hidden, gains[2:3, :], gains[3:4, :])
    bn_out[...] = (regroup(normed, False) if group else normed).astype(BF)


def turn_kernel(group, begins, main, lo, hidden, cot, gains, dh_out, dbr_out, sums):
    grads = added(main, (lo, begins))
    grads = regroup(grads, True) if group else grads
    _, unit, scale = layer_stats(hidden[...], gains[2:3, :], gains[3:4, :])
    dh = cot[...].astype(F32) + layer_back(grads, unit, scale, gains[2:3, :])
    dh_out[...] = dh
    dbr_out[...] = dh.astype(BF)
    tally(sums, grads, unit)


def last_kernel(group, main, x, dh, gains, gx_out, sums):
    grads = added(main, None)
    grads = regroup(grads, True) if group else grads
    _, unit, scale = layer_stats(x[...].astype(F32), gains[0:1, :], gains[1:2, :])
    gx_out[...] = (dh[...] + layer_back(grads, unit, scale, gains[0:1, :])).astype(BF)
    tally(sums, grads, unit)


def row_call(kernel, name, args, kinds, outs, rows, width, tile=16):
    n = args[kinds.index("main")].shape[0] if "main" in kinds else 1
    specs = {
        "main": pl.BlockSpec((n, tile, width), lambda i: (0, i, 0)),
        "lo": pl.BlockSpec((n, tile, width), lambda i: (0, 0, 0)),
        "scalar": pl.BlockSpec(memory_space=pltpu.SMEM),
        "row": pl.BlockSpec((tile, width), lambda i: (i, 0)),
        "gains": pl.BlockSpec((4, width), lambda i: (0, 0)),
        "sums": pl.BlockSpec((8, width), lambda i: (0, 0)),
    }
    return pl.pallas_call(
        kernel,
        grid=(rows // tile,),
        in_specs=[specs[k] for k in kinds],
        out_specs=[specs["sums" if h == 8 else "row"] for h, _ in outs],
        out_shape=[jax.ShapeDtypeStruct((h, width), t) for h, t in outs],
        cost_estimate=cost(4),
        name=name,
    )(*args)


def first_kernel(x, gains, out):
    normed, _, _ = layer_stats(x[...].astype(F32), gains[0:1, :], gains[1:2, :])
    out[...] = normed.astype(BF)


def turned(x, cos, sin, sign):
    half = x.shape[1] // 2
    a, b = x[:, :half], x[:, half:]
    return jnp.concatenate([a * cos - sign * (b * sin), b * cos + sign * (a * sin)], 1)


def heads_kernel(q, k, v, cos, sin, outw, qs, ks, vs, kw, own):
    qs[0] = turned(q[...], cos[...], sin[...], 1.0).astype(BF)
    key = turned(k[...], cos[...], sin[...], 1.0).astype(BF)
    val = v[...].astype(BF)
    late = (key.astype(F32) * outw[0]).astype(BF)
    ks[0], vs[0], kw[0] = key, val, late
    own[0] = mm_tn(late, val).astype(BF)


def weighted(parts, weights):
    h = pl.program_id(0)
    total = parts[0, 0].astype(F32) * weights[0, h]
    for k in range(1, parts.shape[0]):
        total = total + parts[k, 0].astype(F32) * weights[k, h]
    return total.astype(BF)


def unit_of(mixed):
    vals = mixed.astype(F32)
    centred = vals - jnp.mean(vals, axis=-1, keepdims=True)
    scale = lax.rsqrt(jnp.mean(centred * centred, axis=-1, keepdims=True) + norm_eps)
    return centred * scale, scale


def retain_kernel(weights, states, qs, ks, vs, gate, mask, inw, state_out, probs_out, mixed_out, gated):
    state = weighted(states, weights)
    state_out[0] = state
    probs = (mm_t(qs[0], ks[0]) * mask[0]).astype(BF)
    probs_out[0] = probs
    mixed = (mm(probs, vs[0]) + mm(qs[0], state) * inw[0]).astype(BF)
    mixed_out[0] = mixed
    unit, _ = unit_of(mixed)
    pre = gate[...]
    gated[...] = (pre * jax.nn.sigmoid(pre) * unit).astype(BF)


def back_kernel(grads, gate, mixed, qs, ks, vs, state, mask, inw, cos, sin, dgate, dos_out, reach, dsc_out, dq):
    unit, scale = unit_of(mixed[0])
    pre, g = gate[...], grads[...]
    sig = jax.nn.sigmoid(pre)
    dgate[...] = (g * unit * sig * (1.0 + pre * (1.0 - sig))).astype(BF)
    gu = g * (pre * sig)
    lean = jnp.mean(gu * unit, axis=-1, keepdims=True)
    dos = (scale * (gu - jnp.mean(gu, axis=-1, keepdims=True) - unit * lean)).astype(BF)
    dos_out[0] = dos
    read = (dos.astype(F32) * inw[0]).astype(BF)
    reach[0] = mm_tn(qs[0], read).astype(BF)
    dsc = (mm_t(dos, vs[0]) * mask[0]).astype(BF)
    dsc_out[0] = dsc
    dq[...] = turned(mm(dsc, ks[0]) + mm_t(read, state[0]), cos[...], sin[...], -1.0).astype(BF)


def later_kernel(weights, reaches, dsc, qs, vs, probs, dos, kw, outw, cos, sin, dk, dv):
    after = weighted(reaches, weights)
    grad = mm_tn(dsc[0], qs[0]) + mm_t(vs[0], after) * outw[0]
    dk[...] = turned(grad, cos[...], sin[...], -1.0).astype(BF)
    dv[...] = (mm_tn(probs[0], dos[0]) + mm(kw[0], after)).astype(BF)


def head_call(kernel, name, heads, args, specs, outs):
    def spec(v, k):
        if k == "scalar":
            return pl.BlockSpec(memory_space=pltpu.SMEM)
        if k == "all":
            return pl.BlockSpec(v.shape, lambda h: (0,) * len(v.shape))
        if k == "head":
            return pl.BlockSpec((1,) + v.shape[1:], lambda h: (h, 0, 0))
        if k == "parts":
            return pl.BlockSpec((v.shape[0], 1) + v.shape[2:], lambda h: (0, h, 0, 0))
        size, first = k
        return pl.BlockSpec((v.shape[0], size), lambda h: (0, first + h))

    outs = [(jax.ShapeDtypeStruct(shape, BF), k) for shape, k in outs]
    return pl.pallas_call(
        kernel,
        grid=(heads,),
        in_specs=[spec(v, k) for v, k in zip(args, specs)],
        out_specs=[spec(v, k) for v, k in outs],
        out_shape=[v for v, _ in outs],
        cost_estimate=cost(5),
        name=name,
    )(*args)


def shards(
    block_input,
    cotangent,
    decay_rate,
    weight_in,
    weight_out,
    norm_gains,
    moment_in,
    square_in,
    moment_out,
    square_out,
    moment_norm,
    square_norm,
):
    tok_count = block_input.shape[2]
    width = block_input.shape[3]
    sp_n = lax.axis_size("sp")
    ctx_n, f_n = lax.axis_size("ctx"), lax.axis_size("fsdp")
    plane_n = ctx_n * f_n
    heads = H // sp_n
    block_len = tok_count * sp_n
    sp_i = lax.axis_index("sp")
    ctx_i = lax.axis_index("ctx")
    rows_in = weight_in.shape[0]
    qk_w, vd_w = QK // sp_n, VD // sp_n
    widths = (qk_w, qk_w, vd_w, vd_w, vd_w)
    starts = (0, QK, 2 * QK, 2 * QK + VD, 2 * QK + 2 * VD)
    cut = 2 * qk_w + 2 * vd_w

    def perm(v):
        return v.reshape(-1, sp_n, plane_n, rows_in).swapaxes(1, 2).reshape(v.shape)

    def unperm(v):
        return v.reshape(-1, plane_n, sp_n, rows_in).swapaxes(1, 2).reshape(v.shape)

    w_low = weight_in.astype(BF)
    slabs = jnp.concatenate(
        [w_low[:, o : o + sp_n * w].reshape(rows_in, sp_n, w) for o, w in zip(starts, widths)], 2
    )
    slabs = slabs.swapaxes(0, 1)
    o_low = weight_out.astype(BF)
    own_x = block_input.reshape(tok_count, width)
    own_xp = perm(own_x)
    n_dev = sp_n * plane_n
    w_proj, w_o, full_x, gains = spread(
        slabs[:, :, :cut], o_low[:, :width], own_xp, norm_gains.astype(BF), sp_n, f_n, 0
    )
    w_proj, w_o = w_proj.reshape(width, -1), w_o.reshape(-1, width)
    full_x = full_x.reshape(-1, width)
    gains = gains.swapaxes(0, 1).reshape(4, width).astype(F32)
    gains_p = perm(gains)

    grad_ffn_own = cotangent.reshape(tok_count, width)
    held_cot, full_x = lax.optimization_barrier((grad_ffn_own, full_x))
    grad_ffn = lax.all_gather(held_cot, "sp", axis=0, tiled=True)
    (a_low,) = row_call(
        first_kernel, "first", (full_x, gains_p), ("row", "gains"), ((block_len, BF),), block_len, width, 64
    )
    proj = mm(a_low, w_proj)
    head_pos = ctx_i * block_len + jnp.arange(block_len, dtype=jnp.int32)
    cos_h, sin_h = angles(head_pos, DK)

    rates = lax.dynamic_slice_in_dim(decay_rate, sp_i * heads, heads)
    offs = jnp.arange(block_len, dtype=F32)
    spacing = offs[:, None] - offs[None, :]
    mask = jnp.where(
        spacing[None] >= 0.0, jnp.exp(-rates[:, None, None] * jnp.maximum(spacing, 0.0)[None]), 0.0
    )
    inward = jnp.exp(-rates[:, None] * (offs[None, :] + 1.0))[:, :, None]
    outward = jnp.exp(-rates[:, None] * (block_len - 1.0 - offs[None, :]))[:, :, None]
    blocks = jnp.arange(ctx_n)
    back_gap = (ctx_i - 1 - blocks).astype(F32)
    back_w = jnp.where(
        blocks[:, None] < ctx_i,
        jnp.exp(-rates[None, :] * block_len * jnp.maximum(back_gap, 0.0)[:, None]),
        0.0,
    )
    fore_gap = (blocks - ctx_i - 1).astype(F32)
    fore_w = jnp.where(
        blocks[:, None] > ctx_i,
        jnp.exp(-rates[None, :] * block_len * jnp.maximum(fore_gap, 0.0)[:, None]),
        0.0,
    )

    wide, small = (heads, block_len, DV), (heads, block_len, DK)
    corner = (heads, DK, DV)
    qs, ks, vs, kw, own_state = head_call(
        heads_kernel,
        "heads",
        heads,
        (proj, proj, proj, cos_h, sin_h, outward),
        ((DK, 0), (DK, heads), (DV, heads), "all", "all", "head"),
        ((small, "head"), (small, "head"), (wide, "head"), (small, "head"), (corner, "head")),
    )
    states, up_rows = exchange(
        [("block", own_state), ("swap", slabs[:, :, cut:])], sp_n, f_n, 2, 25
    )
    gate_at = (DV, 2 * heads)
    square = (heads, block_len, block_len)
    state, probs, mixed, gated = head_call(
        retain_kernel,
        "retain",
        heads,
        (back_w, states, qs, ks, vs, proj, mask, inward),
        ("scalar", "parts", "head", "head", "head", gate_at, "head", "head"),
        ((corner, "head"), (square, "head"), (wide, "head"), ((block_len, vd_w), (DV, 0))),
    )
    group = rows_in == 64 and sp_n == 4 and plane_n == 8
    fine = 16

    begins = ((sp_i == 0) & (ctx_i == 0)).astype(jnp.int32).reshape(1)

    def parts_of(v):
        return v.astype(BF).reshape(sp_n, tok_count, width)

    def rest_of(dot, left, right, main):
        rows = left.reshape(sp_n, tok_count, -1)[:, :fine].reshape(sp_n * fine, -1)
        exact = dot(rows, right).reshape(sp_n, fine, width)
        return (exact - main[:, :fine].astype(F32)).astype(BF)

    down_rows = o_low[:, width:].reshape(2, -1, width)
    part_h = parts_of(mm(gated, w_o))
    rest_h = rest_of(mm, gated, w_o, part_h)
    got, lo, w_up, w_down = exchange(
        [("swap", part_h), ("lead", rest_h), ("plane", up_rows), ("plane", down_rows)], sp_n, f_n, 4, 50
    )
    w_up, w_down = w_up.reshape(width, -1), w_down.reshape(-1, width)
    hidden, normed_b = row_call(
        functools.partial(ahead_kernel, group),
        "ahead",
        (begins, got, lo, own_x, gains),
        ("scalar", "main", "lo", "row", "gains"),
        ((tok_count, F32), (tok_count, BF)),
        tok_count,
        width,
    )
    (b_low,) = exchange([("gather", normed_b if group else perm(normed_b))], sp_n, f_n, 5, 40)
    b_low = b_low.reshape(block_len, width)
    up = mm(b_low, w_up)
    act_low = jax.nn.gelu(up, approximate=False).astype(BF)
    ffn_part = mm(act_low, w_down).astype(BF)

    grad_act = mm_t(grad_ffn, w_down)
    density = (
        0.5 * (1.0 + lax.erf(up * root_half)) + up * jnp.exp(-0.5 * up * up) * inv_root_tau
    )
    grad_up = (grad_act * density).astype(BF)

    def reduce_rows(v):
        return lax.psum_scatter(v, PLANE, scatter_dimension=0, tiled=True)

    part_down = mm_tn(act_low, grad_ffn).astype(BF)
    part_up = mm_tn(b_low, grad_up).astype(BF)
    part_b = parts_of(mm_t(grad_up, w_up))
    rest_b = rest_of(mm_t, grad_up, w_up, part_b)
    part_b, part_down, part_up = lax.optimization_barrier((part_b, part_down, part_up))
    sum_down = reduce_rows(part_down)
    ctx_own = lambda v: lax.dynamic_index_in_dim(v, ctx_i, 0, False).astype(F32)

    def core_sum(v, others):
        mine = lax.dynamic_index_in_dim(v, lax.axis_index("fsdp"), 1, False)
        return (mine.astype(F32) + jnp.sum(others.astype(F32), 0)).astype(BF)

    part_up = part_up.reshape(ctx_n, f_n, -1, part_up.shape[1])
    if not group:
        part_b, rest_b = unperm(part_b), unperm(rest_b)
    got, lo, up_others = exchange([("swap", part_b), ("lead", rest_b), ("core", part_up)], sp_n, f_n, 6, 50)
    up_half = core_sum(part_up, up_others)
    grad_hidden, grad_branch, sums_b = row_call(
        functools.partial(turn_kernel, group),
        "turn",
        (begins, got, lo, hidden, grad_ffn_own, gains),
        ("scalar", "main", "lo", "row", "row", "gains"),
        ((tok_count, F32), (tok_count, BF), (8, F32)),
        tok_count,
        width,
    )
    grad_branch, up_blocks = exchange([("gather", grad_branch), ("ctx_swap", up_half)], sp_n, f_n, 7, 40)
    grad_branch = grad_branch.reshape(block_len, width)
    sum_up = (ctx_own(up_half) + jnp.sum(up_blocks.astype(F32), 0)).astype(BF)
    part_o = mm_tn(gated, grad_branch).astype(BF)

    grad_gate, grad_mixed, own_reach, grad_scores, grad_q = head_call(
        back_kernel,
        "back",
        heads,
        (mm_t(grad_branch, w_o), proj, mixed, qs, ks, vs, state, mask, inward, cos_h, sin_h),
        ((DV, 0), gate_at) + ("head",) * 7 + ("all", "all"),
        (
            ((block_len, vd_w), (DV, 0)),
            (wide, "head"),
            (corner, "head"),
            (square, "head"),
            ((block_len, qk_w), (DK, 0)),
        ),
    )
    grad_gq = jnp.concatenate([grad_gate, grad_q], 1)
    part_gq = mm_tn(a_low, grad_gq).astype(BF)
    own_reach, part_o, part_gq, sum_down = lax.optimization_barrier(
        (own_reach, part_o, part_gq, sum_down)
    )
    sum_gq = reduce_rows(part_gq)
    part_o = part_o.reshape(ctx_n, f_n, -1, width)

    def home(v):
        return v.reshape(sp_n, rows_in, -1)

    reaches, o_others, back_up = exchange(
        [("block", own_reach), ("core", part_o), ("swap", home(sum_up))], sp_n, f_n, 3, 25
    )
    o_half = core_sum(part_o, o_others)
    grad_k, grad_v = head_call(
        later_kernel,
        "later",
        heads,
        (fore_w, reaches, grad_scores, qs, vs, probs, grad_mixed, kw, outward, cos_h, sin_h),
        ("scalar", "parts") + ("head",) * 7 + ("all", "all"),
        (((block_len, qk_w), (DK, 0)), ((block_len, vd_w), (DV, 0))),
    )
    grad_kv = jnp.concatenate([grad_k, grad_v], 1)
    part_kv = mm_tn(a_low, grad_kv).astype(BF)
    grad_proj = jnp.concatenate([grad_gq[:, vd_w:], grad_kv, grad_gate], 1)
    part_a = parts_of(mm_t(grad_proj, w_proj))
    part_a, part_kv, o_half, sum_gq = lax.optimization_barrier((part_a, part_kv, o_half, sum_gq))
    sum_kv = reduce_rows(part_kv)

    got, o_blocks = exchange(
        [("swap", part_a if group else unperm(part_a)), ("ctx_swap", o_half)], sp_n, f_n, 8, 50
    )
    sum_o = ctx_own(o_half) + jnp.sum(o_blocks.astype(F32), 0)
    grad_x, sums_a = row_call(
        functools.partial(last_kernel, group),
        "last",
        (got, own_x, grad_hidden, gains),
        ("main", "row", "row", "gains"),
        ((tok_count, BF), (8, F32)),
        tok_count,
        width,
    )
    grad_x = grad_x.reshape(block_input.shape)
    norm_terms = jnp.concatenate([sums_a[:2], sums_b[:2]], 0)
    norm_parts = norm_terms.reshape(4, n_dev, -1).swapaxes(0, 1)
    ffn_part, sum_kv, sums_a = lax.optimization_barrier((ffn_part, sum_kv, sums_a))
    ffn = lax.psum_scatter(ffn_part, "sp", scatter_dimension=0, tiled=True)
    block_out = (hidden + ffn.astype(F32)).astype(BF).reshape(block_input.shape)
    norm_terms = jnp.concatenate([sums_a[:2], sums_b[:2]], 0)
    norm_parts = norm_terms.reshape(4, n_dev, -1).swapaxes(0, 1)
    norm_sums, back_gq = exchange([("all", norm_parts), ("swap", home(sum_gq))], sp_n, f_n, 9, 20)
    grad_gains = jnp.sum(norm_sums, 0)
    (back_kv,) = exchange([("swap", home(sum_kv))], sp_n, f_n, 10, 22)
    parts = [back_gq[:, :, vd_w:], back_kv[:, :, :qk_w], back_kv[:, :, qk_w:], back_gq[:, :, :vd_w], back_up]
    grad_first = jnp.concatenate(
        [p.swapaxes(0, 1).reshape(rows_in, -1) for p in parts], 1
    ).astype(F32)
    grad_second = jnp.concatenate([sum_o, sum_down.astype(F32)], 1)
    first_m, first_v, first_step = adam_update(weight_in, grad_first, moment_in, square_in)
    second_m, second_v, second_step = adam_update(weight_out, grad_second, moment_out, square_out)
    gain_m, gain_v, gain_step = adam_update(norm_gains, grad_gains, moment_norm, square_norm)
    return (
        block_out,
        grad_x,
        grad_first,
        first_m,
        first_v,
        first_step,
        grad_second,
        second_m,
        second_v,
        second_step,
        grad_gains,
        gain_m,
        gain_v,
        gain_step,
    )


def solution(mesh):
    tokens = P("fsdp", "ctx", "sp", None)
    rows = P(ALL, None)
    cols = P(None, ALL)
    in_specs = (tokens, tokens, P(), rows, rows, cols, rows, rows, rows, rows, cols, cols)
    out_specs = (tokens, tokens) + (rows,) * 8 + (cols,) * 4
    return jax.shard_map(shards, mesh=mesh, in_specs=in_specs, out_specs=out_specs, check_vma=False)
```

```python
import functools
import math

import jax
import jax.numpy as jnp
from jax import lax
from jax.experimental import pallas as pl
from jax.experimental.pallas import tpu as pltpu
from jax.sharding import PartitionSpec as P

H = 8
DK = 256
DV = 512
SPAN = 512
STEP = 10
QK = 2048
VD = 4096

beta_one = 0.9
beta_two = 0.95
learn_rate = 0.01
decay_weight = 0.1
adam_eps = 1e-08
norm_eps = 1e-05
root_half = 0.7071067811865476
inv_root_tau = 0.3989422804014327


BF = jnp.bfloat16
F32 = jnp.float32
ALL = ("sp", "ctx", "fsdp")
PLANE = ("ctx", "fsdp")


def layer_stats(values, gain_row, shift_row):
    centred = values - jnp.mean(values, axis=-1, keepdims=True)
    inv_std = lax.rsqrt(jnp.mean(centred * centred, axis=-1, keepdims=True) + norm_eps)
    unit_vals = centred * inv_std
    return (unit_vals * gain_row + shift_row, unit_vals, inv_std)


def layer_back(grad_vals, unit_vals, inv_std, gain_row):
    scaled = grad_vals * gain_row
    return inv_std * (
        scaled
        - jnp.mean(scaled, axis=-1, keepdims=True)
        - unit_vals * jnp.mean(scaled * unit_vals, axis=-1, keepdims=True)
    )


def angles(positions, head_size):
    half_size = head_size // 2
    inverse = jnp.exp(
        -math.log(10000.0) * (2.0 * jnp.arange(half_size, dtype=jnp.float32) / head_size)
    )
    phases = positions.astype(jnp.float32)[:, None] * inverse[None, :]
    return (jnp.cos(phases), jnp.sin(phases))


def rotate(values, cosine, sine, sign_flip):
    half_size = values.shape[-1] // 2
    first_half = values[..., :half_size]
    second_half = values[..., half_size:]
    return jnp.concatenate(
        [
            first_half * cosine - sign_flip * (second_half * sine),
            second_half * cosine + sign_flip * (first_half * sine),
        ],
        -1,
    )


def adam_update(weight, grad_vals, moment, square):
    moment_new = beta_one * moment + (1.0 - beta_one) * grad_vals
    square_new = beta_two * square + (1.0 - beta_two) * grad_vals * grad_vals
    moment_hat = moment_new / (1.0 - beta_one**STEP)
    square_hat = square_new / (1.0 - beta_two**STEP)
    step_vals = -learn_rate * (
        moment_hat / (jnp.sqrt(square_hat) + adam_eps) + decay_weight * weight
    )
    return (moment_new, square_new, step_vals)


def mm(a, b):
    return jnp.dot(a, b, preferred_element_type=F32)


def mm_t(a, b):
    return lax.dot_general(a, b, (((1,), (1,)), ((), ())), preferred_element_type=F32)


def mm_tn(a, b):
    return lax.dot_general(a, b, (((0,), (0,)), ((), ())), preferred_element_type=F32)


def ein(spec, a, b):
    return jnp.einsum(spec, a, b, preferred_element_type=F32)


MESH_ID = pl.DeviceIdType.MESH
ANY = pl.BlockSpec(memory_space=pl.ANY)
VM = pl.BlockSpec(memory_space=pltpu.VMEM)


def greet(peers):
    sem = pltpu.get_barrier_semaphore()
    for peer in peers:
        pl.semaphore_signal(sem, inc=1, device_id=peer, device_id_type=MESH_ID)
    pl.semaphore_wait(sem, len(peers))


def push(src, dst, send, recv, peer):
    copy = pltpu.make_async_remote_copy(
        src_ref=src, dst_ref=dst, send_sem=send, recv_sem=recv, device_id=peer, device_id_type=MESH_ID
    )
    copy.start()
    return copy


def arrived(dst, send, recv, peer):
    pltpu.make_async_remote_copy(
        src_ref=dst, dst_ref=dst, send_sem=send, recv_sem=recv, device_id=peer, device_id_type=MESH_ID
    ).wait_recv()


def beside(c):
    low = c + 1 - 2 * (c % 2)
    high = (c + 2) % 4
    return low, high, (low + 2) % 4


def cost(micros):
    return pl.CostEstimate(flops=0, transcendentals=0, bytes_accessed=int(micros * 3.0e6))


def along(s, n):
    if n == 4:
        return [s, s + 1 - 2 * (s % 2), (s + 2) % 4, 3 - s]
    return [lax.rem(s + j, n) for j in range(n)]


def params(ident):
    return pltpu.CompilerParams(collective_id=ident, has_side_effects=True)


def others(s, c, f, sp_n, f_n):
    ids, flat = [], []
    for a in range(sp_n):
        for b in range(4):
            for d in range(f_n):
                if a or b or d:
                    p, q, r = lax.rem(s + a, sp_n), lax.rem(c + b, 4), lax.rem(f + d, f_n)
                    ids.append({"sp": p, "ctx": q, "fsdp": r})
                    flat.append((p * 4 + q) * f_n + r)
    return ids, flat


def spread_kernel(sp_n, f_n, wp_in, wo_in, x_in, g_in, wp, wo, x, g, gs, gr, lsem, zs, zr, xs, xr, ps, pr, cs, cr):
    s, c, f = lax.axis_index("sp"), lax.axis_index("ctx"), lax.axis_index("fsdp")
    low, high, both = beside(c)
    lines = along(s, sp_n)
    cores = [lax.rem(f + k, f_n) for k in range(1, f_n)]
    here = (s * 4 + c) * f_n + f
    ids, flat = others(s, c, f, sp_n, f_n)
    greet(ids)
    n_items = sp_n + 1
    waits = []

    def item_at(i, cc, ff):
        return wp.at[cc, ff, lines[i - 1]] if i else wo.at[cc, ff]

    def key(i):
        return 1 + lines[i - 1] if i else 0

    def start_local(n, src, dst):
        copy = pltpu.make_async_copy(src, dst, lsem.at[n])
        copy.start()
        return copy

    for n, p in enumerate(ids):
        waits.append(push(g_in, g.at[here], gs.at[n], gr.at[here], p))
    for j in range(1, sp_n):
        waits.append(push(wp_in.at[lines[j]], wp.at[c, f, s], zs.at[j], zr.at[s], {"sp": lines[j]}))
    for j in range(1, sp_n):
        waits.append(push(x_in, x.at[s], xs.at[j], xr.at[s], {"sp": lines[j]}))
    own = (wo_in, wp_in.at[s])
    local = [start_local(i, own[i], item_at(i, c, f)) for i in range(2)]
    local.append(start_local(2, x_in, x.at[s]))
    local.append(start_local(3, g_in, g.at[here]))

    def to_cores(i, src, cc):
        for n, p in enumerate(cores):
            waits.append(
                push(
                    src,
                    item_at(i, cc, f),
                    cs.at[(n * 4 + cc) * n_items + i],
                    cr.at[(f * 4 + cc) * n_items + key(i)],
                    {"fsdp": p},
                )
            )

    def first(i):
        if i < 2:
            src = own[i]
        else:
            src = item_at(i, c, f)
            arrived(src, zs.at[0], zr.at[lines[i - 1]], {"sp": lines[i - 1]})
        for n, p in enumerate((low, high)):
            waits.append(
                push(src, item_at(i, c, f), ps.at[3 * i + n], pr.at[c * n_items + key(i)], {"ctx": p})
            )
        to_cores(i, src, c)

    def landed(i, cc):
        arrived(item_at(i, cc, f), ps.at[0], pr.at[cc * n_items + key(i)], {"ctx": cc})

    def second(i):
        for n, (came, goes) in enumerate(((low, high), (high, low))):
            landed(i, came)
            at = item_at(i, came, f)
            if i % 2 == n:
                waits.append(push(at, at, ps.at[3 * i + 2], pr.at[came * n_items + key(i)], {"ctx": goes}))
            to_cores(i, at, came)

    def third(i):
        landed(i, both)
        to_cores(i, item_at(i, both, f), both)

    for i in range(n_items + 2):
        if i < n_items:
            first(i)
        if 1 <= i < n_items + 1:
            second(i - 1)
        if i >= 2:
            third(i - 2)
    for j in range(1, sp_n):
        arrived(x.at[lines[j]], xs.at[0], xr.at[lines[j]], {"sp": lines[j]})
    for p in cores:
        for cc in range(4):
            for i in range(n_items):
                arrived(item_at(i, cc, p), cs.at[0], cr.at[(p * 4 + cc) * n_items + key(i)], {"fsdp": p})
    for k, p in zip(flat, ids):
        arrived(g.at[k], gs.at[0], gr.at[k], p)
    for copy in waits:
        copy.wait_send()
    for copy in local:
        copy.wait()


def spread(wp_in, wo_in, x_in, g_in, sp_n, f_n, ident):
    n_items, n_dev = sp_n + 1, sp_n * 4 * f_n
    shapes = [
        (4, f_n) + wp_in.shape,
        (4, f_n) + wo_in.shape,
        (sp_n,) + x_in.shape,
        (n_dev,) + g_in.shape,
    ]
    dma = pltpu.SemaphoreType.DMA
    return pl.pallas_call(
        functools.partial(spread_kernel, sp_n, f_n),
        out_shape=[jax.ShapeDtypeStruct(v, BF) for v in shapes],
        in_specs=[VM] * 4,
        out_specs=[ANY] * 4,
        scratch_shapes=[
            dma((n_dev,)),
            dma((n_dev,)),
            dma((4,)),
            dma((sp_n,)),
            dma((sp_n,)),
            dma((sp_n,)),
            dma((sp_n,)),
            dma((3 * n_items,)),
            dma((4 * n_items,)),
            dma(((f_n - 1) * 4 * n_items,)),
            dma((f_n * 4 * n_items,)),
        ],
        compiler_params=params(ident),
        cost_estimate=cost(85),
        name="spread",
    )(wp_in, wo_in, x_in, g_in)


def exchange_kernel(plan, sp_n, f_n, *refs):
    m = len(plan)
    ins, outs, (ls, ss, rs) = refs[:m], refs[m : 2 * m], refs[2 * m :]
    s, c, f = lax.axis_index("sp"), lax.axis_index("ctx"), lax.axis_index("fsdp")
    low, high, both = beside(c)
    line = along(s, sp_n)[1:]
    cores = [lax.rem(f + k, f_n) for k in range(1, f_n)]
    kinds = set(plan)
    here = (s * 4 + c) * f_n + f
    ids, flat = others(s, c, f, sp_n, f_n)
    peers = []
    if kinds & {"swap", "gather", "lead"}:
        peers += [{"sp": p} for p in line]
    if kinds & {"ctx_swap"}:
        peers += [{"ctx": p} for p in (low, high, both)]
    elif kinds & {"block", "plane"}:
        peers += [{"ctx": p} for p in (low, high)]
    if kinds & {"core", "plane"}:
        peers += [{"fsdp": p} for p in cores]
    greet(ids if "all" in kinds else peers)
    sends, local, steps, ends = [], [], [], []
    used = [0, 0, 0]

    def take(k, n):
        used[k] += n
        return used[k] - n

    def send(src, dst, r, peer):
        sends.append(push(src, dst, ss.at[take(1, 1)], rs.at[r], peer))

    def keep(src, dst):
        copy = pltpu.make_async_copy(src, dst, ls.at[take(0, 1)])
        copy.start()
        local.append(copy)

    def got(dst, r, peer):
        arrived(dst, ss.at[0], rs.at[r], peer)

    def swap(x, o):
        r = take(2, sp_n)
        for p in line:
            send(x.at[p], o.at[s], r + s, {"sp": p})
        keep(x.at[s], o.at[s])
        ends.append(lambda: [got(o.at[p], r + p, {"sp": p}) for p in line])

    def every(x, o):
        r = take(2, len(ids) + 1)
        for k, p in zip(flat, ids):
            send(x.at[k], o.at[here], r + here, p)
        keep(x.at[here], o.at[here])
        ends.append(lambda: [got(o.at[k], r + k, p) for k, p in zip(flat, ids)])

    def ctx_swap(x, o):
        r = take(2, 3)
        for p in (low, high, both):
            k = lax.rem(c - p + 4, 4) - 1
            send(x.at[p], o.at[k], r + k, {"ctx": p})
        ends.append(lambda: [got(o.at[k], r + k, {"ctx": low}) for k in range(3)])

    def core(x, o):
        r = take(2, f_n - 1)
        for p in cores:
            k = lax.rem(f - p + f_n, f_n) - 1
            send(x.at[:, p], o.at[k], r + k, {"fsdp": p})
        ends.append(lambda: [got(o.at[k], r + k, {"fsdp": cores[0]}) for k in range(f_n - 1)])

    def plane(x, o, wide):
        n = x.shape[0]
        r, rc = take(2, 4 * n), take(2, f_n * 4 * n) if wide else 0
        at = lambda cc, ff, i: o.at[cc, ff, i] if wide else o.at[cc, i]

        def across(src, cc, i):
            if wide:
                for p in cores:
                    send(src, at(cc, f, i), rc + (f * 4 + cc) * n + i, {"fsdp": p})

        for i in range(n):
            for p in (low, high):
                send(x.at[i], at(c, f, i), r + c * n + i, {"ctx": p})
            across(x.at[i], c, i)
        keep(x, o.at[c, f] if wide else o.at[c])

        def near(i):
            for k, (came, goes) in enumerate(((low, high), (high, low))):
                got(at(came, f, i), r + came * n + i, {"ctx": came})
                if i % 2 == k:
                    send(at(came, f, i), at(came, f, i), r + came * n + i, {"ctx": goes})
                across(at(came, f, i), came, i)

        def far(i):
            got(at(both, f, i), r + both * n + i, {"ctx": both})
            across(at(both, f, i), both, i)

        def close():
            for p in cores if wide else ():
                for cc in range(4):
                    for i in range(n):
                        got(at(cc, p, i), rc + (p * 4 + cc) * n + i, {"fsdp": p})

        steps.extend([functools.partial(near, i) for i in range(n)])
        steps.extend([functools.partial(far, i) for i in range(n)])
        ends.append(close)

    def gather(x, o):
        n = sp_n
        r, q = take(2, n), take(1, 2 * n)
        up_ok, down_ok = s + 1 < n, s > 0

        def desc(slot, way, peer, first):
            return pltpu.make_async_remote_copy(
                src_ref=x if first else o.at[slot],
                dst_ref=o.at[slot],
                send_sem=ss.at[q + way * n + slot],
                recv_sem=rs.at[r + slot],
                device_id={"sp": peer},
                device_id_type=MESH_ID,
            )

        def out_going(k, act):
            @pl.when((s - k >= 0) & up_ok)
            def _():
                act(desc(s - k, 0, s + 1, k == 0))

            @pl.when((s + k < n) & down_ok)
            def _():
                act(desc(s + k, 1, s - 1, k == 0))

        def incoming(k):
            @pl.when(s - 1 - k >= 0)
            def _():
                desc(s - 1 - k, 0, s - 1, False).wait_recv()

            @pl.when(s + 1 + k < n)
            def _():
                desc(s + 1 + k, 1, s + 1, False).wait_recv()

        def step(k):
            incoming(k)
            if k + 1 < n - 1:
                out_going(k + 1, lambda d: d.start())

        def close():
            for k in range(n - 1):
                out_going(k, lambda d: d.wait_send())

        out_going(0, lambda d: d.start())
        keep(x, o.at[s])
        steps.extend([functools.partial(step, k) for k in range(n - 1)])
        ends.append(close)

    def lead(x, o):
        r, q = take(2, sp_n), take(1, 1)
        goes, comes = (c == 0) & (s > 0), (c == 0) & (s == 0)

        def desc(k):
            return pltpu.make_async_remote_copy(
                src_ref=x.at[0],
                dst_ref=o.at[k],
                send_sem=ss.at[q],
                recv_sem=rs.at[r + k],
                device_id={"sp": 0},
                device_id_type=MESH_ID,
            )

        @pl.when(goes)
        def _():
            desc(s).start()

        keep(x.at[0], o.at[0])

        def close():
            @pl.when(comes)
            def _():
                for k in range(1, sp_n):
                    desc(k).wait_recv()

            @pl.when(goes)
            def _():
                desc(s).wait_send()

        ends.append(close)

    for kind, x, o in zip(plan, ins, outs):
        if kind == "swap":
            swap(x, o)
        elif kind == "lead":
            lead(x, o)
        elif kind == "all":
            every(x, o)
        elif kind == "ctx_swap":
            ctx_swap(x, o)
        elif kind == "core":
            core(x, o)
        elif kind == "gather":
            gather(x, o)
        else:
            plane(x, o, kind == "plane")
    for step in steps:
        step()
    for end in ends:
        end()
    for copy in sends:
        copy.wait_send()
    for copy in local:
        copy.wait()


def exchange(ops, sp_n, f_n, ident, micros):
    plan = tuple(kind for kind, _ in ops)
    outs, n_send, n_recv = [], 0, 0
    for kind, x in ops:
        n = x.shape[0]
        if kind == "swap":
            shape, a, b = x.shape, sp_n - 1, sp_n
        elif kind == "lead":
            shape, a, b = x.shape, 1, sp_n
        elif kind == "all":
            shape, a, b = x.shape, n, n
        elif kind == "ctx_swap":
            shape, a, b = (3,) + x.shape[1:], 3, 3
        elif kind == "core":
            shape, a, b = (f_n - 1, x.shape[0]) + x.shape[2:], f_n - 1, f_n - 1
        elif kind == "gather":
            shape, a, b = (sp_n,) + x.shape, 2 * sp_n, sp_n
        elif kind == "block":
            shape, a, b = (4,) + x.shape, 3 * n, 4 * n
        else:
            shape, a, b = (4, f_n) + x.shape, 3 * n + 4 * n * (f_n - 1), 4 * n * (f_n + 1)
        outs.append(jax.ShapeDtypeStruct(shape, x.dtype))
        n_send, n_recv = n_send + a, n_recv + b
    dma = pltpu.SemaphoreType.DMA
    far = ("core", "ctx_swap")
    return pl.pallas_call(
        functools.partial(exchange_kernel, plan, sp_n, f_n),
        out_shape=outs,
        in_specs=[ANY if kind in far else VM for kind in plan],
        out_specs=[ANY if kind in far + ("plane",) else VM for kind in plan],
        scratch_shapes=[dma((len(ops),)), dma((n_send,)), dma((n_recv,))],
        compiler_params=params(ident),
        cost_estimate=cost(micros),
        name="exchange_" + "_".join(plan),
    )(*[x for _, x in ops])


def regroup(v, back):
    lane = lax.broadcasted_iota(jnp.int32, (v.shape[0], 128), 1) < 64
    piece = lambda k: v[:, 128 * k : 128 * k + 128]
    turn = lambda p: pltpu.roll(p, 64, 1)
    out = []
    for k in range(v.shape[1] // 128):
        if back:
            s, pair = k // 4, k % 4
            a, b, odd = 4 * pair + s // 2, 4 * pair + 2 + s // 2, s % 2
        else:
            cf, half = k // 2, k % 2
            a, b, odd = 8 * half + cf // 2, 8 * half + 4 + cf // 2, cf % 2
        if odd:
            out.append(jnp.where(lane, turn(piece(a)), piece(b)))
        else:
            out.append(jnp.where(lane, piece(a), turn(piece(b))))
    return jnp.concatenate(out, 1)


def added(main, lead):
    total = main[0].astype(F32)
    for k in range(1, main.shape[0]):
        total = total + main[k].astype(F32)
    if lead is not None:
        lo, begins = lead
        rest = lo[0].astype(F32)
        for k in range(1, lo.shape[0]):
            rest = rest + lo[k].astype(F32)
        total = total + jnp.where((pl.program_id(0) == 0) & (begins[0] == 1), rest, 0.0)
    return total


def tally(sums, grads, unit):
    @pl.when(pl.program_id(0) == 0)
    def _():
        sums[...] = jnp.zeros_like(sums)

    sums[0:1, :] += jnp.sum(grads * unit, 0, keepdims=True)
    sums[1:2, :] += jnp.sum(grads, 0, keepdims=True)


def ahead_kernel(group, begins, main, lo, x, gains, hidden_out, bn_out):
    hidden = x[...].astype(F32) + added(main, (lo, begins))
    hidden_out[...] = hidden
    normed, _, _ = layer_stats(hidden, gains[2:3, :], gains[3:4, :])
    bn_out[...] = (regroup(normed, False) if group else normed).astype(BF)


def turn_kernel(group, begins, main, lo, hidden, cot, gains, dh_out, dbr_out, sums):
    grads = added(main, (lo, begins))
    grads = regroup(grads, True) if group else grads
    _, unit, scale = layer_stats(hidden[...], gains[2:3, :], gains[3:4, :])
    dh = cot[...].astype(F32) + layer_back(grads, unit, scale, gains[2:3, :])
    dh_out[...] = dh
    dbr_out[...] = dh.astype(BF)
    tally(sums, grads, unit)


def last_kernel(group, main, x, dh, gains, gx_out, sums):
    grads = added(main, None)
    grads = regroup(grads, True) if group else grads
    _, unit, scale = layer_stats(x[...].astype(F32), gains[0:1, :], gains[1:2, :])
    gx_out[...] = (dh[...] + layer_back(grads, unit, scale, gains[0:1, :])).astype(BF)
    tally(sums, grads, unit)


def row_call(kernel, name, args, kinds, outs, rows, width, tile=16):
    n = args[kinds.index("main")].shape[0] if "main" in kinds else 1
    specs = {
        "main": pl.BlockSpec((n, tile, width), lambda i: (0, i, 0)),
        "lo": pl.BlockSpec((n, tile, width), lambda i: (0, 0, 0)),
        "scalar": pl.BlockSpec(memory_space=pltpu.SMEM),
        "row": pl.BlockSpec((tile, width), lambda i: (i, 0)),
        "gains": pl.BlockSpec((4, width), lambda i: (0, 0)),
        "sums": pl.BlockSpec((8, width), lambda i: (0, 0)),
    }
    return pl.pallas_call(
        kernel,
        grid=(rows // tile,),
        in_specs=[specs[k] for k in kinds],
        out_specs=[specs["sums" if h == 8 else "row"] for h, _ in outs],
        out_shape=[jax.ShapeDtypeStruct((h, width), t) for h, t in outs],
        cost_estimate=cost(4),
        name=name,
    )(*args)


def first_kernel(x, gains, out):
    normed, _, _ = layer_stats(x[...].astype(F32), gains[0:1, :], gains[1:2, :])
    out[...] = normed.astype(BF)


def turned(x, cos, sin, sign):
    half = x.shape[1] // 2
    a, b = x[:, :half], x[:, half:]
    return jnp.concatenate([a * cos - sign * (b * sin), b * cos + sign * (a * sin)], 1)


def heads_kernel(q, k, v, cos, sin, outw, qs, ks, vs, kw, own):
    qs[0] = turned(q[...], cos[...], sin[...], 1.0).astype(BF)
    key = turned(k[...], cos[...], sin[...], 1.0).astype(BF)
    val = v[...].astype(BF)
    late = (key.astype(F32) * outw[0]).astype(BF)
    ks[0], vs[0], kw[0] = key, val, late
    own[0] = mm_tn(late, val).astype(BF)


def weighted(parts, weights):
    h = pl.program_id(0)
    total = parts[0, 0].astype(F32) * weights[0, h]
    for k in range(1, parts.shape[0]):
        total = total + parts[k, 0].astype(F32) * weights[k, h]
    return total.astype(BF)


def unit_of(mixed):
    vals = mixed.astype(F32)
    centred = vals - jnp.mean(vals, axis=-1, keepdims=True)
    scale = lax.rsqrt(jnp.mean(centred * centred, axis=-1, keepdims=True) + norm_eps)
    return centred * scale, scale


def retain_kernel(weights, states, qs, ks, vs, gate, mask, inw, state_out, probs_out, mixed_out, gated):
    state = weighted(states, weights)
    state_out[0] = state
    probs = (mm_t(qs[0], ks[0]) * mask[0]).astype(BF)
    probs_out[0] = probs
    mixed = (mm(probs, vs[0]) + mm(qs[0], state) * inw[0]).astype(BF)
    mixed_out[0] = mixed
    unit, _ = unit_of(mixed)
    pre = gate[...]
    gated[...] = (pre * jax.nn.sigmoid(pre) * unit).astype(BF)


def back_kernel(grads, gate, mixed, qs, ks, vs, state, mask, inw, cos, sin, dgate, dos_out, reach, dsc_out, dq):
    unit, scale = unit_of(mixed[0])
    pre, g = gate[...], grads[...]
    sig = jax.nn.sigmoid(pre)
    dgate[...] = (g * unit * sig * (1.0 + pre * (1.0 - sig))).astype(BF)
    gu = g * (pre * sig)
    lean = jnp.mean(gu * unit, axis=-1, keepdims=True)
    dos = (scale * (gu - jnp.mean(gu, axis=-1, keepdims=True) - unit * lean)).astype(BF)
    dos_out[0] = dos
    read = (dos.astype(F32) * inw[0]).astype(BF)
    reach[0] = mm_tn(qs[0], read).astype(BF)
    dsc = (mm_t(dos, vs[0]) * mask[0]).astype(BF)
    dsc_out[0] = dsc
    dq[...] = turned(mm(dsc, ks[0]) + mm_t(read, state[0]), cos[...], sin[...], -1.0).astype(BF)


def later_kernel(weights, reaches, dsc, qs, vs, probs, dos, kw, outw, cos, sin, dk, dv):
    after = weighted(reaches, weights)
    grad = mm_tn(dsc[0], qs[0]) + mm_t(vs[0], after) * outw[0]
    dk[...] = turned(grad, cos[...], sin[...], -1.0).astype(BF)
    dv[...] = (mm_tn(probs[0], dos[0]) + mm(kw[0], after)).astype(BF)


def head_call(kernel, name, heads, args, specs, outs):
    def spec(v, k):
        if k == "scalar":
            return pl.BlockSpec(memory_space=pltpu.SMEM)
        if k == "all":
            return pl.BlockSpec(v.shape, lambda h: (0,) * len(v.shape))
        if k == "head":
            return pl.BlockSpec((1,) + v.shape[1:], lambda h: (h, 0, 0))
        if k == "parts":
            return pl.BlockSpec((v.shape[0], 1) + v.shape[2:], lambda h: (0, h, 0, 0))
        size, first = k
        return pl.BlockSpec((v.shape[0], size), lambda h: (0, first + h))

    outs = [(jax.ShapeDtypeStruct(shape, BF), k) for shape, k in outs]
    return pl.pallas_call(
        kernel,
        grid=(heads,),
        in_specs=[spec(v, k) for v, k in zip(args, specs)],
        out_specs=[spec(v, k) for v, k in outs],
        out_shape=[v for v, _ in outs],
        cost_estimate=cost(5),
        name=name,
    )(*args)


def shards(
    block_input,
    cotangent,
    decay_rate,
    weight_in,
    weight_out,
    norm_gains,
    moment_in,
    square_in,
    moment_out,
    square_out,
    moment_norm,
    square_norm,
):
    tok_count = block_input.shape[2]
    width = block_input.shape[3]
    sp_n = lax.axis_size("sp")
    ctx_n, f_n = lax.axis_size("ctx"), lax.axis_size("fsdp")
    plane_n = ctx_n * f_n
    heads = H // sp_n
    block_len = tok_count * sp_n
    sp_i = lax.axis_index("sp")
    ctx_i = lax.axis_index("ctx")
    rows_in = weight_in.shape[0]
    qk_w, vd_w = QK // sp_n, VD // sp_n
    widths = (qk_w, qk_w, vd_w, vd_w, vd_w)
    starts = (0, QK, 2 * QK, 2 * QK + VD, 2 * QK + 2 * VD)
    cut = 2 * qk_w + 2 * vd_w

    def perm(v):
        return v.reshape(-1, sp_n, plane_n, rows_in).swapaxes(1, 2).reshape(v.shape)

    def unperm(v):
        return v.reshape(-1, plane_n, sp_n, rows_in).swapaxes(1, 2).reshape(v.shape)

    w_low = weight_in.astype(BF)
    slabs = jnp.concatenate(
        [w_low[:, o : o + sp_n * w].reshape(rows_in, sp_n, w) for o, w in zip(starts, widths)], 2
    )
    slabs = slabs.swapaxes(0, 1)
    o_low = weight_out.astype(BF)
    own_x = block_input.reshape(tok_count, width)
    own_xp = perm(own_x)
    n_dev = sp_n * plane_n
    w_proj, w_o, full_x, gains = spread(
        slabs[:, :, :cut], o_low[:, :width], own_xp, norm_gains.astype(BF), sp_n, f_n, 0
    )
    w_proj, w_o = w_proj.reshape(width, -1), w_o.reshape(-1, width)
    full_x = full_x.reshape(-1, width)
    gains = gains.swapaxes(0, 1).reshape(4, width).astype(F32)
    gains_p = perm(gains)

    grad_ffn_own = cotangent.reshape(tok_count, width)
    held_cot, full_x = lax.optimization_barrier((grad_ffn_own, full_x))
    grad_ffn = lax.all_gather(held_cot, "sp", axis=0, tiled=True)
    (a_low,) = row_call(
        first_kernel, "first", (full_x, gains_p), ("row", "gains"), ((block_len, BF),), block_len, width, 64
    )
    proj = mm(a_low, w_proj)
    head_pos = ctx_i * block_len + jnp.arange(block_len, dtype=jnp.int32)
    cos_h, sin_h = angles(head_pos, DK)

    rates = lax.dynamic_slice_in_dim(decay_rate, sp_i * heads, heads)
    offs = jnp.arange(block_len, dtype=F32)
    spacing = offs[:, None] - offs[None, :]
    mask = jnp.where(
        spacing[None] >= 0.0, jnp.exp(-rates[:, None, None] * jnp.maximum(spacing, 0.0)[None]), 0.0
    )
    inward = jnp.exp(-rates[:, None] * (offs[None, :] + 1.0))[:, :, None]
    outward = jnp.exp(-rates[:, None] * (block_len - 1.0 - offs[None, :]))[:, :, None]
    blocks = jnp.arange(ctx_n)
    back_gap = (ctx_i - 1 - blocks).astype(F32)
    back_w = jnp.where(
        blocks[:, None] < ctx_i,
        jnp.exp(-rates[None, :] * block_len * jnp.maximum(back_gap, 0.0)[:, None]),
        0.0,
    )
    fore_gap = (blocks - ctx_i - 1).astype(F32)
    fore_w = jnp.where(
        blocks[:, None] > ctx_i,
        jnp.exp(-rates[None, :] * block_len * jnp.maximum(fore_gap, 0.0)[:, None]),
        0.0,
    )

    wide, small = (heads, block_len, DV), (heads, block_len, DK)
    corner = (heads, DK, DV)
    qs, ks, vs, kw, own_state = head_call(
        heads_kernel,
        "heads",
        heads,
        (proj, proj, proj, cos_h, sin_h, outward),
        ((DK, 0), (DK, heads), (DV, heads), "all", "all", "head"),
        ((small, "head"), (small, "head"), (wide, "head"), (small, "head"), (corner, "head")),
    )
    states, up_rows = exchange(
        [("block", own_state), ("swap", slabs[:, :, cut:])], sp_n, f_n, 2, 25
    )
    gate_at = (DV, 2 * heads)
    square = (heads, block_len, block_len)
    state, probs, mixed, gated = head_call(
        retain_kernel,
        "retain",
        heads,
        (back_w, states, qs, ks, vs, proj, mask, inward),
        ("scalar", "parts", "head", "head", "head", gate_at, "head", "head"),
        ((corner, "head"), (square, "head"), (wide, "head"), ((block_len, vd_w), (DV, 0))),
    )
    group = rows_in == 64 and sp_n == 4 and plane_n == 8
    fine = 16

    begins = ((sp_i == 0) & (ctx_i == 0)).astype(jnp.int32).reshape(1)

    def parts_of(v):
        return v.astype(BF).reshape(sp_n, tok_count, width)

    def rest_of(dot, left, right, main):
        rows = left.reshape(sp_n, tok_count, -1)[:, :fine].reshape(sp_n * fine, -1)
        exact = dot(rows, right).reshape(sp_n, fine, width)
        return (exact - main[:, :fine].astype(F32)).astype(BF)

    down_rows = o_low[:, width:].reshape(2, -1, width)
    part_h = parts_of(mm(gated, w_o))
    rest_h = rest_of(mm, gated, w_o, part_h)
    got, lo, w_up, w_down = exchange(
        [("swap", part_h), ("lead", rest_h), ("plane", up_rows), ("plane", down_rows)], sp_n, f_n, 4, 50
    )
    w_up, w_down = w_up.reshape(width, -1), w_down.reshape(-1, width)
    hidden, normed_b = row_call(
        functools.partial(ahead_kernel, group),
        "ahead",
        (begins, got, lo, own_x, gains),
        ("scalar", "main", "lo", "row", "gains"),
        ((tok_count, F32), (tok_count, BF)),
        tok_count,
        width,
    )
    (b_low,) = exchange([("gather", normed_b if group else perm(normed_b))], sp_n, f_n, 5, 40)
    b_low = b_low.reshape(block_len, width)
    up = mm(b_low, w_up)
    act_low = jax.nn.gelu(up, approximate=False).astype(BF)
    ffn_part = mm(act_low, w_down).astype(BF)

    grad_act = mm_t(grad_ffn, w_down)
    density = (
        0.5 * (1.0 + lax.erf(up * root_half)) + up * jnp.exp(-0.5 * up * up) * inv_root_tau
    )
    grad_up = (grad_act * density).astype(BF)

    def reduce_rows(v):
        return lax.psum_scatter(v, PLANE, scatter_dimension=0, tiled=True)

    part_down = mm_tn(act_low, grad_ffn).astype(BF)
    part_up = mm_tn(b_low, grad_up).astype(BF)
    part_b = parts_of(mm_t(grad_up, w_up))
    rest_b = rest_of(mm_t, grad_up, w_up, part_b)
    part_b, part_down, part_up = lax.optimization_barrier((part_b, part_down, part_up))
    sum_down = reduce_rows(part_down)
    ctx_own = lambda v: lax.dynamic_index_in_dim(v, ctx_i, 0, False).astype(F32)

    def core_sum(v, others):
        mine = lax.dynamic_index_in_dim(v, lax.axis_index("fsdp"), 1, False)
        return (mine.astype(F32) + jnp.sum(others.astype(F32), 0)).astype(BF)

    part_up = part_up.reshape(ctx_n, f_n, -1, part_up.shape[1])
    if not group:
        part_b, rest_b = unperm(part_b), unperm(rest_b)
    got, lo, up_others = exchange([("swap", part_b), ("lead", rest_b), ("core", part_up)], sp_n, f_n, 6, 50)
    up_half = core_sum(part_up, up_others)
    grad_hidden, grad_branch, sums_b = row_call(
        functools.partial(turn_kernel, group),
        "turn",
        (begins, got, lo, hidden, grad_ffn_own, gains),
        ("scalar", "main", "lo", "row", "row", "gains"),
        ((tok_count, F32), (tok_count, BF), (8, F32)),
        tok_count,
        width,
    )
    grad_branch, sum_down = lax.optimization_barrier((grad_branch, sum_down))
    grad_branch, up_blocks = exchange([("gather", grad_branch), ("ctx_swap", up_half)], sp_n, f_n, 7, 40)
    grad_branch = grad_branch.reshape(block_len, width)
    sum_up = (ctx_own(up_half) + jnp.sum(up_blocks.astype(F32), 0)).astype(BF)
    ffn_part, grad_branch = lax.optimization_barrier((ffn_part, grad_branch))
    ffn = lax.psum_scatter(ffn_part, "sp", scatter_dimension=0, tiled=True)
    part_o = mm_tn(gated, grad_branch).astype(BF)

    grad_gate, grad_mixed, own_reach, grad_scores, grad_q = head_call(
        back_kernel,
        "back",
        heads,
        (mm_t(grad_branch, w_o), proj, mixed, qs, ks, vs, state, mask, inward, cos_h, sin_h),
        ((DV, 0), gate_at) + ("head",) * 7 + ("all", "all"),
        (
            ((block_len, vd_w), (DV, 0)),
            (wide, "head"),
            (corner, "head"),
            (square, "head"),
            ((block_len, qk_w), (DK, 0)),
        ),
    )
    grad_gq = jnp.concatenate([grad_gate, grad_q], 1)
    part_gq = mm_tn(a_low, grad_gq).astype(BF)
    own_reach, part_o, part_gq, sum_down, ffn = lax.optimization_barrier(
        (own_reach, part_o, part_gq, sum_down, ffn)
    )
    sum_gq = reduce_rows(part_gq)
    block_out = (hidden + ffn.astype(F32)).astype(BF).reshape(block_input.shape)
    part_o = part_o.reshape(ctx_n, f_n, -1, width)

    def home(v):
        return v.reshape(sp_n, rows_in, -1)

    reaches, o_others, back_up = exchange(
        [("block", own_reach), ("core", part_o), ("swap", home(sum_up))], sp_n, f_n, 3, 25
    )
    o_half = core_sum(part_o, o_others)
    grad_k, grad_v = head_call(
        later_kernel,
        "later",
        heads,
        (fore_w, reaches, grad_scores, qs, vs, probs, grad_mixed, kw, outward, cos_h, sin_h),
        ("scalar", "parts") + ("head",) * 7 + ("all", "all"),
        (((block_len, qk_w), (DK, 0)), ((block_len, vd_w), (DV, 0))),
    )
    grad_kv = jnp.concatenate([grad_k, grad_v], 1)
    part_kv = mm_tn(a_low, grad_kv).astype(BF)
    grad_proj = jnp.concatenate([grad_gq[:, vd_w:], grad_kv, grad_gate], 1)
    part_a = parts_of(mm_t(grad_proj, w_proj))
    part_a, part_kv, o_half, sum_gq = lax.optimization_barrier((part_a, part_kv, o_half, sum_gq))
    sum_kv = reduce_rows(part_kv)

    got, o_blocks = exchange(
        [("swap", part_a if group else unperm(part_a)), ("ctx_swap", o_half)], sp_n, f_n, 8, 50
    )
    sum_o = ctx_own(o_half) + jnp.sum(o_blocks.astype(F32), 0)
    grad_x, sums_a = row_call(
        functools.partial(last_kernel, group),
        "last",
        (got, own_x, grad_hidden, gains),
        ("main", "row", "row", "gains"),
        ((tok_count, BF), (8, F32)),
        tok_count,
        width,
    )
    grad_x = grad_x.reshape(block_input.shape)
    norm_terms = jnp.concatenate([sums_a[:2], sums_b[:2]], 0)
    norm_parts = norm_terms.reshape(4, n_dev, -1).swapaxes(0, 1)
    norm_sums, back_gq = exchange([("all", norm_parts), ("swap", home(sum_gq))], sp_n, f_n, 9, 20)
    grad_gains = jnp.sum(norm_sums, 0)
    (back_kv,) = exchange([("swap", home(sum_kv))], sp_n, f_n, 10, 22)
    parts = [back_gq[:, :, vd_w:], back_kv[:, :, :qk_w], back_kv[:, :, qk_w:], back_gq[:, :, :vd_w], back_up]
    grad_first = jnp.concatenate(
        [p.swapaxes(0, 1).reshape(rows_in, -1) for p in parts], 1
    ).astype(F32)
    grad_second = jnp.concatenate([sum_o, sum_down.astype(F32)], 1)
    first_m, first_v, first_step = adam_update(weight_in, grad_first, moment_in, square_in)
    second_m, second_v, second_step = adam_update(weight_out, grad_second, moment_out, square_out)
    gain_m, gain_v, gain_step = adam_update(norm_gains, grad_gains, moment_norm, square_norm)
    return (
        block_out,
        grad_x,
        grad_first,
        first_m,
        first_v,
        first_step,
        grad_second,
        second_m,
        second_v,
        second_step,
        grad_gains,
        gain_m,
        gain_v,
        gain_step,
    )


def solution(mesh):
    tokens = P("fsdp", "ctx", "sp", None)
    rows = P(ALL, None)
    cols = P(None, ALL)
    in_specs = (tokens, tokens, P(), rows, rows, cols, rows, rows, rows, rows, cols, cols)
    out_specs = (tokens, tokens) + (rows,) * 8 + (cols,) * 4
    return jax.shard_map(shards, mesh=mesh, in_specs=in_specs, out_specs=out_specs, check_vma=False)
```
